128 devices in a mesh: layer: 2 (over core), px: 16 (over x, z), py: 4 (over y).
Axes of the slice: x: 4, y: 4, z: 4, core: 2. Of those that a mesh axis runs over, the one named last changes fastest.
Arguments:
- right_side: float32 [8, 2048, 4096], P('layer', 'px', 'py'), may hold values from -30 to 30
- row_conduct: float32 [8, 2048, 4096], P('layer', 'px', 'py'), may hold values from 0.5 to 2
- column_conduct: float32 [8, 2048, 4096], P('layer', 'px', 'py'), may hold values from 0.5 to 2
- via_conduct: float32 [8, 2048, 4096], P('layer', 'px', 'py'), may hold values from 0.5 to 4
- via_mask: int32 [8, 2048, 4096], P('layer', 'px', 'py'), may hold values 0 or 1
- ground_conduct: float32 [8, 2048, 4096], P('layer', 'px', 'py'), may hold values from 0.01 to 0.1
Outputs:
- solution_field: float32 [8, 2048, 4096], P('layer', 'px', 'py')
- residual: float32 [8, 2048, 4096], P('layer', 'px', 'py')
The draws below stay inside these ranges and needn't reach their ends.
All inputs are finite; a program needn't handle non-finite values. No bound on the sum of `via_mask` on one device may be relied on, other than what follows from the above.
Results may differ from the reference program's by a relative error of at most 0.0001.
Values sent between devices are 32-bit elements; how exact they have to be, the bound alone decides.
A program may use at most 128 MiB of HBM per device.

```python
import math
import jax
import jax.numpy as jnp

ITERS = 2
LAYERS = 8
NX = 2048
NY = 4096


def draw_right_side(key, part):
    noise = jax.random.normal(key, (LAYERS, NX, NY), jnp.float32)
    rows = jnp.arange(NX, dtype=jnp.float32) / NX
    ramp = jnp.exp(jnp.log(3.0) * rows)[None, :, None]
    value = noise * ramp
    return jnp.clip(value, -30.0, 30.0)


def touch_ends(drawn, own_key, smallest, high):
    spot = [jax.random.randint(jax.random.fold_in(own_key, axis), (), 0, length) for axis, length in enumerate(drawn.shape)]
    longest = drawn.shape.index(max(drawn.shape))
    next_to = spot[:longest] + [(spot[longest] + 1) % drawn.shape[longest]] + spot[longest + 1:]
    return drawn.at[tuple(spot)].set(smallest).at[tuple(next_to)].set(high)


def shard_levels(key, dims, cuts, low, top_value):
    loudness = 1.0
    for dim, parts in cuts:
        heights = jax.random.uniform(jax.random.fold_in(jax.random.fold_in(key, 6), dim), (parts,), jnp.float32, low / len(cuts), top_value / len(cuts))
        loudness = loudness * jnp.repeat(jnp.exp(heights), dims[dim] // parts).reshape((-1,) + (1,) * (len(dims) - 1 - dim))
    return loudness


def setup_inputs(seed: int = 0) -> dict:
    streams_of = jax.random.split(jax.random.key(seed), 7)
    return {
        "right_side": draw_right_side(jax.random.fold_in(streams_of[6], 71), 0),
        "row_conduct": jnp.clip(jnp.exp(math.log(2.0) - 1.3862944 * jax.random.uniform(streams_of[1], (LAYERS, NX, NY), jnp.float32) ** shard_levels(streams_of[1], (LAYERS, NX, NY), ((0, 2), (1, 16), (2, 4)), -0.2, 0.2)), 0.5, 2.0),
        "column_conduct": jnp.clip(jnp.exp(math.log(2.0) - 1.3862944 * jax.random.uniform(streams_of[2], (LAYERS, NX, NY), jnp.float32) ** shard_levels(streams_of[2], (LAYERS, NX, NY), ((0, 2), (1, 16), (2, 4)), -0.2, 0.2)), 0.5, 2.0),
        "via_conduct": jnp.clip(jnp.exp(math.log(4.0) - 2.0794415 * jax.random.uniform(streams_of[3], (LAYERS, NX, NY), jnp.float32) ** shard_levels(streams_of[3], (LAYERS, NX, NY), ((0, 2), (1, 16), (2, 4)), -0.2, 0.2)), 0.5, 4.0),
        "via_mask": touch_ends((jax.random.randint(streams_of[4], (LAYERS, NX, NY), 0, 4) < 3).astype(jnp.int32), jax.random.fold_in(streams_of[4], 1), 0, 1),
        "ground_conduct": jnp.clip(jnp.exp(math.log(0.1) - 2.3025851 * jax.random.uniform(streams_of[5], (LAYERS, NX, NY), jnp.float32) ** shard_levels(streams_of[5], (LAYERS, NX, NY), ((0, 2), (1, 16), (2, 4)), -0.2, 0.2)), 0.01, 0.1),
    }


def factor_layers(diagonal, vertical, vertical_below, carried):
    gains = []
    inverses = []
    previous = carried
    for index in range(diagonal.shape[0]):
        inverse = 1.0 / (diagonal[index] - vertical_below[index] * previous)
        previous = vertical[index] * inverse
        gains.append(previous)
        inverses.append(inverse)
    return jnp.stack(gains), jnp.stack(inverses)


def forward_layers(residual, vertical_below, inverses, carried):
    values = []
    previous = carried
    for index in range(residual.shape[0]):
        previous = (residual[index] + vertical_below[index] * previous) * inverses[index]
        values.append(previous)
    return jnp.stack(values)


def back_layers(forward, gains, carried):
    count = forward.shape[0]
    values = [None] * count
    following = carried
    for index in range(count - 1, -1, -1):
        following = forward[index] + gains[index] * following
        values[index] = following
    return jnp.stack(values)


def operate(field, coeffs):
    diagonal, row_conduct, row_upper, column_conduct, column_left, vertical, vertical_below = coeffs
    padded = jnp.pad(field, 1)
    return (diagonal * field
            - row_conduct * padded[1:-1, 2:, 1:-1]
            - row_upper * padded[1:-1, :-2, 1:-1]
            - column_conduct * padded[1:-1, 1:-1, 2:]
            - column_left * padded[1:-1, 1:-1, :-2]
            - vertical * padded[2:, 1:-1, 1:-1]
            - vertical_below * padded[:-2, 1:-1, 1:-1])


def reference(right_side, row_conduct, column_conduct, via_conduct, via_mask, ground_conduct):
    level = jnp.arange(LAYERS, dtype=jnp.int32)
    keep = (level < LAYERS - 1).astype(right_side.dtype)[:, None, None]
    vertical = via_conduct * via_mask.astype(right_side.dtype) * keep
    row_upper = jnp.concatenate([jnp.zeros_like(row_conduct[:, :1, :]), row_conduct[:, :-1, :]], axis=1)
    column_left = jnp.concatenate([jnp.zeros_like(column_conduct[:, :, :1]), column_conduct[:, :, :-1]], axis=2)
    vertical_below = jnp.concatenate([jnp.zeros_like(vertical[:1]), vertical[:-1]], axis=0)
    diagonal = ground_conduct + row_conduct + row_upper + column_conduct + column_left + vertical + vertical_below
    coeffs = (diagonal, row_conduct, row_upper, column_conduct, column_left, vertical, vertical_below)
    plane = jnp.zeros_like(right_side[0])
    gains, inverses = factor_layers(diagonal, vertical, vertical_below, plane)

    def precondition(residual):
        forward = forward_layers(residual, vertical_below, inverses, plane)
        return back_layers(forward, gains, plane)

    solution_field = jnp.zeros_like(right_side)
    residual = right_side
    precond = precondition(residual)
    direction = precond
    rho = jnp.sum(residual * precond)
    for step in range(ITERS):
        image = operate(direction, coeffs)
        alpha = rho / jnp.sum(direction * image)
        solution_field = solution_field + alpha * direction
        residual = residual - alpha * image
        if step + 1 < ITERS:
            precond = precondition(residual)
            rho_next = jnp.sum(residual * precond)
            direction = precond + (rho_next / rho) * direction
            rho = rho_next
    return solution_field, residual
```

```python
import functools

import jax
import jax.numpy as jnp
from jax import lax
from jax.experimental import pallas as pl
from jax.experimental.pallas import tpu as pltpu
from jax.sharding import PartitionSpec as P

MESH = pl.DeviceIdType.MESH
F32 = jnp.float32
D = 4
T = 8
W = 128


def kernel(
    shape, counts,
    b_hbm, rw_hbm, cl_hbm, vi_hbm, mk_hbm, gd_hbm,
    x_ref, r_ref,
    bb, rwp, cl, vi, mk, gd, inv, gain, num, w_ref, v_ref, c3, q3a, q3b,
    zb, qb, yb, qyb, fg_out, fg_in, f_out, f_in,
    row_out, row_in, col_out, col_in,
    zrow_out, zrow_in, zcol_out, zcol_in,
    part, group, total_out, total_in,
    load_sem, s_send, s_recv, z_send, z_recv, m_send, m_recv, g_send, g_recv, p_send, p_recv,
):
    rows, cols = shape
    layers, pxs, pys = counts
    nt = cols // W
    ni = rows // T
    layer = lax.axis_index("layer")
    px = lax.axis_index("px")
    py = lax.axis_index("py")
    bottom = layer == 0
    loc = [s + layer * (D - 1 - 2 * s) for s in range(D)]
    via = [s + layer * (D - 2 - 2 * s) for s in range(D - 1)]
    size1 = layers * pys
    me1 = layer * pys + py

    def group_peer(d):
        other = lax.rem(me1 + d, size1)
        return {"layer": other // pys, "py": lax.rem(other, pys)}

    def px_peer(d):
        return {"px": lax.rem(px + d, pxs)}

    def py_peer(d):
        return {"py": lax.rem(py + d, pys)}

    partner = {"layer": 1 - layer}
    barrier = pltpu.get_barrier_semaphore()
    for d in range(1, size1):
        pl.semaphore_signal(barrier, inc=1, device_id=group_peer(d), device_id_type=MESH)
    for d in range(1, pxs):
        pl.semaphore_signal(barrier, inc=1, device_id=px_peer(d), device_id_type=MESH)

    slot = [0]

    def load(src, dst):
        copy = pltpu.make_async_copy(src, dst, load_sem.at[slot[0]])
        slot[0] += 1
        copy.start()
        return copy

    last = (nt - 1) * W
    first_loads = [
        load(rw_hbm.at[:, rows - T : rows, :], rwp.at[:, rows : rows + T, :]),
        load(cl_hbm.at[:, :, last : last + W], cl.at[:, :, last : last + W]),
        load(vi_hbm.at[D - 1], vi.at[D - 1]),
        load(mk_hbm.at[D - 1], mk.at[D - 1]),
    ]
    chunks = 4
    step = rows // chunks
    chunk_loads = []
    for c in range(chunks):
        at = pl.ds(c * step, step)
        short = step - T if c == chunks - 1 else step
        chunk_loads.append([
            load(rw_hbm.at[:, pl.ds(c * step, short), :], rwp.at[:, pl.ds(T + c * step, short), :]),
            load(cl_hbm.at[:, at, 0:last], cl.at[:, at, 0:last]),
            load(vi_hbm.at[0 : D - 1, at, :], vi.at[0 : D - 1, at, :]),
            load(mk_hbm.at[0 : D - 1, at, :], mk.at[0 : D - 1, at, :]),
            load(gd_hbm.at[:, at, :], gd.at[:, at, :]),
            load(b_hbm.at[:, at, :], bb.at[:, at, :]),
        ])

    lane = lax.broadcasted_iota(jnp.int32, (T, W), 1)
    sub = lax.broadcasted_iota(jnp.int32, (T, W), 0)
    zero = jnp.zeros((T, W), F32)

    def remote(src, dst, send, recv, peer):
        return pltpu.make_async_remote_copy(
            src_ref=src, dst_ref=dst, send_sem=send, recv_sem=recv,
            device_id=peer, device_id_type=MESH,
        )

    def lanes(t):
        return slice(t * W, (t + 1) * W)

    def tile_at(r):
        return pl.ds(pl.multiple_of(r, T), T)

    for copy in first_loads:
        copy.wait()
    for s in range(D):
        for t in range(nt):
            row_out[s, t : t + 1, :] = rwp[loc[s], rows + T - 1 : rows + T, lanes(t)]

    def pack_col(i, packed):
        at = tile_at(i * T)
        for s in range(D):
            k = s * ni + i
            packed = jnp.where(lane == k, pltpu.roll(cl[loc[s], at, lanes(nt - 1)], k + 1, axis=1), packed)
        return packed

    col_out[...] = lax.fori_loop(0, ni, pack_col, zero)

    def join(i, carry):
        at = tile_at(i * T)
        c3[at, :] = vi[D - 1, at, :] * mk[D - 1, at, :].astype(F32)
        return carry

    @pl.when(bottom)
    def _():
        lax.fori_loop(0, ni, join, 0)

    pl.semaphore_wait(barrier, size1 - 1 + pxs - 1)
    row_copy = remote(row_out, row_in, s_send.at[0], s_recv.at[0], px_peer(1))
    col_copy = remote(col_out, col_in, s_send.at[1], s_recv.at[1], py_peer(1))
    row_copy.start()
    col_copy.start()
    c3_copy = remote(c3, c3, s_send.at[2], s_recv.at[2], partner)

    @pl.when(bottom)
    def _():
        c3_copy.start()

    sends = [row_copy, col_copy]

    def inner(i):
        r = i * T
        return [(r, t) for t in range(1, nt - 1)]

    def sides(j):
        starts = [j * 4 * T + m * T for m in range(4)]
        return [(r, t) for r in starts for t in (0, nt - 1)]

    def ends(j):
        r = j * (rows - T)
        return [(r, t) for t in range(1, nt - 1)]

    def edge_work(body, carry):
        carry = lax.fori_loop(0, ni // 4, lambda j, c: body(sides(j), c), carry)
        return lax.fori_loop(0, 2, lambda j, c: body(ends(j), c), carry)

    def inner_work(body, carry, start=1, stop=None):
        stop = ni - 1 if stop is None else stop
        return lax.fori_loop(start, stop, lambda i, c: body(inner(i), c), carry)

    def spread(packed, k, to):
        return pltpu.roll(packed, lax.rem(to + W - k, W), axis=1)

    def factor(items, carry):
        g = [None] * len(items)
        n = [None] * len(items)
        below = [None] * len(items)
        for s in range(D):
            l = loc[s]
            for m, (r, t) in enumerate(items):
                at = tile_at(r)
                rw = rwp[l, tile_at(r + T), lanes(t)]
                before = rwp[l, at, lanes(t)]
                up = pltpu.roll(jnp.where(sub == T - 1, before, rw), 1, axis=0)
                c = cl[l, at, lanes(t)]
                if t == 0:
                    k = s * ni + r // T
                    left = jnp.where(lane == 0, spread(col_in[...], k, 0), pltpu.roll(c, 1, axis=1))
                else:
                    left = pltpu.roll(jnp.where(lane == W - 1, cl[l, at, lanes(t - 1)], c), 1, axis=1)
                if s < D - 1:
                    above = vi[via[s], at, lanes(t)] * mk[via[s], at, lanes(t)].astype(F32)
                else:
                    above = c3[at, lanes(t)]
                diagonal = gd[l, at, lanes(t)] + rw + up + c + left + above
                right_side = bb[l, at, lanes(t)]
                if s:
                    diagonal = diagonal + below[m]
                    inverse = 1.0 / (diagonal - below[m] * g[m])
                    n[m] = right_side + g[m] * n[m]
                else:
                    inverse = 1.0 / diagonal
                    n[m] = right_side
                below[m] = above
                g[m] = above * inverse
                inv[s, at, lanes(t)] = inverse
                gain[s, at, lanes(t)] = g[m]
                num[s, at, lanes(t)] = n[m]
                if s == D - 1:
                    fg_out[0, at, lanes(t)] = n[m] * inverse
                    fg_out[1, at, lanes(t)] = g[m]
        return carry

    regions = [
        (pl.ds(T, rows - 2 * T), pl.ds(W, cols - 2 * W)),
        (pl.ds(0, rows), pl.ds(0, W)),
        (pl.ds(0, rows), pl.ds(cols - W, W)),
        (pl.ds(0, T), pl.ds(W, cols - 2 * W)),
        (pl.ds(rows - T, T), pl.ds(W, cols - 2 * W)),
    ]

    def middle(out, into, which, base):
        copies = []
        for e in which:
            i, j = regions[e]
            if len(out.shape) == 3:
                src, dst = out.at[:, i, j], into.at[:, i, j]
            else:
                src, dst = out.at[i, j], into.at[i, j]
            copies.append(remote(src, dst, m_send.at[base + e], m_recv.at[base + e], partner))
        for copy in copies:
            copy.start()
        sends.extend(copies)
        return copies

    @pl.when(jnp.logical_not(bottom))
    def _():
        c3_copy.wait_recv()

    for c in range(chunks):
        for copy in chunk_loads[c]:
            copy.wait()
        lo = max(1, c * step // T)
        hi = min(ni - 1, (c + 1) * step // T)
        inner_work(factor, 0, lo, hi)
    fg_inner = middle(fg_out, fg_in, [0], 0)

    row_copy.wait_recv()
    col_copy.wait_recv()
    has_upper = px > 0
    has_left = py > 0
    for s in range(D):
        for t in range(nt):
            rwp[loc[s], T - 1 : T, lanes(t)] = jnp.where(has_upper, row_in[s, t : t + 1, :], 0.0)
    col_in[...] = jnp.where(has_left, col_in[...], 0.0)
    edge_work(factor, 0)
    fg_edge = middle(fg_out, fg_in, [1, 2, 3, 4], 0)

    def solve(first, z, q, f_ref, items, carry):
        rho, pack_l, pack_r = carry
        following = [None] * len(items)
        terms = []
        for s in range(D - 1, -1, -1):
            l = loc[s]
            for m, (r, t) in enumerate(items):
                at = tile_at(r)
                if s == D - 1:
                    if first:
                        other = fg_in[1, at, lanes(t)]
                        g = gain[s, at, lanes(t)]
                        quotient = 1.0 / (1.0 - g * other)
                        scale = quotient * inv[s, at, lanes(t)]
                        g = quotient * g
                        q3a[at, lanes(t)] = scale
                        q3b[at, lanes(t)] = g
                        theirs = fg_in[0, at, lanes(t)]
                    else:
                        scale = q3a[at, lanes(t)]
                        g = q3b[at, lanes(t)]
                        theirs = f_ref[at, lanes(t)]
                    value = scale * num[s, at, lanes(t)] + g * theirs
                else:
                    value = num[s, at, lanes(t)] * inv[s, at, lanes(t)] + gain[s, at, lanes(t)] * following[m]
                following[m] = value
                z[s, t, tile_at(r + T), :] = value
                q[s, t, tile_at(r + T), :] = rwp[l, tile_at(r + T), lanes(t)] * value
                if first:
                    terms.append(bb[l, at, lanes(t)] * value)
                if t == 0:
                    k = s * ni + r // T
                    pack_l = jnp.where(lane == k, pltpu.roll(value, k, axis=1), pack_l)
                if t == nt - 1:
                    k = s * ni + r // T
                    side = cl[l, at, lanes(t)] * value
                    pack_r = jnp.where(lane == k, pltpu.roll(side, k + 1, axis=1), pack_r)
        if first:
            rho = rho + tree(terms)
        return rho, pack_l, pack_r

    def tree(values):
        while len(values) > 1:
            values = [a + b for a, b in zip(values[::2], values[1::2])] + ([values[-1]] if len(values) % 2 else [])
        return values[0]

    def halo_send(z, q, pack_l, pack_r, stage):
        zcol_out[stage, 0] = pack_l
        zcol_out[stage, 1] = pack_r
        for s in range(D):
            for t in range(nt):
                zrow_out[stage, 0, s, t : t + 1, :] = z[s, t, T : T + 1, :]
                zrow_out[stage, 1, s, t : t + 1, :] = q[s, t, rows + T - 1 : rows + T, :]
        copies = []
        for n, (out, into, peer) in enumerate((
            (zcol_out.at[stage, 0], zcol_in.at[stage, 0], py_peer(pys - 1)),
            (zcol_out.at[stage, 1], zcol_in.at[stage, 1], py_peer(1)),
            (zrow_out.at[stage, 0], zrow_in.at[stage, 0], px_peer(pxs - 1)),
            (zrow_out.at[stage, 1], zrow_in.at[stage, 1], px_peer(1)),
        )):
            copies.append(remote(out, into, z_send.at[4 * stage + n], z_recv.at[4 * stage + n], peer))
        for copy in copies:
            copy.start()
        sends.extend(copies)
        return copies

    def halo_wait(copies, z, q, stage):
        for copy in copies:
            copy.wait_recv()
        has_lower = px < pxs - 1
        has_right = py < pys - 1
        zcol_in[stage, 0] = jnp.where(has_right, zcol_in[stage, 0], 0.0)
        zcol_in[stage, 1] = jnp.where(has_left, zcol_in[stage, 1], 0.0)
        for s in range(D):
            for t in range(nt):
                z[s, t, rows + T : rows + T + 1, :] = jnp.where(has_lower, zrow_in[stage, 0, s, t : t + 1, :], 0.0)
                q[s, t, T - 1 : T, :] = jnp.where(has_upper, zrow_in[stage, 1, s, t : t + 1, :], 0.0)

    solve_z = functools.partial(solve, True, zb, qb, None)
    carry = (zero, zero, zero)
    for copy in fg_inner + fg_edge:
        copy.wait_recv()
    carry = edge_work(solve_z, carry)
    z_copies = halo_send(zb, qb, carry[1], carry[2], 0)
    rho_part = inner_work(solve_z, carry)[0]

    def coupled(z, q, stage, s, items):
        l = loc[s]
        zs, ps, out = {}, {}, []

        def own(m, r, t):
            if (m, t) not in zs:
                zs[m, t] = z[s, t, tile_at(r + T), :]
            return zs[m, t]

        def product(m, r, t):
            if (m, t) not in ps:
                ps[m, t] = cl[l, tile_at(r), lanes(t)] * own(m, r, t)
            return ps[m, t]

        rows_seen = []
        for r, t in items:
            m = next((n for n, other in enumerate(rows_seen) if other is r), None)
            if m is None:
                rows_seen.append(r)
                m = len(rows_seen) - 1
            at = tile_at(r)
            value = own(m, r, t)
            down = z[s, t, pl.ds(r + T + 1, T), :]
            up = q[s, t, pl.ds(r + T - 1, T), :]
            k = s * ni + r // T
            if t == nt - 1:
                right = jnp.where(lane == W - 1, spread(zcol_in[stage, 0], k, W - 1), pltpu.roll(value, W - 1, axis=1))
            else:
                right = pltpu.roll(jnp.where(lane == 0, own(m, r, t + 1), value), W - 1, axis=1)
            if t == 0:
                left = jnp.where(lane == 0, spread(zcol_in[stage, 1], k, 0), pltpu.roll(product(m, r, t), 1, axis=1))
            else:
                left = pltpu.roll(jnp.where(lane == W - 1, product(m, r, t - 1), product(m, r, t)), 1, axis=1)
            rw = rwp[l, tile_at(r + T), lanes(t)]
            c = cl[l, at, lanes(t)]
            out.append((value, rw * down + up + (c * right + left)))
        return out

    def apply_z(items, curve):
        n = [None] * len(items)
        terms = []
        for s in range(D):
            for m, ((r, t), (value, h)) in enumerate(zip(items, coupled(zb, qb, 0, s, items))):
                at = tile_at(r)
                w = bb[loc[s], at, lanes(t)] - h
                w_ref[s, at, lanes(t)] = w
                terms.append(value * w)
                n[m] = w if s == 0 else w + gain[s - 1, at, lanes(t)] * n[m]
                num[s, at, lanes(t)] = n[m]
                if s == D - 1:
                    f_out[at, lanes(t)] = n[m] * inv[s, at, lanes(t)]
        return curve + tree(terms)

    curve_part = inner_work(apply_z, zero)
    f_inner = middle(f_out, f_in, [0], 5)
    halo_wait(z_copies, zb, qb, 0)
    curve_part = edge_work(apply_z, curve_part)
    f_edge = middle(f_out, f_in, [1, 2, 3, 4], 5)

    def full(value):
        return jnp.sum(jnp.sum(value, axis=0, keepdims=True), axis=1, keepdims=True)

    row_lane = lax.broadcasted_iota(jnp.int32, (1, W), 1)

    def line(values):
        out = jnp.zeros((1, W), F32)
        for n, value in enumerate(values):
            out = jnp.where(row_lane == n, value, out)
        return out

    def gather_group(stage, values):
        part[stage] = line(values)
        group[stage, pl.ds(me1, 1)] = line(values)[None]
        copies = [
            remote(
                part.at[stage], group.at[stage, me1],
                g_send.at[stage * size1 + d], g_recv.at[stage * size1 + d], group_peer(d),
            )
            for d in range(1, size1)
        ]
        for copy in copies:
            copy.start()
        sends.extend(copies)
        return copies

    def group_sum(stage, copies):
        for copy in copies:
            copy.wait_recv()
        return tree([group[stage, m] for m in range(size1)])

    group_copies = gather_group(0, [full(rho_part), full(curve_part)])

    solve_y = functools.partial(solve, False, yb, qyb, f_in)
    carry = (zero, zero, zero)
    for copy in f_inner:
        copy.wait_recv()
    carry = inner_work(solve_y, carry)
    for copy in f_edge:
        copy.wait_recv()
    carry = edge_work(solve_y, carry)
    y_copies = halo_send(yb, qyb, carry[1], carry[2], 1)

    sums = group_sum(0, group_copies)

    def pick(value, n):
        return jnp.sum(jnp.where(row_lane == n, value, 0.0), axis=1, keepdims=True)

    rho_group, curve_group = pick(sums, 0), pick(sums, 1)
    ok = (rho_group > 0.0) & (curve_group > 0.0)
    centre = jnp.where(ok, rho_group / jnp.where(ok, curve_group, 1.0), 1.0)
    centre_tile = jnp.broadcast_to(centre, (T, W))

    def apply_y(items, acc):
        terms = [[] for _ in acc]
        for s in range(D):
            for (r, t), (y, h) in zip(items, coupled(yb, qyb, 1, s, items)):
                at = tile_at(r)
                w = w_ref[s, at, lanes(t)]
                v = w - h
                v_ref[s, at, lanes(t)] = v
                z = zb[s, t, tile_at(r + T), :]
                res = bb[loc[s], at, lanes(t)] - centre_tile * w
                pre = z - centre_tile * y
                image = w - centre_tile * v
                for n, term in enumerate((res * pre, w * y, pre * image, y * v, z * v)):
                    terms[n].append(term)
        return tuple(a + tree(b) for a, b in zip(acc, terms))

    acc = inner_work(apply_y, (zero,) * 5)
    halo_wait(y_copies, yb, qyb, 1)
    acc = edge_work(apply_y, acc)

    group_copies = gather_group(1, [full(a) for a in acc])
    sums2 = group_sum(1, group_copies)
    message = line([pick(sums2, n) for n in range(5)] + [centre, rho_group, curve_group])
    total_out[...] = message
    total_in[pl.ds(px, 1), :] = message
    copies = [
        remote(total_out, total_in.at[pl.ds(px, 1), :], p_send.at[d], p_recv.at[d], px_peer(d))
        for d in range(1, pxs)
    ]
    for copy in copies:
        copy.start()
    sends.extend(copies)
    for copy in copies:
        copy.wait_recv()
    table = total_in[...]
    table_lane = lax.broadcasted_iota(jnp.int32, table.shape, 1)
    s0, s2, t0, t2, zv, at0, rho_g, curve_g = (
        jnp.sum(jnp.where(table_lane == n, table, 0.0), axis=1, keepdims=True) for n in range(8)
    )

    def over(value):
        return jnp.sum(value, axis=0, keepdims=True)

    rho = over(rho_g)
    alpha = rho / over(curve_g)
    delta = jnp.broadcast_to(alpha, at0.shape) - at0
    rho_next = over(s0 - delta * (2.0 * (curve_g - at0 * s2) - delta * s2))
    curve = over(t0 - delta * ((s2 + zv - 2.0 * at0 * t2) - delta * t2))
    beta = rho_next / rho
    alpha_next = rho_next / (curve - beta * rho_next / alpha)
    big = jnp.broadcast_to(alpha + alpha_next * (1.0 + beta), (T, W))
    small = jnp.broadcast_to(alpha * alpha_next, (T, W))

    def finish(i, carry):
        at = tile_at(i * T)
        for s in range(D):
            l = loc[s]
            for t in range(nt):
                z = zb[s, t, tile_at(i * T + T), :]
                y = yb[s, t, tile_at(i * T + T), :]
                x_ref[l, at, lanes(t)] = big * z - small * y
                r_ref[l, at, lanes(t)] = bb[l, at, lanes(t)] - big * w_ref[s, at, lanes(t)] + small * v_ref[s, at, lanes(t)]
        return carry

    lax.fori_loop(0, ni, finish, 0)
    for copy in sends:
        copy.wait_send()

    @pl.when(bottom)
    def _():
        c3_copy.wait_send()


def solution(mesh):
    layers, pxs, pys = (mesh.shape[a] for a in ("layer", "px", "py"))
    spec = P("layer", "px", "py")

    def step(*args):
        depth, rows, cols = args[0].shape
        nt = cols // W
        block = (depth, rows, cols)
        padded = (depth, nt, rows + 2 * T, W)
        size1 = layers * pys
        dma = pltpu.SemaphoreType.DMA
        vmem = lambda *dims: pltpu.VMEM(dims, F32)
        scratch = [
            vmem(*block), vmem(depth, rows + T, cols), vmem(*block), vmem(*block),
            pltpu.VMEM(block, jnp.int32), vmem(*block), vmem(*block), vmem(*block), vmem(*block),
            vmem(*block), vmem(*block), vmem(rows, cols), vmem(rows, cols), vmem(rows, cols),
            vmem(*padded), vmem(*padded), vmem(*padded), vmem(*padded),
            vmem(2, rows, cols), vmem(2, rows, cols), vmem(rows, cols), vmem(rows, cols),
            vmem(depth, nt, W), vmem(depth, nt, W), vmem(T, W), vmem(T, W),
            vmem(2, 2, depth, nt, W), vmem(2, 2, depth, nt, W), vmem(2, 2, T, W), vmem(2, 2, T, W),
            vmem(2, 1, W), vmem(2, size1, 1, W), vmem(1, W), vmem(pxs, W),
            dma((28,)), dma((3,)), dma((3,)), dma((8,)), dma((8,)), dma((10,)), dma((10,)),
            dma((2 * size1,)), dma((2 * size1,)), dma((pxs,)), dma((pxs,)),
        ]
        out = jax.ShapeDtypeStruct(block, F32)
        return pl.pallas_call(
            functools.partial(kernel, (rows, cols), (layers, pxs, pys)),
            out_shape=(out, out),
            in_specs=[pl.BlockSpec(memory_space=pltpu.HBM)] * 6,
            out_specs=(pl.BlockSpec(memory_space=pltpu.VMEM),) * 2,
            scratch_shapes=scratch,
            compiler_params=pltpu.CompilerParams(
                collective_id=0, has_side_effects=True, vmem_limit_bytes=48 * 2**20
            ),
        )(*args)

    return jax.shard_map(step, mesh=mesh, in_specs=(spec,) * 6, out_specs=(spec, spec), check_vma=False)
```

```python
import functools

import jax
import jax.numpy as jnp
from jax import lax
from jax.experimental import pallas as pl
from jax.experimental.pallas import tpu as pltpu
from jax.sharding import PartitionSpec as P

MESH = pl.DeviceIdType.MESH
F32 = jnp.float32
D = 4
T = 8
W = 128


def kernel(
    shape, counts,
    b_hbm, rw_hbm, cl_hbm, vi_hbm, mk_hbm, gd_hbm,
    bb, zb, yb, w_ref, v_ref, factors,
    rwp, cl, vi, mk, gd, inv, gain, num, c3, q3a, q3b,
    qb, qyb, fg_out, fg_in, f_out, f_in,
    row_out, row_in, col_out, col_in,
    zrow_out, zrow_in, zcol_out, zcol_in,
    part, group, total_out, total_in,
    load_sem, s_send, s_recv, z_send, z_recv, m_send, m_recv, g_send, g_recv, p_send, p_recv, far_sem,
):
    rows, cols = shape
    layers, pxs, pys = counts
    nt = cols // W
    ni = rows // T
    layer = lax.axis_index("layer")
    px = lax.axis_index("px")
    py = lax.axis_index("py")
    bottom = layer == 0
    loc = [s + layer * (D - 1 - 2 * s) for s in range(D)]
    via = [s + layer * (D - 2 - 2 * s) for s in range(D - 1)]
    size1 = layers * pys
    me1 = layer * pys + py

    def group_peer(d):
        other = lax.rem(me1 + d, size1)
        return {"layer": other // pys, "py": lax.rem(other, pys)}

    def px_peer(d):
        return {"px": lax.rem(px + d, pxs)}

    def py_peer(d):
        return {"py": lax.rem(py + d, pys)}

    partner = {"layer": 1 - layer}
    near = [partner, px_peer(1), px_peer(pxs - 1), py_peer(1), py_peer(pys - 1)]

    slot = [0]

    def load(src, dst):
        copy = pltpu.make_async_copy(src, dst, load_sem.at[slot[0]])
        slot[0] += 1
        return copy

    last = (nt - 1) * W
    cl_edge = load(cl_hbm.at[:, :, last : last + W], cl.at[:, :, last : last + W])
    rw_edge = load(rw_hbm.at[:, rows - T : rows, :], rwp.at[:, rows : rows + T, :])
    top_loads = [load(vi_hbm.at[D - 1], vi.at[D - 1]), load(mk_hbm.at[D - 1], mk.at[D - 1])]
    cl_edge.start()
    rw_edge.start()

    @pl.when(bottom)
    def _():
        for copy in top_loads:
            copy.start()

    barrier = pltpu.get_barrier_semaphore()
    for peer in near:
        pl.semaphore_signal(barrier, inc=1, device_id=peer, device_id_type=MESH)

    chunks = 4
    step = rows // chunks
    chunk_loads = []
    for c in range(chunks):
        at = pl.ds(c * step, step)
        short = step - T if c == chunks - 1 else step
        chunk_loads.append([
            load(rw_hbm.at[:, pl.ds(c * step, short), :], rwp.at[:, pl.ds(T + c * step, short), :]),
            load(cl_hbm.at[:, at, 0:last], cl.at[:, at, 0:last]),
            load(vi_hbm.at[0 : D - 1, at, :], vi.at[0 : D - 1, at, :]),
            load(mk_hbm.at[0 : D - 1, at, :], mk.at[0 : D - 1, at, :]),
            load(gd_hbm.at[:, at, :], gd.at[:, at, :]),
            load(b_hbm.at[:, at, :], bb.at[:, at, :]),
        ])
        for copy in chunk_loads[-1]:
            copy.start()

    lane = lax.broadcasted_iota(jnp.int32, (T, W), 1)
    sub = lax.broadcasted_iota(jnp.int32, (T, W), 0)
    zero = jnp.zeros((T, W), F32)

    def remote(src, dst, send, recv, peer):
        return pltpu.make_async_remote_copy(
            src_ref=src, dst_ref=dst, send_sem=send, recv_sem=recv,
            device_id=peer, device_id_type=MESH,
        )

    def lanes(t):
        return slice(t * W, (t + 1) * W)

    def tile_at(r):
        return pl.ds(pl.multiple_of(r, T), T)

    cl_edge.wait()
    packs = []
    for s in range(D):
        packed = zero
        for i in range(ni):
            k = s * ni + i
            value = cl[loc[s], i * T : (i + 1) * T, lanes(nt - 1)]
            packed = jnp.where(lane == k, pltpu.roll(value, (k + 1) % W, axis=1), packed)
        packs.append(packed)
    col_out[...] = (packs[0] + packs[1]) + (packs[2] + packs[3])
    rw_edge.wait()
    for s in range(D):
        for t in range(nt):
            row_out[s, t : t + 1, :] = rwp[loc[s], rows + T - 1 : rows + T, lanes(t)]

    pl.semaphore_wait(barrier, len(near))
    row_copy = remote(row_out, row_in, s_send.at[0], s_recv.at[0], px_peer(1))
    col_copy = remote(col_out, col_in, s_send.at[1], s_recv.at[1], py_peer(1))
    col_copy.start()
    row_copy.start()
    c3_copies = [
        remote(c3.at[pl.ds(c * step, step)], c3.at[pl.ds(c * step, step)], s_send.at[2 + c], s_recv.at[2 + c], partner)
        for c in range(chunks)
    ]

    def join(i, carry):
        at = tile_at(i * T)
        c3[at, :] = vi[D - 1, at, :] * mk[D - 1, at, :].astype(F32)
        return carry

    @pl.when(bottom)
    def _():
        for copy in top_loads:
            copy.wait()
        for c in range(chunks):
            lax.fori_loop(c * step // T, (c + 1) * step // T, join, 0)
            c3_copies[c].start()

    sends = [row_copy, col_copy]

    def inner(i):
        r = i * T
        return [(r, t) for t in range(1, nt - 1)]

    def sides(j):
        starts = [j * 4 * T + m * T for m in range(4)]
        return [(r, t) for r in starts for t in (0, nt - 1)]

    def ends(j):
        r = j * (rows - T)
        return [(r, t) for t in range(1, nt - 1)]

    def edge_work(body, carry):
        carry = lax.fori_loop(0, ni // 4, lambda j, c: body(sides(j), c), carry)
        return lax.fori_loop(0, 2, lambda j, c: body(ends(j), c), carry)

    def inner_work(body, carry, start=1, stop=None):
        stop = ni - 1 if stop is None else stop
        return lax.fori_loop(start, stop, lambda i, c: body(inner(i), c), carry)

    def spread(packed, k, to):
        return pltpu.roll(packed, lax.rem(to + W - k, W), axis=1)

    def factor(items, carry):
        g = [None] * len(items)
        n = [None] * len(items)
        below = [None] * len(items)
        for s in range(D):
            l = loc[s]
            for m, (r, t) in enumerate(items):
                at = tile_at(r)
                rw = rwp[l, tile_at(r + T), lanes(t)]
                before = rwp[l, at, lanes(t)]
                up = pltpu.roll(jnp.where(sub == T - 1, before, rw), 1, axis=0)
                c = cl[l, at, lanes(t)]
                if t == 0:
                    k = s * ni + r // T
                    left = jnp.where(lane == 0, spread(col_in[...], k, 0), pltpu.roll(c, 1, axis=1))
                else:
                    left = pltpu.roll(jnp.where(lane == W - 1, cl[l, at, lanes(t - 1)], c), 1, axis=1)
                if s < D - 1:
                    above = vi[via[s], at, lanes(t)] * mk[via[s], at, lanes(t)].astype(F32)
                else:
                    above = c3[at, lanes(t)]
                diagonal = gd[l, at, lanes(t)] + rw + up + c + left + above
                right_side = bb[l, at, lanes(t)]
                if s:
                    diagonal = diagonal + below[m]
                    inverse = 1.0 / (diagonal - below[m] * g[m])
                    n[m] = right_side + g[m] * n[m]
                else:
                    inverse = 1.0 / diagonal
                    n[m] = right_side
                below[m] = above
                g[m] = above * inverse
                inv[s, at, lanes(t)] = inverse
                gain[s, at, lanes(t)] = g[m]
                num[s, at, lanes(t)] = n[m]
                if s == D - 1:
                    fg_out[0, at, lanes(t)] = n[m] * inverse
                    fg_out[1, at, lanes(t)] = g[m]
        return carry

    regions = [
        (pl.ds(T, rows - 2 * T), pl.ds(W, cols - 2 * W)),
        (pl.ds(0, rows), pl.ds(0, W)),
        (pl.ds(0, rows), pl.ds(cols - W, W)),
        (pl.ds(0, T), pl.ds(W, cols - 2 * W)),
        (pl.ds(rows - T, T), pl.ds(W, cols - 2 * W)),
    ]

    def middle(out, into, which, base):
        copies = []
        for e in which:
            i, j = regions[e]
            if len(out.shape) == 3:
                src, dst = out.at[:, i, j], into.at[:, i, j]
            else:
                src, dst = out.at[i, j], into.at[i, j]
            copies.append(remote(src, dst, m_send.at[base + e], m_recv.at[base + e], partner))
        for copy in copies:
            copy.start()
        sends.extend(copies)
        return copies

    for c in range(chunks):
        for copy in chunk_loads[c]:
            copy.wait()

        @pl.when(jnp.logical_not(bottom))
        def _():
            c3_copies[c].wait_recv()

        lo = max(1, c * step // T)
        hi = min(ni - 1, (c + 1) * step // T)
        inner_work(factor, 0, lo, hi)
    fg_inner = middle(fg_out, fg_in, [0], 0)

    row_copy.wait_recv()
    col_copy.wait_recv()
    has_upper = px > 0
    has_left = py > 0
    for s in range(D):
        for t in range(nt):
            rwp[loc[s], T - 1 : T, lanes(t)] = jnp.where(has_upper, row_in[s, t : t + 1, :], 0.0)
    col_in[...] = jnp.where(has_left, col_in[...], 0.0)
    edge_work(factor, 0)
    fg_edge = middle(fg_out, fg_in, [1, 2, 3, 4], 0)

    def solve(first, z, q, f_ref, items, carry):
        rho, pack_l, pack_r = carry
        following = [None] * len(items)
        terms = []
        for s in range(D - 1, -1, -1):
            l = loc[s]
            for m, (r, t) in enumerate(items):
                at = tile_at(r)
                if s == D - 1:
                    if first:
                        other = fg_in[1, at, lanes(t)]
                        g = gain[s, at, lanes(t)]
                        quotient = 1.0 / (1.0 - g * other)
                        scale = quotient * inv[s, at, lanes(t)]
                        g = quotient * g
                        q3a[at, lanes(t)] = scale
                        q3b[at, lanes(t)] = g
                        theirs = fg_in[0, at, lanes(t)]
                    else:
                        scale = q3a[at, lanes(t)]
                        g = q3b[at, lanes(t)]
                        theirs = f_ref[at, lanes(t)]
                    value = scale * num[s, at, lanes(t)] + g * theirs
                else:
                    value = num[s, at, lanes(t)] * inv[s, at, lanes(t)] + gain[s, at, lanes(t)] * following[m]
                following[m] = value
                z[s, t, tile_at(r + T), :] = value
                q[s, t, tile_at(r + T), :] = rwp[l, tile_at(r + T), lanes(t)] * value
                if first:
                    terms.append(bb[l, at, lanes(t)] * value)
                if t == 0:
                    k = s * ni + r // T
                    pack_l = jnp.where(lane == k, pltpu.roll(value, k, axis=1), pack_l)
                if t == nt - 1:
                    k = s * ni + r // T
                    side = cl[l, at, lanes(t)] * value
                    pack_r = jnp.where(lane == k, pltpu.roll(side, k + 1, axis=1), pack_r)
        if first:
            rho = rho + tree(terms)
        return rho, pack_l, pack_r

    def tree(values):
        while len(values) > 1:
            values = [a + b for a, b in zip(values[::2], values[1::2])] + ([values[-1]] if len(values) % 2 else [])
        return values[0]

    def halo_send(z, q, pack_l, pack_r, stage):
        zcol_out[stage, 0] = pack_l
        zcol_out[stage, 1] = pack_r
        for s in range(D):
            for t in range(nt):
                zrow_out[stage, 0, s, t : t + 1, :] = z[s, t, T : T + 1, :]
                zrow_out[stage, 1, s, t : t + 1, :] = q[s, t, rows + T - 1 : rows + T, :]
        copies = []
        for n, (out, into, peer) in enumerate((
            (zcol_out.at[stage, 0], zcol_in.at[stage, 0], py_peer(pys - 1)),
            (zcol_out.at[stage, 1], zcol_in.at[stage, 1], py_peer(1)),
            (zrow_out.at[stage, 0], zrow_in.at[stage, 0], px_peer(pxs - 1)),
            (zrow_out.at[stage, 1], zrow_in.at[stage, 1], px_peer(1)),
        )):
            copies.append(remote(out, into, z_send.at[4 * stage + n], z_recv.at[4 * stage + n], peer))
        for copy in copies:
            copy.start()
        sends.extend(copies)
        return copies

    def halo_wait(copies, z, q, stage):
        for copy in copies:
            copy.wait_recv()
        has_lower = px < pxs - 1
        has_right = py < pys - 1
        zcol_in[stage, 0] = jnp.where(has_right, zcol_in[stage, 0], 0.0)
        zcol_in[stage, 1] = jnp.where(has_left, zcol_in[stage, 1], 0.0)
        for s in range(D):
            for t in range(nt):
                z[s, t, rows + T : rows + T + 1, :] = jnp.where(has_lower, zrow_in[stage, 0, s, t : t + 1, :], 0.0)
                q[s, t, T - 1 : T, :] = jnp.where(has_upper, zrow_in[stage, 1, s, t : t + 1, :], 0.0)

    solve_z = functools.partial(solve, True, zb, qb, None)
    for copy in fg_inner:
        copy.wait_recv()
    rho_inner = inner_work(solve_z, (zero, zero, zero))[0]
    for copy in fg_edge:
        copy.wait_recv()
    rho_edge, pack_l, pack_r = edge_work(solve_z, (zero, zero, zero))
    z_copies = halo_send(zb, qb, pack_l, pack_r, 0)

    def coupled(z, q, stage, s, items):
        l = loc[s]
        zs, ps, out = {}, {}, []

        def own(m, r, t):
            if (m, t) not in zs:
                zs[m, t] = z[s, t, tile_at(r + T), :]
            return zs[m, t]

        def product(m, r, t):
            if (m, t) not in ps:
                ps[m, t] = cl[l, tile_at(r), lanes(t)] * own(m, r, t)
            return ps[m, t]

        rows_seen = []
        for r, t in items:
            m = next((n for n, other in enumerate(rows_seen) if other is r), None)
            if m is None:
                rows_seen.append(r)
                m = len(rows_seen) - 1
            at = tile_at(r)
            value = own(m, r, t)
            down = z[s, t, pl.ds(r + T + 1, T), :]
            up = q[s, t, pl.ds(r + T - 1, T), :]
            k = s * ni + r // T
            if t == nt - 1:
                right = jnp.where(lane == W - 1, spread(zcol_in[stage, 0], k, W - 1), pltpu.roll(value, W - 1, axis=1))
            else:
                right = pltpu.roll(jnp.where(lane == 0, own(m, r, t + 1), value), W - 1, axis=1)
            if t == 0:
                left = jnp.where(lane == 0, spread(zcol_in[stage, 1], k, 0), pltpu.roll(product(m, r, t), 1, axis=1))
            else:
                left = pltpu.roll(jnp.where(lane == W - 1, product(m, r, t - 1), product(m, r, t)), 1, axis=1)
            rw = rwp[l, tile_at(r + T), lanes(t)]
            c = cl[l, at, lanes(t)]
            out.append((value, rw * down + up + (c * right + left)))
        return out

    def apply_z(items, curve):
        n = [None] * len(items)
        terms = []
        for s in range(D):
            for m, ((r, t), (value, h)) in enumerate(zip(items, coupled(zb, qb, 0, s, items))):
                at = tile_at(r)
                w = bb[loc[s], at, lanes(t)] - h
                w_ref[s, at, lanes(t)] = w
                terms.append(value * w)
                n[m] = w if s == 0 else w + gain[s - 1, at, lanes(t)] * n[m]
                num[s, at, lanes(t)] = n[m]
                if s == D - 1:
                    f_out[at, lanes(t)] = n[m] * inv[s, at, lanes(t)]
        return curve + tree(terms)

    def full(value):
        return jnp.sum(jnp.sum(value, axis=0, keepdims=True), axis=1, keepdims=True)

    row_lane = lax.broadcasted_iota(jnp.int32, (1, W), 1)

    def line(values):
        out = jnp.zeros((1, W), F32)
        for n, value in enumerate(values):
            out = jnp.where(row_lane == n, value, out)
        return out

    def gather_group(stage, values):
        part[stage] = line(values)
        group[stage, pl.ds(me1, 1)] = line(values)[None]
        copies = [
            remote(
                part.at[stage], group.at[stage, me1],
                g_send.at[stage * size1 + d], g_recv.at[stage * size1 + d], group_peer(d),
            )
            for d in range(1, size1)
        ]
        for copy in copies:
            copy.start()
        sends.extend(copies)
        return copies

    def group_sum(stage, copies):
        for copy in copies:
            copy.wait_recv()
        return tree([group[stage, m] for m in range(size1)])

    curve_inner = inner_work(apply_z, zero)
    f_inner = middle(f_out, f_in, [0], 5)
    group_copies = gather_group(0, [full(rho_inner), full(curve_inner)])
    halo_wait(z_copies, zb, qb, 0)

    hops = []
    while (2 << len(hops)) * 2 < pxs:
        hops.append(2 << len(hops))

    def greet(n):
        for d in (hops[n], pxs - hops[n]):
            pl.semaphore_signal(far_sem.at[n], inc=1, device_id=px_peer(d), device_id_type=MESH)

    if hops:
        greet(0)
    curve_edge = edge_work(apply_z, zero)
    f_edge = middle(f_out, f_in, [1, 2, 3, 4], 5)

    solve_y = functools.partial(solve, False, yb, qyb, f_in)
    carry = (zero, zero, zero)
    for copy in f_inner:
        copy.wait_recv()
    carry = inner_work(solve_y, carry)
    for copy in f_edge:
        copy.wait_recv()
    carry = edge_work(solve_y, carry)
    y_copies = halo_send(yb, qyb, carry[1], carry[2], 1)
    if hops:
        pl.semaphore_wait(far_sem.at[0], 2)
        if len(hops) > 1:
            greet(1)

    sums = group_sum(0, group_copies)

    def pick(value, n):
        return jnp.sum(jnp.where(row_lane == n, value, 0.0), axis=1, keepdims=True)

    rho_group, curve_group = pick(sums, 0), pick(sums, 1)
    ok = (rho_group > 0.0) & (curve_group > 0.0)
    centre = jnp.where(ok, rho_group / jnp.where(ok, curve_group, 1.0), 1.0)
    centre_tile = jnp.broadcast_to(centre, (T, W))

    def apply_y(items, acc):
        terms = [[] for _ in acc]
        for s in range(D):
            for (r, t), (y, h) in zip(items, coupled(yb, qyb, 1, s, items)):
                at = tile_at(r)
                w = w_ref[s, at, lanes(t)]
                v = w - h
                v_ref[s, at, lanes(t)] = v
                z = zb[s, t, tile_at(r + T), :]
                res = bb[loc[s], at, lanes(t)] - centre_tile * w
                pre = z - centre_tile * y
                image = w - centre_tile * v
                for n, term in enumerate((res * pre, w * y, pre * image, y * v, z * v)):
                    terms[n].append(term)
        return tuple(a + tree(b) for a, b in zip(acc, terms))

    acc = inner_work(apply_y, (zero,) * 5)
    halo_wait(y_copies, yb, qyb, 1)
    acc = edge_work(apply_y, acc)

    s0, s2, t0, t2, zv, rho_own, curve_own = (
        full(value) for value in acc + (rho_inner + rho_edge, curve_inner + curve_edge)
    )
    group_copies = gather_group(1, [
        s0, 2.0 * (curve_own - centre * s2), s2,
        t0, s2 + zv - 2.0 * centre * t2, t2,
        rho_own, curve_own,
    ])
    for n in range(1, len(hops)):
        pl.semaphore_wait(far_sem.at[n], 2)
        if n + 1 < len(hops):
            greet(n + 1)
    message = jnp.where(row_lane == 8, centre, group_sum(1, group_copies))
    total_out[...] = message
    total_in[pl.ds(px, 1), :] = message
    copies = [
        remote(total_out, total_in.at[pl.ds(px, 1), :], p_send.at[d], p_recv.at[d], px_peer(d))
        for d in range(1, pxs)
    ]
    for copy in copies:
        copy.start()
    sends.extend(copies)
    for copy in copies:
        copy.wait_recv()
    table = total_in[...]
    table_lane = lax.broadcasted_iota(jnp.int32, table.shape, 1)
    centres = jnp.sum(jnp.where(table_lane == 8, table, 0.0), axis=1, keepdims=True)
    plain = jnp.sum(table, axis=0, keepdims=True)
    rho, curve_first = pick(plain, 6), pick(plain, 7)
    alpha = rho / curve_first
    delta = alpha - centres
    linear = (table_lane == 1) | (table_lane == 4)
    square = (table_lane == 2) | (table_lane == 5)
    powers = jnp.where(linear, -delta, jnp.where(square, delta * delta, 1.0))
    moved = jnp.sum(table * powers, axis=0, keepdims=True)
    rho_next = jnp.sum(jnp.where(row_lane < 3, moved, 0.0), axis=1, keepdims=True)
    curve = jnp.sum(jnp.where((row_lane >= 3) & (row_lane < 6), moved, 0.0), axis=1, keepdims=True)
    beta = rho_next / rho
    alpha_next = rho_next / (curve - beta * rho_next / alpha)
    factors[0] = jnp.broadcast_to(alpha + alpha_next * (1.0 + beta), (T, W))
    factors[1] = jnp.broadcast_to(alpha * alpha_next, (T, W))
    for copy in sends:
        copy.wait_send()

    @pl.when(bottom)
    def _():
        for copy in c3_copies:
            copy.wait_send()


def finish(shape, bb, zb, yb, w_ref, v_ref, factors, x_hbm, r_hbm, x_buf, r_buf, sem):
    rows, cols = shape
    layer = lax.axis_index("layer")
    loc = [s + layer * (D - 1 - 2 * s) for s in range(D)]
    big, small = factors[0], factors[1]
    chunks = 4
    step = rows // chunks
    copies = []

    def body(i, carry):
        r = i * T
        at = pl.ds(pl.multiple_of(r, T), T)
        above = pl.ds(pl.multiple_of(r + T, T), T)
        for s in range(D):
            l = loc[s]
            for t in range(cols // W):
                col = slice(t * W, (t + 1) * W)
                x_buf[l, at, col] = big * zb[s, t, above, :] - small * yb[s, t, above, :]
                r_buf[l, at, col] = bb[l, at, col] - big * w_ref[s, at, col] + small * v_ref[s, at, col]
        return carry

    for c in range(chunks):
        lax.fori_loop(c * step // T, (c + 1) * step // T, body, 0)
        at = pl.ds(c * step, step)
        for n, (src, dst) in enumerate(((x_buf, x_hbm), (r_buf, r_hbm))):
            copies.append(pltpu.make_async_copy(src.at[:, at, :], dst.at[:, at, :], sem.at[2 * c + n]))
            copies[-1].start()
    for copy in copies:
        copy.wait()


def solution(mesh):
    layers, pxs, pys = (mesh.shape[a] for a in ("layer", "px", "py"))
    spec = P("layer", "px", "py")

    def step(*args):
        depth, rows, cols = args[0].shape
        nt = cols // W
        block = (depth, rows, cols)
        padded = (depth, nt, rows + 2 * T, W)
        size1 = layers * pys
        dma = pltpu.SemaphoreType.DMA
        vmem = lambda *dims: pltpu.VMEM(dims, F32)
        scratch = [
            vmem(depth, rows + T, cols), vmem(*block), vmem(*block), pltpu.VMEM(block, jnp.int32), vmem(*block),
            vmem(*block), vmem(*block), vmem(*block), vmem(rows, cols), vmem(rows, cols), vmem(rows, cols),
            vmem(*padded), vmem(*padded),
            vmem(2, rows, cols), vmem(2, rows, cols), vmem(rows, cols), vmem(rows, cols),
            vmem(depth, nt, W), vmem(depth, nt, W), vmem(T, W), vmem(T, W),
            vmem(2, 2, depth, nt, W), vmem(2, 2, depth, nt, W), vmem(2, 2, T, W), vmem(2, 2, T, W),
            vmem(2, 1, W), vmem(2, size1, 1, W), vmem(1, W), vmem(pxs, W),
            dma((28,)), dma((6,)), dma((6,)), dma((8,)), dma((8,)), dma((10,)), dma((10,)),
            dma((2 * size1,)), dma((2 * size1,)), dma((pxs,)), dma((pxs,)), pltpu.SemaphoreType.REGULAR((4,)),
        ]
        out = lambda *dims: jax.ShapeDtypeStruct(dims, F32)
        in_vmem = pl.BlockSpec(memory_space=pltpu.VMEM)
        in_hbm = pl.BlockSpec(memory_space=pltpu.HBM)
        kept = pl.pallas_call(
            functools.partial(kernel, (rows, cols), (layers, pxs, pys)),
            out_shape=(vmem(*block), vmem(*padded), vmem(*padded), vmem(*block), vmem(*block), vmem(2, T, W)),
            in_specs=[in_hbm] * 6,
            out_specs=(in_vmem,) * 6,
            scratch_shapes=scratch,
            compiler_params=pltpu.CompilerParams(
                collective_id=0, has_side_effects=True, vmem_limit_bytes=36 * 2**20
            ),
        )(*(pltpu.with_memory_space_constraint(arg, pltpu.HBM) for arg in args))
        return pl.pallas_call(
            functools.partial(finish, (rows, cols)),
            out_shape=(out(*block), out(*block)),
            in_specs=[in_vmem] * 6,
            out_specs=(in_hbm, in_hbm),
            scratch_shapes=[vmem(*block), vmem(*block), dma((8,))],
            compiler_params=pltpu.CompilerParams(vmem_limit_bytes=6 * 2**20),
        )(*kept)

    return jax.shard_map(step, mesh=mesh, in_specs=(spec,) * 6, out_specs=(spec, spec), check_vma=False)
```

```python
import functools

import jax
import jax.numpy as jnp
from jax import lax
from jax.experimental import pallas as pl
from jax.experimental.pallas import tpu as pltpu
from jax.sharding import PartitionSpec as P

MESH = pl.DeviceIdType.MESH
F32 = jnp.float32
D = 4
T = 8
W = 128


def kernel(shape, counts, *refs):
    dma = pltpu.SemaphoreType.DMA
    pl.run_scoped(functools.partial(solve_all, shape, counts, *refs), dma((28,)), dma((32,)))


def solve_all(
    shape, counts,
    b_hbm, rw_hbm, cl_hbm, vi_hbm, mk_hbm, gd_hbm,
    bb, zb, yb, w_ref, v_ref, factors,
    rwp, cl, vi, mk, gd, inv, gain, num, c3, q3a, q3b,
    qb, qyb, fg_out, fg_in, f_out, f_in,
    row_out, row_in, col_out, col_in,
    zrow_out, zrow_in, zcol_out, zcol_in,
    part, group, total_out, table_ref, sized,
    s_recv, z_recv, m_recv, g_recv, p_recv, far_sem,
    load_sem, out_sem,
):
    rows, cols = shape
    layers, pxs, pys = counts
    nt = cols // W
    ni = rows // T
    layer = lax.axis_index("layer")
    px = lax.axis_index("px")
    py = lax.axis_index("py")
    bottom = layer == 0
    loc = [s + layer * (D - 1 - 2 * s) for s in range(D)]
    via = [s + layer * (D - 2 - 2 * s) for s in range(D - 1)]
    size1 = layers * pys
    me1 = layer * pys + py

    def group_peer(d):
        other = lax.rem(me1 + d, size1)
        return {"layer": other // pys, "py": lax.rem(other, pys)}

    def px_peer(d):
        return {"px": lax.rem(px + d, pxs)}

    def py_peer(d):
        return {"py": lax.rem(py + d, pys)}

    partner = {"layer": 1 - layer}
    near = [partner, px_peer(1), px_peer(pxs - 1), py_peer(1), py_peer(pys - 1)]

    slot = [0]

    def load(src, dst):
        copy = pltpu.make_async_copy(src, dst, load_sem.at[slot[0]])
        slot[0] += 1
        return copy

    last = (nt - 1) * W
    cl_edge = load(cl_hbm.at[:, :, last : last + W], cl.at[:, :, last : last + W])
    rw_edge = load(rw_hbm.at[:, rows - T : rows, :], rwp.at[:, rows : rows + T, :])
    top_loads = [load(vi_hbm.at[D - 1], vi.at[D - 1]), load(mk_hbm.at[D - 1], mk.at[D - 1])]
    cl_edge.start()
    rw_edge.start()

    @pl.when(bottom)
    def _():
        for copy in top_loads:
            copy.start()

    barrier = pltpu.get_barrier_semaphore()
    for peer in near:
        pl.semaphore_signal(barrier, inc=1, device_id=peer, device_id_type=MESH)

    chunks = 4
    step = rows // chunks
    chunk_loads = []
    for c in range(chunks):
        at = pl.ds(c * step, step)
        short = step - T if c == chunks - 1 else step
        chunk_loads.append([
            load(rw_hbm.at[:, pl.ds(c * step, short), :], rwp.at[:, pl.ds(T + c * step, short), :]),
            load(cl_hbm.at[:, at, 0:last], cl.at[:, at, 0:last]),
            load(vi_hbm.at[0 : D - 1, at, :], vi.at[0 : D - 1, at, :]),
            load(mk_hbm.at[0 : D - 1, at, :], mk.at[0 : D - 1, at, :]),
            load(gd_hbm.at[:, at, :], gd.at[:, at, :]),
            load(b_hbm.at[:, at, :], bb.at[:, at, :]),
        ])
        for copy in chunk_loads[-1]:
            copy.start()

    lane = lax.broadcasted_iota(jnp.int32, (T, W), 1)
    sub = lax.broadcasted_iota(jnp.int32, (T, W), 0)
    zero = jnp.zeros((T, W), F32)

    out_slot = [2]

    def remote(src, dst, recv, peer, send=None):
        if send is None:
            send = out_sem.at[out_slot[0]]
            out_slot[0] += 1
        return pltpu.make_async_remote_copy(
            src_ref=src, dst_ref=dst, send_sem=send, recv_sem=recv,
            device_id=peer, device_id_type=MESH,
        )

    def wait_rows(count, sem):
        pltpu.make_async_copy(sized.at[0:count], sized.at[0:count], sem).wait()

    def lanes(t):
        return slice(t * W, (t + 1) * W)

    def tile_at(r):
        return pl.ds(pl.multiple_of(r, T), T)

    cl_edge.wait()
    packs = []
    for s in range(D):
        packed = zero
        for i in range(ni):
            k = s * ni + i
            value = cl[loc[s], i * T : (i + 1) * T, lanes(nt - 1)]
            packed = jnp.where(lane == k, pltpu.roll(value, (k + 1) % W, axis=1), packed)
        packs.append(packed)
    col_out[...] = (packs[0] + packs[1]) + (packs[2] + packs[3])
    rw_edge.wait()
    for s in range(D):
        for t in range(nt):
            row_out[s, t : t + 1, :] = rwp[loc[s], rows + T - 1 : rows + T, lanes(t)]

    pl.semaphore_wait(barrier, len(near))
    row_copy = remote(row_out, row_in, s_recv.at[0], px_peer(1))
    col_copy = remote(col_out, col_in, s_recv.at[1], py_peer(1))
    col_copy.start()
    row_copy.start()
    for peer in near:
        pl.semaphore_signal(far_sem.at[0], inc=1, device_id=peer, device_id_type=MESH)
    pieces = 2
    piece = rows // pieces
    c3_copies = [
        remote(c3.at[pl.ds(c * piece, piece)], c3.at[pl.ds(c * piece, piece)], s_recv.at[2 + c], partner)
        for c in range(pieces)
    ]

    def join(i, carry):
        at = tile_at(i * T)
        c3[at, :] = vi[D - 1, at, :] * mk[D - 1, at, :].astype(F32)
        return carry

    @pl.when(bottom)
    def _():
        for copy in top_loads:
            copy.wait()
        for c in range(pieces):
            lax.fori_loop(c * piece // T, (c + 1) * piece // T, join, 0)
            c3_copies[c].start()

    sends = [row_copy, col_copy]

    hops = []
    while (2 << len(hops)) < pxs // 2:
        hops.append(2 << len(hops))

    def greet(n):
        if n < len(hops):
            for d in (hops[n], pxs - hops[n]):
                pl.semaphore_signal(far_sem.at[1 + n], inc=1, device_id=px_peer(d), device_id_type=MESH)

    def greeted(n):
        if n < len(hops):
            pl.semaphore_wait(far_sem.at[1 + n], 2)

    def inner(i):
        r = i * T
        return [(r, t) for t in range(1, nt - 1)]

    def sides(j):
        starts = [j * 4 * T + m * T for m in range(4)]
        return [(r, t) for r in starts for t in (0, nt - 1)]

    def ends(j):
        r = j * (rows - T)
        return [(r, t) for t in range(1, nt - 1)]

    def edge_work(body, carry):
        carry = lax.fori_loop(0, ni // 4, lambda j, c: body(sides(j), c), carry)
        return lax.fori_loop(0, 2, lambda j, c: body(ends(j), c), carry)

    def inner_work(body, carry, start=1, stop=None):
        stop = ni - 1 if stop is None else stop
        return lax.fori_loop(start, stop, lambda i, c: body(inner(i), c), carry)

    def spread(packed, k, to):
        return pltpu.roll(packed, lax.rem(to + W - k, W), axis=1)

    def coupling(s, at, t):
        return vi[via[s], at, lanes(t)] * mk[via[s], at, lanes(t)].astype(F32)

    def factor(first, stop, items, carry):
        g = [None] * len(items)
        n = [None] * len(items)
        below = [None] * len(items)
        if first:
            for m, (r, t) in enumerate(items):
                at = tile_at(r)
                g[m] = gain[first - 1, at, lanes(t)]
                n[m] = num[first - 1, at, lanes(t)]
                below[m] = coupling(first - 1, at, t)
        for s in range(first, stop):
            l = loc[s]
            for m, (r, t) in enumerate(items):
                at = tile_at(r)
                rw = rwp[l, tile_at(r + T), lanes(t)]
                before = rwp[l, at, lanes(t)]
                up = pltpu.roll(jnp.where(sub == T - 1, before, rw), 1, axis=0)
                c = cl[l, at, lanes(t)]
                if t == 0:
                    k = s * ni + r // T
                    left = jnp.where(lane == 0, spread(col_in[...], k, 0), pltpu.roll(c, 1, axis=1))
                else:
                    left = pltpu.roll(jnp.where(lane == W - 1, cl[l, at, lanes(t - 1)], c), 1, axis=1)
                if s < D - 1:
                    above = coupling(s, at, t)
                else:
                    above = c3[at, lanes(t)]
                diagonal = gd[l, at, lanes(t)] + rw + up + c + left + above
                right_side = bb[l, at, lanes(t)]
                if s:
                    diagonal = diagonal + below[m]
                    inverse = 1.0 / (diagonal - below[m] * g[m])
                    n[m] = right_side + g[m] * n[m]
                else:
                    inverse = 1.0 / diagonal
                    n[m] = right_side
                below[m] = above
                g[m] = above * inverse
                inv[s, at, lanes(t)] = inverse
                gain[s, at, lanes(t)] = g[m]
                num[s, at, lanes(t)] = n[m]
                if s == D - 1:
                    fg_out[0, at, lanes(t)] = n[m] * inverse
                    fg_out[1, at, lanes(t)] = g[m]
        return carry

    regions = [
        (pl.ds(T, rows - 2 * T), pl.ds(W, cols - 2 * W)),
        (pl.ds(0, rows), pl.ds(0, W)),
        (pl.ds(0, rows), pl.ds(cols - W, W)),
        (pl.ds(0, T), pl.ds(W, cols - 2 * W)),
        (pl.ds(rows - T, T), pl.ds(W, cols - 2 * W)),
    ]

    def middle(out, into, which, base):
        copies = []
        for e, (i, j) in enumerate(which):
            if len(out.shape) == 3:
                src, dst = out.at[:, i, j], into.at[:, i, j]
            else:
                src, dst = out.at[i, j], into.at[i, j]
            copies.append(remote(src, dst, m_recv.at[base + e], partner))
        for copy in copies:
            copy.start()
        sends.extend(copies)
        return copies

    def deep(i):
        r = i * T
        return [(r, t) for t in range(1, nt)]

    outer_levels = functools.partial(factor, 0, D - 1)
    last_level = functools.partial(factor, D - 1, D)
    all_levels = functools.partial(factor, 0, D)
    for c in range(chunks):
        for copy in chunk_loads[c]:
            copy.wait()
        lax.fori_loop(max(1, c * step // T), (c + 1) * step // T, lambda i, x: outer_levels(deep(i), x), 0)
    for c in range(pieces):
        @pl.when(jnp.logical_not(bottom))
        def _():
            c3_copies[c].wait_recv()

        lax.fori_loop(max(1, c * piece // T), (c + 1) * piece // T, lambda i, x: last_level(deep(i), x), 0)
    fg_inner = middle(fg_out, fg_in, [(pl.ds(T, rows - T), pl.ds(W, cols - W))], 0)

    pl.semaphore_wait(far_sem.at[0], len(near))
    greet(0)
    row_copy.wait_recv()
    col_copy.wait_recv()
    has_upper = px > 0
    has_left = py > 0
    for s in range(D):
        for t in range(nt):
            rwp[loc[s], T - 1 : T, lanes(t)] = jnp.where(has_upper, row_in[s, t : t + 1, :], 0.0)
    col_in[...] = jnp.where(has_left, col_in[...], 0.0)
    group_of = min(8, ni)
    lax.fori_loop(
        0, ni // group_of,
        lambda j, x: all_levels([(j * group_of * T + m * T, 0) for m in range(group_of)], x), 0,
    )
    lax.fori_loop(0, 1, lambda i, x: all_levels(deep(i), x), 0)
    fg_edge = middle(fg_out, fg_in, [(pl.ds(0, rows), pl.ds(0, W)), (pl.ds(0, T), pl.ds(W, cols - W))], 1)

    def solve(first, z, q, f_ref, items, carry):
        rho, pack_l, pack_r = carry
        following = [None] * len(items)
        terms = []
        for s in range(D - 1, -1, -1):
            l = loc[s]
            for m, (r, t) in enumerate(items):
                at = tile_at(r)
                if s == D - 1:
                    if first:
                        other = fg_in[1, at, lanes(t)]
                        g = gain[s, at, lanes(t)]
                        quotient = 1.0 / (1.0 - g * other)
                        scale = quotient * inv[s, at, lanes(t)]
                        g = quotient * g
                        q3a[at, lanes(t)] = scale
                        q3b[at, lanes(t)] = g
                        theirs = fg_in[0, at, lanes(t)]
                    else:
                        scale = q3a[at, lanes(t)]
                        g = q3b[at, lanes(t)]
                        theirs = f_ref[at, lanes(t)]
                    value = scale * num[s, at, lanes(t)] + g * theirs
                else:
                    value = num[s, at, lanes(t)] * inv[s, at, lanes(t)] + gain[s, at, lanes(t)] * following[m]
                following[m] = value
                z[s, t, tile_at(r + T), :] = value
                q[s, t, tile_at(r + T), :] = rwp[l, tile_at(r + T), lanes(t)] * value
                if first:
                    terms.append(bb[l, at, lanes(t)] * value)
                if t == 0:
                    k = s * ni + r // T
                    pack_l = jnp.where(lane == k, pltpu.roll(value, k, axis=1), pack_l)
                if t == nt - 1:
                    k = s * ni + r // T
                    side = cl[l, at, lanes(t)] * value
                    pack_r = jnp.where(lane == k, pltpu.roll(side, k + 1, axis=1), pack_r)
        if first:
            rho = rho + tree(terms)
        return rho, pack_l, pack_r

    def tree(values):
        while len(values) > 1:
            values = [a + b for a, b in zip(values[::2], values[1::2])] + ([values[-1]] if len(values) % 2 else [])
        return values[0]

    def halo_send(z, q, pack_l, pack_r, stage):
        zcol_out[stage, 0] = pack_l
        zcol_out[stage, 1] = pack_r
        for s in range(D):
            for t in range(nt):
                zrow_out[stage, 0, s, t : t + 1, :] = z[s, t, T : T + 1, :]
                zrow_out[stage, 1, s, t : t + 1, :] = q[s, t, rows + T - 1 : rows + T, :]
        copies = []
        for n, (out, into, peer) in enumerate((
            (zcol_out.at[stage, 0], zcol_in.at[stage, 0], py_peer(pys - 1)),
            (zcol_out.at[stage, 1], zcol_in.at[stage, 1], py_peer(1)),
            (zrow_out.at[stage, 0], zrow_in.at[stage, 0], px_peer(pxs - 1)),
            (zrow_out.at[stage, 1], zrow_in.at[stage, 1], px_peer(1)),
        )):
            copies.append(remote(out, into, z_recv.at[4 * stage + n], peer))
        for copy in copies:
            copy.start()
        sends.extend(copies)
        return copies

    def halo_wait(copies, z, q, stage):
        for copy in copies:
            copy.wait_recv()
        has_lower = px < pxs - 1
        has_right = py < pys - 1
        zcol_in[stage, 0] = jnp.where(has_right, zcol_in[stage, 0], 0.0)
        zcol_in[stage, 1] = jnp.where(has_left, zcol_in[stage, 1], 0.0)
        for s in range(D):
            for t in range(nt):
                z[s, t, rows + T : rows + T + 1, :] = jnp.where(has_lower, zrow_in[stage, 0, s, t : t + 1, :], 0.0)
                q[s, t, T - 1 : T, :] = jnp.where(has_upper, zrow_in[stage, 1, s, t : t + 1, :], 0.0)

    solve_z = functools.partial(solve, True, zb, qb, None)
    for copy in fg_inner:
        copy.wait_recv()
    rho_inner = inner_work(solve_z, (zero, zero, zero))[0]
    greeted(0)
    greet(1)
    for copy in fg_edge:
        copy.wait_recv()
    rho_edge, pack_l, pack_r = edge_work(solve_z, (zero, zero, zero))
    z_copies = halo_send(zb, qb, pack_l, pack_r, 0)

    def coupled(z, q, stage, s, items):
        l = loc[s]
        zs, ps, out = {}, {}, []

        def own(m, r, t):
            if (m, t) not in zs:
                zs[m, t] = z[s, t, tile_at(r + T), :]
            return zs[m, t]

        def product(m, r, t):
            if (m, t) not in ps:
                ps[m, t] = cl[l, tile_at(r), lanes(t)] * own(m, r, t)
            return ps[m, t]

        rows_seen = []
        for r, t in items:
            m = next((n for n, other in enumerate(rows_seen) if other is r), None)
            if m is None:
                rows_seen.append(r)
                m = len(rows_seen) - 1
            at = tile_at(r)
            value = own(m, r, t)
            down = z[s, t, pl.ds(r + T + 1, T), :]
            up = q[s, t, pl.ds(r + T - 1, T), :]
            k = s * ni + r // T
            if t == nt - 1:
                right = jnp.where(lane == W - 1, spread(zcol_in[stage, 0], k, W - 1), pltpu.roll(value, W - 1, axis=1))
            else:
                right = pltpu.roll(jnp.where(lane == 0, own(m, r, t + 1), value), W - 1, axis=1)
            if t == 0:
                left = jnp.where(lane == 0, spread(zcol_in[stage, 1], k, 0), pltpu.roll(product(m, r, t), 1, axis=1))
            else:
                left = pltpu.roll(jnp.where(lane == W - 1, product(m, r, t - 1), product(m, r, t)), 1, axis=1)
            rw = rwp[l, tile_at(r + T), lanes(t)]
            c = cl[l, at, lanes(t)]
            out.append((value, rw * down + up + (c * right + left)))
        return out

    def apply_z(items, curve):
        n = [None] * len(items)
        terms = []
        for s in range(D):
            for m, ((r, t), (value, h)) in enumerate(zip(items, coupled(zb, qb, 0, s, items))):
                at = tile_at(r)
                w = bb[loc[s], at, lanes(t)] - h
                w_ref[s, at, lanes(t)] = w
                terms.append(value * w)
                n[m] = w if s == 0 else w + gain[s - 1, at, lanes(t)] * n[m]
                num[s, at, lanes(t)] = n[m]
                if s == D - 1:
                    f_out[at, lanes(t)] = n[m] * inv[s, at, lanes(t)]
        return curve + tree(terms)

    def full(value):
        return jnp.sum(jnp.sum(value, axis=0, keepdims=True), axis=1, keepdims=True)

    row_lane = lax.broadcasted_iota(jnp.int32, (1, W), 1)

    def line(values):
        out = jnp.zeros((1, W), F32)
        for n, value in enumerate(values):
            out = jnp.where(row_lane == n, value, out)
        return out

    def gather_group(values):
        part[0] = line(values)
        group[pl.ds(me1, 1)] = line(values)[None]
        for d in range(1, size1):
            remote(part.at[0], group.at[me1], g_recv, group_peer(d), out_sem.at[0]).start()

    def group_sum():
        wait_rows(size1 - 1, g_recv)
        return tree([group[m] for m in range(size1)])

    curve_inner = inner_work(apply_z, zero)
    f_inner = middle(f_out, f_in, regions[:1], 3)
    for n in range(1, len(hops)):
        greeted(n)
        greet(n + 1)
    gather_group([full(rho_inner), full(curve_inner)])
    halo_wait(z_copies, zb, qb, 0)

    curve_edge = edge_work(apply_z, zero)
    f_edge = middle(f_out, f_in, regions[1:], 4)

    solve_y = functools.partial(solve, False, yb, qyb, f_in)
    carry = (zero, zero, zero)
    for copy in f_inner:
        copy.wait_recv()
    carry = inner_work(solve_y, carry)
    for copy in f_edge:
        copy.wait_recv()
    carry = edge_work(solve_y, carry)
    y_copies = halo_send(yb, qyb, carry[1], carry[2], 1)

    sums = group_sum()

    def pick(value, n):
        return jnp.sum(jnp.where(row_lane == n, value, 0.0), axis=1, keepdims=True)

    rho_group, curve_group = pick(sums, 0), pick(sums, 1)
    ok = (rho_group > 0.0) & (curve_group > 0.0)
    centre = jnp.where(ok, rho_group / jnp.where(ok, curve_group, 1.0), 1.0)
    centre_tile = jnp.broadcast_to(centre, (T, W))

    def apply_y(items, acc):
        terms = [[] for _ in acc]
        for s in range(D):
            for (r, t), (y, h) in zip(items, coupled(yb, qyb, 1, s, items)):
                at = tile_at(r)
                w = w_ref[s, at, lanes(t)]
                v = w - h
                v_ref[s, at, lanes(t)] = v
                z = zb[s, t, tile_at(r + T), :]
                res = bb[loc[s], at, lanes(t)] - centre_tile * w
                pre = z - centre_tile * y
                image = w - centre_tile * v
                for n, term in enumerate((res * pre, w * y, pre * image, y * v, z * v)):
                    terms[n].append(term)
        return tuple(a + tree(b) for a, b in zip(acc, terms))

    acc = inner_work(apply_y, (zero,) * 5)
    halo_wait(y_copies, yb, qyb, 1)
    acc = edge_work(apply_y, acc)

    s0, s2, t0, t2, zv, rho_own, curve_own = (
        full(value) for value in acc + (rho_inner + rho_edge, curve_inner + curve_edge)
    )
    total_out[...] = line([
        s0, 2.0 * (curve_own - centre * s2), s2,
        t0, s2 + zv - 2.0 * centre * t2, t2,
        rho_own, curve_own, centre,
    ])
    mine = table_ref.at[pl.ds((layer * pxs + px) * pys + py, 1), :]
    pz = 4 if pxs % 4 == 0 else pxs
    px_hi = pxs // pz
    there = [
        (a, x, z, y) for a in range(layers) for x in range(px_hi) for z in range(pz) for y in range(pys)
    ]
    ring = lambda d, n: min(d, n - d)
    there.sort(key=lambda o: -(ring(o[1], px_hi) + ring(o[2], pz) + ring(o[3], pys)))
    for a, x, z, y in there:
        if a or x or z or y:
            peer = {
                "layer": lax.rem(layer + a, layers),
                "px": lax.rem(px // pz + x, px_hi) * pz + lax.rem(lax.rem(px, pz) + z, pz),
                "py": lax.rem(py + y, pys),
            }
            remote(total_out, mine, p_recv, peer, out_sem.at[1]).start()
    pltpu.make_async_copy(total_out, mine, p_recv).start()
    pltpu.make_async_copy(table_ref, table_ref, p_recv).wait()
    table = table_ref[...]
    table_lane = lax.broadcasted_iota(jnp.int32, table.shape, 1)
    centres = jnp.sum(jnp.where(table_lane == 8, table, 0.0), axis=1, keepdims=True)
    plain = jnp.sum(table, axis=0, keepdims=True)
    rho, curve_first = pick(plain, 6), pick(plain, 7)
    alpha = rho / curve_first
    delta = alpha - centres
    linear = (table_lane == 1) | (table_lane == 4)
    square = (table_lane == 2) | (table_lane == 5)
    powers = jnp.where(linear, -delta, jnp.where(square, delta * delta, 1.0))
    moved = jnp.sum(table * powers, axis=0, keepdims=True)
    rho_next = jnp.sum(jnp.where(row_lane < 3, moved, 0.0), axis=1, keepdims=True)
    curve = jnp.sum(jnp.where((row_lane >= 3) & (row_lane < 6), moved, 0.0), axis=1, keepdims=True)
    beta = rho_next / rho
    alpha_next = rho_next / (curve - beta * rho_next / alpha)
    factors[0] = jnp.broadcast_to(alpha + alpha_next * (1.0 + beta), (T, W))
    factors[1] = jnp.broadcast_to(alpha * alpha_next, (T, W))
    for copy in sends:
        copy.wait_send()
    wait_rows(size1 - 1, out_sem.at[0])
    wait_rows(len(there) - 1, out_sem.at[1])

    @pl.when(bottom)
    def _():
        for copy in c3_copies:
            copy.wait_send()


def finish(shape, bb, zb, yb, w_ref, v_ref, factors, x_hbm, r_hbm, x_buf, r_buf, sem):
    rows, cols = shape
    layer = lax.axis_index("layer")
    loc = [s + layer * (D - 1 - 2 * s) for s in range(D)]
    big, small = factors[0], factors[1]
    chunks = 4
    step = rows // chunks
    copies = []

    def body(i, carry):
        r = i * T
        at = pl.ds(pl.multiple_of(r, T), T)
        above = pl.ds(pl.multiple_of(r + T, T), T)
        for s in range(D):
            l = loc[s]
            for t in range(cols // W):
                col = slice(t * W, (t + 1) * W)
                x_buf[l, at, col] = big * zb[s, t, above, :] - small * yb[s, t, above, :]
                r_buf[l, at, col] = bb[l, at, col] - big * w_ref[s, at, col] + small * v_ref[s, at, col]
        return carry

    for c in range(chunks):
        lax.fori_loop(c * step // T, (c + 1) * step // T, body, 0)
        at = pl.ds(c * step, step)
        for n, (src, dst) in enumerate(((x_buf, x_hbm), (r_buf, r_hbm))):
            copies.append(pltpu.make_async_copy(src.at[:, at, :], dst.at[:, at, :], sem.at[2 * c + n]))
            copies[-1].start()
    for copy in copies:
        copy.wait()


def solution(mesh):
    layers, pxs, pys = (mesh.shape[a] for a in ("layer", "px", "py"))
    spec = P("layer", "px", "py")

    def step(*args):
        depth, rows, cols = args[0].shape
        nt = cols // W
        block = (depth, rows, cols)
        padded = (depth, nt, rows + 2 * T, W)
        size1 = layers * pys
        dma = pltpu.SemaphoreType.DMA
        vmem = lambda *dims: pltpu.VMEM(dims, F32)
        scratch = [
            vmem(depth, rows + T, cols), vmem(*block), vmem(*block), pltpu.VMEM(block, jnp.int32), vmem(*block),
            vmem(*block), vmem(*block), vmem(*block), vmem(rows, cols), vmem(rows, cols), vmem(rows, cols),
            vmem(*padded), vmem(*padded),
            vmem(2, rows, cols), vmem(2, rows, cols), vmem(rows, cols), vmem(rows, cols),
            vmem(depth, nt, W), vmem(depth, nt, W), vmem(T, W), vmem(T, W),
            vmem(2, 2, depth, nt, W), vmem(2, 2, depth, nt, W), vmem(2, 2, T, W), vmem(2, 2, T, W),
            vmem(1, 1, W), vmem(size1, 1, W), vmem(1, W), vmem(size1 * pxs, W), vmem(size1 * pxs, 1, W),
            dma((4,)), dma((8,)), dma((8,)), dma, dma, pltpu.SemaphoreType.REGULAR((4,)),
        ]
        out = lambda *dims: jax.ShapeDtypeStruct(dims, F32)
        in_vmem = pl.BlockSpec(memory_space=pltpu.VMEM)
        in_hbm = pl.BlockSpec(memory_space=pltpu.HBM)
        kept = pl.pallas_call(
            functools.partial(kernel, (rows, cols), (layers, pxs, pys)),
            out_shape=(vmem(*block), vmem(*padded), vmem(*padded), vmem(*block), vmem(*block), vmem(2, T, W)),
            in_specs=[in_hbm] * 6,
            out_specs=(in_vmem,) * 6,
            scratch_shapes=scratch,
            compiler_params=pltpu.CompilerParams(
                collective_id=0, has_side_effects=True, vmem_limit_bytes=36 * 2**20
            ),
        )(*(pltpu.with_memory_space_constraint(arg, pltpu.HBM) for arg in args))
        return pl.pallas_call(
            functools.partial(finish, (rows, cols)),
            out_shape=(out(*block), out(*block)),
            in_specs=[in_vmem] * 6,
            out_specs=(in_hbm, in_hbm),
            scratch_shapes=[vmem(*block), vmem(*block), dma((8,))],
            compiler_params=pltpu.CompilerParams(vmem_limit_bytes=6 * 2**20),
        )(*kept)

    return jax.shard_map(step, mesh=mesh, in_specs=(spec,) * 6, out_specs=(spec, spec), check_vma=False)
```

```python
import functools

import jax
import jax.numpy as jnp
from jax import lax
from jax.experimental import pallas as pl
from jax.experimental.pallas import tpu as pltpu
from jax.sharding import PartitionSpec as P

MESH = pl.DeviceIdType.MESH
F32 = jnp.float32
D = 4
T = 8
W = 128


def kernel(shape, counts, *refs):
    dma = pltpu.SemaphoreType.DMA
    pl.run_scoped(functools.partial(solve_all, shape, counts, *refs), dma((28,)), dma((32,)))


def solve_all(
    shape, counts,
    b_hbm, rw_hbm, cl_hbm, vi_hbm, mk_hbm, gd_hbm,
    bb, zb, yb, w_ref, v_ref, factors,
    rwp, cl, vi, mk, gd, inv, gain, num, c3, q3a, q3b,
    qb, qyb, fg_out, fg_in, f_out, f_in,
    row_out, row_in, col_out, col_in,
    zrow_out, zrow_in, zcol_out, zcol_in,
    part, group, total_out, table_ref, sized,
    s_recv, z_recv, m_recv, g_recv, p_recv, far_sem,
    load_sem, out_sem,
):
    rows, cols = shape
    layers, pxs, pys = counts
    nt = cols // W
    ni = rows // T
    layer = lax.axis_index("layer")
    px = lax.axis_index("px")
    py = lax.axis_index("py")
    bottom = layer == 0
    loc = [s + layer * (D - 1 - 2 * s) for s in range(D)]
    via = [s + layer * (D - 2 - 2 * s) for s in range(D - 1)]
    size1 = layers * pys
    me1 = layer * pys + py

    def group_peer(d):
        other = lax.rem(me1 + d, size1)
        return {"layer": other // pys, "py": lax.rem(other, pys)}

    def px_peer(d):
        return {"px": lax.rem(px + d, pxs)}

    def py_peer(d):
        return {"py": lax.rem(py + d, pys)}

    partner = {"layer": 1 - layer}
    near = [partner, px_peer(1), px_peer(pxs - 1), py_peer(1), py_peer(pys - 1)]

    barrier = pltpu.get_barrier_semaphore()
    for peer in near:
        pl.semaphore_signal(barrier, inc=1, device_id=peer, device_id_type=MESH)
    has_upper, has_lower = px > 0, px < pxs - 1
    has_left, has_right = py > 0, py < pys - 1

    slot = [0]

    def load(src, dst):
        copy = pltpu.make_async_copy(src, dst, load_sem.at[slot[0]])
        slot[0] += 1
        return copy

    last = (nt - 1) * W
    cl_edge = load(cl_hbm.at[:, :, last : last + W], cl.at[:, :, last : last + W])
    rw_edge = load(rw_hbm.at[:, rows - T : rows, :], rwp.at[:, rows : rows + T, :])
    top_loads = [load(vi_hbm.at[D - 1], vi.at[D - 1]), load(mk_hbm.at[D - 1], mk.at[D - 1])]
    cl_edge.start()
    rw_edge.start()

    @pl.when(bottom)
    def _():
        for copy in top_loads:
            copy.start()

    chunks = 4
    step = rows // chunks
    chunk_loads = []
    for c in range(chunks):
        at = pl.ds(c * step, step)
        short = step - T if c == chunks - 1 else step
        chunk_loads.append([
            load(rw_hbm.at[:, pl.ds(c * step, short), :], rwp.at[:, pl.ds(T + c * step, short), :]),
            load(cl_hbm.at[:, at, 0:last], cl.at[:, at, 0:last]),
            load(vi_hbm.at[0 : D - 1, at, :], vi.at[0 : D - 1, at, :]),
            load(mk_hbm.at[0 : D - 1, at, :], mk.at[0 : D - 1, at, :]),
            load(gd_hbm.at[:, at, :], gd.at[:, at, :]),
            load(b_hbm.at[:, at, :], bb.at[:, at, :]),
        ])
        for copy in chunk_loads[-1]:
            copy.start()

    lane = lax.broadcasted_iota(jnp.int32, (T, W), 1)
    sub = lax.broadcasted_iota(jnp.int32, (T, W), 0)
    zero = jnp.zeros((T, W), F32)

    def gate(condition, *actions):
        @pl.when(condition)
        def _():
            for action in actions:
                action()

    out_slot = [2]

    def remote(src, dst, recv, peer, send=None):
        if send is None:
            send = out_sem.at[out_slot[0]]
            out_slot[0] += 1
        return pltpu.make_async_remote_copy(
            src_ref=src, dst_ref=dst, send_sem=send, recv_sem=recv,
            device_id=peer, device_id_type=MESH,
        )

    def wait_rows(count, sem):
        pltpu.make_async_copy(sized.at[0:count], sized.at[0:count], sem).wait()

    def lanes(t):
        return slice(t * W, (t + 1) * W)

    def tile_at(r):
        return pl.ds(pl.multiple_of(r, T), T)

    cl_edge.wait()
    packs = []
    for s in range(D):
        packed = zero
        for i in range(ni):
            k = s * ni + i
            value = cl[loc[s], i * T : (i + 1) * T, lanes(nt - 1)]
            packed = jnp.where(lane == k, pltpu.roll(value, (k + 1) % W, axis=1), packed)
        packs.append(packed)
    col_out[...] = (packs[0] + packs[1]) + (packs[2] + packs[3])
    rw_edge.wait()
    for s in range(D):
        for t in range(nt):
            row_out[s, t : t + 1, :] = rwp[loc[s], rows + T - 1 : rows + T, lanes(t)]

    pl.semaphore_wait(barrier, len(near))
    row_copy = remote(row_out, row_in, s_recv.at[0], px_peer(1))
    col_copy = remote(col_out, col_in, s_recv.at[1], py_peer(1))
    gate(has_right, col_copy.start)
    gate(has_lower, row_copy.start)
    for peer in near:
        pl.semaphore_signal(far_sem.at[0], inc=1, device_id=peer, device_id_type=MESH)
    pieces = 2
    piece = rows // pieces
    c3_copies = [
        remote(c3.at[pl.ds(c * piece, piece)], c3.at[pl.ds(c * piece, piece)], s_recv.at[2 + c], partner)
        for c in range(pieces)
    ]

    def join(i, carry):
        at = tile_at(i * T)
        c3[at, :] = vi[D - 1, at, :] * mk[D - 1, at, :].astype(F32)
        return carry

    @pl.when(bottom)
    def _():
        for copy in top_loads:
            copy.wait()
        for c in range(pieces):
            lax.fori_loop(c * piece // T, (c + 1) * piece // T, join, 0)
            c3_copies[c].start()

    gated = [(has_lower, row_copy), (has_right, col_copy)]
    sends = []

    hops = []
    while (2 << len(hops)) < pxs // 2:
        hops.append(2 << len(hops))

    def greet(n):
        if n < len(hops):
            for d in (hops[n], pxs - hops[n]):
                pl.semaphore_signal(far_sem.at[1 + n], inc=1, device_id=px_peer(d), device_id_type=MESH)

    def greeted(n):
        if n < len(hops):
            pl.semaphore_wait(far_sem.at[1 + n], 2)

    def inner(i):
        r = i * T
        return [(r, t) for t in range(1, nt - 1)]

    def sides(j):
        starts = [j * 4 * T + m * T for m in range(4)]
        return [(r, t) for r in starts for t in (0, nt - 1)]

    def ends(j):
        r = j * (rows - T)
        return [(r, t) for t in range(1, nt - 1)]

    def edge_work(body, carry):
        carry = lax.fori_loop(0, ni // 4, lambda j, c: body(sides(j), c), carry)
        return lax.fori_loop(0, 2, lambda j, c: body(ends(j), c), carry)

    def inner_work(body, carry, start=1, stop=None):
        stop = ni - 1 if stop is None else stop
        return lax.fori_loop(start, stop, lambda i, c: body(inner(i), c), carry)

    def spread(packed, k, to):
        return pltpu.roll(packed, lax.rem(to + W - k, W), axis=1)

    def coupling(s, at, t):
        return vi[via[s], at, lanes(t)] * mk[via[s], at, lanes(t)].astype(F32)

    def factor(first, stop, items, carry):
        g = [None] * len(items)
        n = [None] * len(items)
        below = [None] * len(items)
        if first:
            for m, (r, t) in enumerate(items):
                at = tile_at(r)
                g[m] = gain[first - 1, at, lanes(t)]
                n[m] = num[first - 1, at, lanes(t)]
                below[m] = coupling(first - 1, at, t)
        for s in range(first, stop):
            l = loc[s]
            for m, (r, t) in enumerate(items):
                at = tile_at(r)
                rw = rwp[l, tile_at(r + T), lanes(t)]
                before = rwp[l, at, lanes(t)]
                up = pltpu.roll(jnp.where(sub == T - 1, before, rw), 1, axis=0)
                c = cl[l, at, lanes(t)]
                if t == 0:
                    k = s * ni + r // T
                    left = jnp.where(lane == 0, spread(col_in[...], k, 0), pltpu.roll(c, 1, axis=1))
                else:
                    left = pltpu.roll(jnp.where(lane == W - 1, cl[l, at, lanes(t - 1)], c), 1, axis=1)
                if s < D - 1:
                    above = coupling(s, at, t)
                else:
                    above = c3[at, lanes(t)]
                diagonal = gd[l, at, lanes(t)] + rw + up + c + left + above
                right_side = bb[l, at, lanes(t)]
                if s:
                    diagonal = diagonal + below[m]
                    inverse = 1.0 / (diagonal - below[m] * g[m])
                    n[m] = right_side + g[m] * n[m]
                else:
                    inverse = 1.0 / diagonal
                    n[m] = right_side
                below[m] = above
                g[m] = above * inverse
                inv[s, at, lanes(t)] = inverse
                gain[s, at, lanes(t)] = g[m]
                num[s, at, lanes(t)] = n[m]
                if s == D - 1:
                    fg_out[0, at, lanes(t)] = n[m] * inverse
                    fg_out[1, at, lanes(t)] = g[m]
        return carry

    regions = [
        (pl.ds(T, rows - 2 * T), pl.ds(W, cols - 2 * W)),
        (pl.ds(0, rows), pl.ds(0, W)),
        (pl.ds(0, rows), pl.ds(cols - W, W)),
        (pl.ds(0, T), pl.ds(W, cols - 2 * W)),
        (pl.ds(rows - T, T), pl.ds(W, cols - 2 * W)),
    ]

    def middle(out, into, which, base):
        copies = []
        for e, (i, j) in enumerate(which):
            if len(out.shape) == 3:
                src, dst = out.at[:, i, j], into.at[:, i, j]
            else:
                src, dst = out.at[i, j], into.at[i, j]
            copies.append(remote(src, dst, m_recv.at[base + e], partner))
        for copy in copies:
            copy.start()
        sends.extend(copies)
        return copies

    def deep(i):
        r = i * T
        return [(r, t) for t in range(1, nt)]

    outer_levels = functools.partial(factor, 0, D - 1)
    last_level = functools.partial(factor, D - 1, D)
    all_levels = functools.partial(factor, 0, D)
    fg_inner = []

    def outer_part(c):
        for copy in chunk_loads[c]:
            copy.wait()
        lax.fori_loop(max(1, c * step // T), (c + 1) * step // T, lambda i, x: outer_levels(deep(i), x), 0)

    def last_part(c):
        if c * step % piece == 0:
            gate(jnp.logical_not(bottom), c3_copies[c * step // piece].wait_recv)
        lo = max(T, c * step)
        lax.fori_loop(lo // T, (c + 1) * step // T, lambda i, x: last_level(deep(i), x), 0)
        fg_inner.append(middle(fg_out, fg_in, [(pl.ds(lo, (c + 1) * step - lo), pl.ds(W, cols - W))], c)[0])

    for c in range(chunks):
        outer_part(c)
        if c >= chunks // 2:
            last_part(c - chunks // 2)
    for c in range(chunks // 2, chunks):
        last_part(c)

    pl.semaphore_wait(far_sem.at[0], len(near))
    greet(0)
    gate(has_left, col_copy.wait_recv)
    gate(has_upper, row_copy.wait_recv)
    for s in range(D):
        for t in range(nt):
            rwp[loc[s], T - 1 : T, lanes(t)] = jnp.where(has_upper, row_in[s, t : t + 1, :], 0.0)
    col_in[...] = jnp.where(has_left, col_in[...], 0.0)
    group_of = min(8, ni)
    lax.fori_loop(
        0, ni // group_of,
        lambda j, x: all_levels([(j * group_of * T + m * T, 0) for m in range(group_of)], x), 0,
    )
    lax.fori_loop(0, 1, lambda i, x: all_levels(deep(i), x), 0)
    fg_edge = middle(fg_out, fg_in, [(pl.ds(0, rows), pl.ds(0, W)), (pl.ds(0, T), pl.ds(W, cols - W))], 4)

    def solve(first, z, q, f_ref, items, carry):
        rho, pack_l, pack_r = carry
        following = [None] * len(items)
        terms = []
        for s in range(D - 1, -1, -1):
            l = loc[s]
            for m, (r, t) in enumerate(items):
                at = tile_at(r)
                if s == D - 1:
                    if first:
                        other = fg_in[1, at, lanes(t)]
                        g = gain[s, at, lanes(t)]
                        quotient = 1.0 / (1.0 - g * other)
                        scale = quotient * inv[s, at, lanes(t)]
                        g = quotient * g
                        q3a[at, lanes(t)] = scale
                        q3b[at, lanes(t)] = g
                        theirs = fg_in[0, at, lanes(t)]
                    else:
                        scale = q3a[at, lanes(t)]
                        g = q3b[at, lanes(t)]
                        theirs = f_ref[at, lanes(t)]
                    value = scale * num[s, at, lanes(t)] + g * theirs
                else:
                    value = num[s, at, lanes(t)] * inv[s, at, lanes(t)] + gain[s, at, lanes(t)] * following[m]
                following[m] = value
                z[s, t, tile_at(r + T), :] = value
                q[s, t, tile_at(r + T), :] = rwp[l, tile_at(r + T), lanes(t)] * value
                if first:
                    terms.append(bb[l, at, lanes(t)] * value)
                if t == 0:
                    k = s * ni + r // T
                    pack_l = jnp.where(lane == k, pltpu.roll(value, k, axis=1), pack_l)
                if t == nt - 1:
                    k = s * ni + r // T
                    side = cl[l, at, lanes(t)] * value
                    pack_r = jnp.where(lane == k, pltpu.roll(side, k + 1, axis=1), pack_r)
        if first:
            rho = rho + tree(terms)
        return rho, pack_l, pack_r

    def tree(values):
        while len(values) > 1:
            values = [a + b for a, b in zip(values[::2], values[1::2])] + ([values[-1]] if len(values) % 2 else [])
        return values[0]

    def halo_send(z, q, pack_l, pack_r, stage):
        zcol_out[stage, 0] = pack_l
        zcol_out[stage, 1] = pack_r
        for s in range(D):
            for t in range(nt):
                zrow_out[stage, 0, s, t : t + 1, :] = z[s, t, T : T + 1, :]
                zrow_out[stage, 1, s, t : t + 1, :] = q[s, t, rows + T - 1 : rows + T, :]
        copies = [
            remote(out, into, z_recv.at[4 * stage + n], peer)
            for n, (out, into, peer) in enumerate((
                (zcol_out.at[stage, 0], zcol_in.at[stage, 0], py_peer(pys - 1)),
                (zcol_out.at[stage, 1], zcol_in.at[stage, 1], py_peer(1)),
                (zrow_out.at[stage, 0], zrow_in.at[stage, 0], px_peer(pxs - 1)),
                (zrow_out.at[stage, 1], zrow_in.at[stage, 1], px_peer(1)),
            ))
        ]
        for condition, copy in zip((has_upper, has_lower, has_left, has_right), copies[2:] + copies[:2]):
            gate(condition, copy.start)
            gated.append((condition, copy))
        return copies

    def halo_wait(copies, stage):
        for condition, copy in zip((has_right, has_left, has_lower, has_upper), copies):
            gate(condition, copy.wait_recv)
        zcol_in[stage, 0] = jnp.where(has_right, zcol_in[stage, 0], 0.0)
        zcol_in[stage, 1] = jnp.where(has_left, zcol_in[stage, 1], 0.0)
        zrow_in[stage, 0] = jnp.where(has_lower, zrow_in[stage, 0], 0.0)
        zrow_in[stage, 1] = jnp.where(has_upper, zrow_in[stage, 1], 0.0)

    def place_rows(z, q, stage):
        for s in range(D):
            for t in range(nt):
                z[s, t, rows + T : rows + T + 1, :] = zrow_in[stage, 0, s, t : t + 1, :]
                q[s, t, T - 1 : T, :] = zrow_in[stage, 1, s, t : t + 1, :]

    solve_z = functools.partial(solve, True, zb, qb, None)
    for copy in fg_inner:
        copy.wait_recv()
    rho_inner = inner_work(solve_z, (zero, zero, zero))[0]
    greeted(0)
    greet(1)
    for copy in fg_edge:
        copy.wait_recv()
    rho_edge, pack_l, pack_r = edge_work(solve_z, (zero, zero, zero))
    z_copies = halo_send(zb, qb, pack_l, pack_r, 0)

    def coupled(z, q, stage, s, items):
        l = loc[s]
        zs, ps, out = {}, {}, []

        def own(m, r, t):
            if (m, t) not in zs:
                zs[m, t] = z[s, t, tile_at(r + T), :]
            return zs[m, t]

        def product(m, r, t):
            if (m, t) not in ps:
                ps[m, t] = cl[l, tile_at(r), lanes(t)] * own(m, r, t)
            return ps[m, t]

        rows_seen = []
        for r, t in items:
            m = next((n for n, other in enumerate(rows_seen) if other is r), None)
            if m is None:
                rows_seen.append(r)
                m = len(rows_seen) - 1
            at = tile_at(r)
            value = own(m, r, t)
            down = z[s, t, pl.ds(r + T + 1, T), :]
            up = q[s, t, pl.ds(r + T - 1, T), :]
            k = s * ni + r // T
            if t == nt - 1 and stage is None:
                right = pltpu.roll(jnp.where(lane == 0, 0.0, value), W - 1, axis=1)
            elif t == nt - 1:
                right = jnp.where(lane == W - 1, spread(zcol_in[stage, 0], k, W - 1), pltpu.roll(value, W - 1, axis=1))
            else:
                right = pltpu.roll(jnp.where(lane == 0, own(m, r, t + 1), value), W - 1, axis=1)
            if t == 0 and stage is None:
                left = pltpu.roll(jnp.where(lane == W - 1, 0.0, product(m, r, t)), 1, axis=1)
            elif t == 0:
                left = jnp.where(lane == 0, spread(zcol_in[stage, 1], k, 0), pltpu.roll(product(m, r, t), 1, axis=1))
            else:
                left = pltpu.roll(jnp.where(lane == W - 1, product(m, r, t - 1), product(m, r, t)), 1, axis=1)
            rw = rwp[l, tile_at(r + T), lanes(t)]
            c = cl[l, at, lanes(t)]
            out.append((value, rw * down + up + (c * right + left)))
        return out

    def apply_z(items, curve):
        n = [None] * len(items)
        terms = []
        for s in range(D):
            for m, ((r, t), (value, h)) in enumerate(zip(items, coupled(zb, qb, 0, s, items))):
                at = tile_at(r)
                w = bb[loc[s], at, lanes(t)] - h
                w_ref[s, at, lanes(t)] = w
                terms.append(value * w)
                n[m] = w if s == 0 else w + gain[s - 1, at, lanes(t)] * n[m]
                num[s, at, lanes(t)] = n[m]
                if s == D - 1:
                    f_out[at, lanes(t)] = n[m] * inv[s, at, lanes(t)]
        return curve + tree(terms)

    def down(value):
        return jnp.sum(value, axis=0, keepdims=True)

    def full(value):
        return jnp.sum(down(value), axis=1, keepdims=True)

    row_lane = lax.broadcasted_iota(jnp.int32, (1, W), 1)

    def line(values):
        out = jnp.zeros((1, W), F32)
        for n, value in enumerate(values):
            out = jnp.where(row_lane == n, value, out)
        return out

    def gather_group(values):
        part[0] = line(values)
        group[pl.ds(me1, 1)] = line(values)[None]
        for d in range(1, size1):
            remote(part.at[0], group.at[me1], g_recv, group_peer(d), out_sem.at[0]).start()

    def group_sum():
        wait_rows(size1 - 1, g_recv)
        return tree([group[m] for m in range(size1)])

    curve_inner = inner_work(apply_z, zero)
    f_inner = middle(f_out, f_in, regions[:1], 6)
    for n in range(1, len(hops)):
        greeted(n)
        greet(n + 1)
    gather_group([full(rho_inner), full(curve_inner)])
    halo_wait(z_copies, 0)
    place_rows(zb, qb, 0)

    curve_edge = edge_work(apply_z, zero)
    f_edge = middle(f_out, f_in, regions[1:], 7)

    solve_y = functools.partial(solve, False, yb, qyb, f_in)
    carry = (zero, zero, zero)
    for copy in f_inner:
        copy.wait_recv()
    carry = inner_work(solve_y, carry)
    for copy in f_edge:
        copy.wait_recv()
    carry = edge_work(solve_y, carry)
    y_copies = halo_send(yb, qyb, carry[1], carry[2], 1)

    sums = group_sum()

    def pick(value, n):
        return jnp.sum(jnp.where(row_lane == n, value, 0.0), axis=1, keepdims=True)

    rho_group, curve_group = pick(sums, 0), pick(sums, 1)
    ok = (rho_group > 0.0) & (curve_group > 0.0)
    centre = jnp.where(ok, rho_group / jnp.where(ok, curve_group, 1.0), 1.0)
    centre_tile = jnp.broadcast_to(centre, (T, W))

    def apply_y(items, acc):
        terms = [[] for _ in acc]
        for s in range(D):
            for (r, t), (y, h) in zip(items, coupled(yb, qyb, None, s, items)):
                at = tile_at(r)
                w = w_ref[s, at, lanes(t)]
                v = w - h
                v_ref[s, at, lanes(t)] = v
                z = zb[s, t, tile_at(r + T), :]
                res = bb[loc[s], at, lanes(t)] - centre_tile * w
                pre = z - centre_tile * y
                image = w - centre_tile * v
                for n, term in enumerate((res * pre, w * y, pre * image, y * v, z * v)):
                    terms[n].append(term)
        return tuple(a + tree(b) for a, b in zip(acc, terms))

    for s in range(D):
        for t in range(nt):
            yb[s, t, rows + T : rows + 2 * T, :] = zero
            qyb[s, t, 0:T, :] = zero

    def whole(i):
        r = i * T
        return [(r, t) for t in range(nt)]

    acc = lax.fori_loop(0, ni, lambda i, c: apply_y(whole(i), c), (zero,) * 5)
    halo_wait(y_copies, 1)

    def edge_sums(stage):
        cols_part = tree([zcol_out[stage, n] * zcol_in[1, 1 - n] for n in range(2)])
        rows_part = tree([zrow_out[stage, n, s] * zrow_in[1, 1 - n, s] for n in range(2) for s in range(D)])
        return down(cols_part) + down(rows_part)

    edge_y, edge_z = edge_sums(1), edge_sums(0)
    acc = tuple(down(a) for a in acc)
    acc = (acc[0], acc[1], acc[2] + centre * (edge_z - centre * edge_y), acc[3] - edge_y, acc[4] - edge_z)

    s0, s2, t0, t2, zv, rho_own, curve_own = (
        full(value) for value in acc + (rho_inner + rho_edge, curve_inner + curve_edge)
    )
    total_out[...] = line([
        s0, 2.0 * (curve_own - centre * s2), s2,
        t0, s2 + zv - 2.0 * centre * t2, t2,
        rho_own, curve_own, centre,
    ])
    mine = table_ref.at[pl.ds((layer * pxs + px) * pys + py, 1), :]
    pz = 4 if pxs % 4 == 0 else pxs
    px_hi = pxs // pz
    there = [
        (a, x, z, y) for a in range(layers) for x in range(px_hi) for z in range(pz) for y in range(pys)
    ]
    ring = lambda d, n: min(d, n - d)
    there.sort(key=lambda o: -(ring(o[1], px_hi) + ring(o[2], pz) + ring(o[3], pys)))
    for a, x, z, y in there:
        if a or x or z or y:
            peer = {
                "layer": lax.rem(layer + a, layers),
                "px": lax.rem(px // pz + x, px_hi) * pz + lax.rem(lax.rem(px, pz) + z, pz),
                "py": lax.rem(py + y, pys),
            }
            remote(total_out, mine, p_recv, peer, out_sem.at[1]).start()
    pltpu.make_async_copy(total_out, mine, p_recv).start()
    for s in range(D):
        for t in range(nt):
            v_ref[s, 0:1, lanes(t)] = v_ref[s, 0:1, lanes(t)] - zrow_in[1, 1, s, t : t + 1, :]
            v_ref[s, rows - 1 : rows, lanes(t)] = (
                v_ref[s, rows - 1 : rows, lanes(t)] - row_out[s, t : t + 1, :] * zrow_in[1, 0, s, t : t + 1, :]
            )
    right_part = col_out[...] * zcol_in[1, 0]
    left_part = zcol_in[1, 1]

    def mend(i, carry):
        at = tile_at(i * T)
        for s in range(D):
            k = s * ni + i
            first, final = lanes(0), lanes(nt - 1)
            v_ref[s, at, first] = v_ref[s, at, first] - jnp.where(lane == 0, spread(left_part, k, 0), 0.0)
            v_ref[s, at, final] = v_ref[s, at, final] - jnp.where(lane == W - 1, spread(right_part, k, W - 1), 0.0)
        return carry

    lax.fori_loop(0, ni, mend, 0)
    pltpu.make_async_copy(table_ref, table_ref, p_recv).wait()
    table = table_ref[...]
    table_lane = lax.broadcasted_iota(jnp.int32, table.shape, 1)
    centres = jnp.sum(jnp.where(table_lane == 8, table, 0.0), axis=1, keepdims=True)
    plain = jnp.sum(table, axis=0, keepdims=True)
    rho, curve_first = pick(plain, 6), pick(plain, 7)
    alpha = rho / curve_first
    delta = alpha - centres
    linear = (table_lane == 1) | (table_lane == 4)
    square = (table_lane == 2) | (table_lane == 5)
    powers = jnp.where(linear, -delta, jnp.where(square, delta * delta, 1.0))
    moved = jnp.sum(table * powers, axis=0, keepdims=True)
    rho_next = jnp.sum(jnp.where(row_lane < 3, moved, 0.0), axis=1, keepdims=True)
    curve = jnp.sum(jnp.where((row_lane >= 3) & (row_lane < 6), moved, 0.0), axis=1, keepdims=True)
    beta = rho_next / rho
    alpha_next = rho_next / (curve - beta * rho_next / alpha)
    factors[0] = jnp.broadcast_to(alpha + alpha_next * (1.0 + beta), (T, W))
    factors[1] = jnp.broadcast_to(alpha * alpha_next, (T, W))
    for copy in sends:
        copy.wait_send()
    for condition, copy in gated:
        gate(condition, copy.wait_send)
    wait_rows(size1 - 1, out_sem.at[0])
    wait_rows(len(there) - 1, out_sem.at[1])

    @pl.when(bottom)
    def _():
        for copy in c3_copies:
            copy.wait_send()


def finish(shape, bb, zb, yb, w_ref, v_ref, factors, x_hbm, r_hbm, x_buf, r_buf, sem):
    rows, cols = shape
    layer = lax.axis_index("layer")
    loc = [s + layer * (D - 1 - 2 * s) for s in range(D)]
    big, small = factors[0], factors[1]
    stops = [0, T, rows // 4, rows // 2, 3 * rows // 4, rows]
    copies = []

    def body(i, carry):
        r = i * T
        at = pl.ds(pl.multiple_of(r, T), T)
        above = pl.ds(pl.multiple_of(r + T, T), T)
        for s in range(D):
            l = loc[s]
            for t in range(cols // W):
                col = slice(t * W, (t + 1) * W)
                x_buf[l, at, col] = big * zb[s, t, above, :] - small * yb[s, t, above, :]
                r_buf[l, at, col] = bb[l, at, col] - big * w_ref[s, at, col] + small * v_ref[s, at, col]
        return carry

    for c, (lo, hi) in enumerate(zip(stops, stops[1:])):
        if hi == lo:
            continue
        lax.fori_loop(lo // T, hi // T, body, 0)
        at = pl.ds(lo, hi - lo)
        for n, (src, dst) in enumerate(((x_buf, x_hbm), (r_buf, r_hbm))):
            copies.append(pltpu.make_async_copy(src.at[:, at, :], dst.at[:, at, :], sem.at[2 * c + n]))
            copies[-1].start()
    for copy in copies:
        copy.wait()


def solution(mesh):
    layers, pxs, pys = (mesh.shape[a] for a in ("layer", "px", "py"))
    spec = P("layer", "px", "py")

    def step(*args):
        depth, rows, cols = args[0].shape
        nt = cols // W
        block = (depth, rows, cols)
        padded = (depth, nt, rows + 2 * T, W)
        size1 = layers * pys
        dma = pltpu.SemaphoreType.DMA
        vmem = lambda *dims: pltpu.VMEM(dims, F32)
        scratch = [
            vmem(depth, rows + T, cols), vmem(*block), vmem(*block), pltpu.VMEM(block, jnp.int32), vmem(*block),
            vmem(*block), vmem(*block), vmem(*block), vmem(rows, cols), vmem(rows, cols), vmem(rows, cols),
            vmem(*padded), vmem(*padded),
            vmem(2, rows, cols), vmem(2, rows, cols), vmem(rows, cols), vmem(rows, cols),
            vmem(depth, nt, W), vmem(depth, nt, W), vmem(T, W), vmem(T, W),
            vmem(2, 2, depth, nt, W), vmem(2, 2, depth, nt, W), vmem(2, 2, T, W), vmem(2, 2, T, W),
            vmem(1, 1, W), vmem(size1, 1, W), vmem(1, W), vmem(size1 * pxs, W), vmem(size1 * pxs, 1, W),
            dma((4,)), dma((8,)), dma((11,)), dma, dma, pltpu.SemaphoreType.REGULAR((4,)),
        ]
        out = lambda *dims: jax.ShapeDtypeStruct(dims, F32)
        in_vmem = pl.BlockSpec(memory_space=pltpu.VMEM)
        in_hbm = pl.BlockSpec(memory_space=pltpu.HBM)
        kept = pl.pallas_call(
            functools.partial(kernel, (rows, cols), (layers, pxs, pys)),
            out_shape=(vmem(*block), vmem(*padded), vmem(*padded), vmem(*block), vmem(*block), vmem(2, T, W)),
            in_specs=[in_hbm] * 6,
            out_specs=(in_vmem,) * 6,
            scratch_shapes=scratch,
            compiler_params=pltpu.CompilerParams(
                collective_id=0, has_side_effects=True, vmem_limit_bytes=36 * 2**20
            ),
        )(*(pltpu.with_memory_space_constraint(arg, pltpu.HBM) for arg in args))
        return pl.pallas_call(
            functools.partial(finish, (rows, cols)),
            out_shape=(out(*block), out(*block)),
            in_specs=[in_vmem] * 6,
            out_specs=(in_hbm, in_hbm),
            scratch_shapes=[vmem(*block), vmem(*block), dma((10,))],
            compiler_params=pltpu.CompilerParams(vmem_limit_bytes=6 * 2**20),
        )(*kept)

    return jax.shard_map(step, mesh=mesh, in_specs=(spec,) * 6, out_specs=(spec, spec), check_vma=False)
```

```python
import functools

import jax
import jax.numpy as jnp
from jax import lax
from jax.experimental import pallas as pl
from jax.experimental.pallas import tpu as pltpu
from jax.sharding import PartitionSpec as P

MESH = pl.DeviceIdType.MESH
F32 = jnp.float32
D = 4
T = 8
W = 128


def kernel(shape, counts, *refs):
    dma = pltpu.SemaphoreType.DMA
    pl.run_scoped(functools.partial(solve_all, shape, counts, *refs), dma((28,)), dma((32,)))


def solve_all(
    shape, counts,
    b_hbm, rw_hbm, cl_hbm, vi_hbm, mk_hbm, gd_hbm,
    bb, zb, yb, w_ref, v_ref, factors,
    rwp, cl, vi, mk, gd, inv, gain, num, c3, q3a, q3b,
    qb, qyb, fg_out, fg_in, f_out, f_in,
    row_out, row_in, col_out, col_in,
    zrow_out, zrow_in, zcol_out, zcol_in,
    part, group, total_out, table_ref, sized,
    s_recv, z_recv, m_recv, g_recv, p_recv, far_sem, met_sem,
    load_sem, out_sem,
):
    rows, cols = shape
    layers, pxs, pys = counts
    nt = cols // W
    ni = rows // T
    layer = lax.axis_index("layer")
    px = lax.axis_index("px")
    py = lax.axis_index("py")
    bottom = layer == 0
    loc = [s + layer * (D - 1 - 2 * s) for s in range(D)]
    via = [s + layer * (D - 2 - 2 * s) for s in range(D - 1)]
    size1 = layers * pys
    me1 = layer * pys + py

    def group_peer(d):
        other = lax.rem(me1 + d, size1)
        return {"layer": other // pys, "py": lax.rem(other, pys)}

    def px_peer(d):
        return {"px": lax.rem(px + d, pxs)}

    def py_peer(d):
        return {"py": lax.rem(py + d, pys)}

    partner = {"layer": 1 - layer}
    near = [partner, px_peer(1), px_peer(pxs - 1), py_peer(1), py_peer(pys - 1)]

    barrier = pltpu.get_barrier_semaphore()
    for peer in near:
        pl.semaphore_signal(barrier, inc=1, device_id=peer, device_id_type=MESH)
    has_upper, has_lower = px > 0, px < pxs - 1
    has_left, has_right = py > 0, py < pys - 1

    slot = [0]

    def load(src, dst):
        copy = pltpu.make_async_copy(src, dst, load_sem.at[slot[0]])
        slot[0] += 1
        return copy

    last = (nt - 1) * W
    cl_edge = load(cl_hbm.at[:, :, last : last + W], cl.at[:, :, last : last + W])
    rw_edge = load(rw_hbm.at[:, rows - T : rows, :], rwp.at[:, rows : rows + T, :])
    top_loads = [load(vi_hbm.at[D - 1], vi.at[D - 1]), load(mk_hbm.at[D - 1], mk.at[D - 1])]
    cl_edge.start()
    rw_edge.start()

    @pl.when(bottom)
    def _():
        for copy in top_loads:
            copy.start()

    chunks = 4
    step = rows // chunks
    chunk_loads = []
    for c in range(chunks):
        at = pl.ds(c * step, step)
        short = step - T if c == chunks - 1 else step
        chunk_loads.append([
            load(rw_hbm.at[:, pl.ds(c * step, short), :], rwp.at[:, pl.ds(T + c * step, short), :]),
            load(cl_hbm.at[:, at, 0:last], cl.at[:, at, 0:last]),
            load(vi_hbm.at[0 : D - 1, at, :], vi.at[0 : D - 1, at, :]),
            load(mk_hbm.at[0 : D - 1, at, :], mk.at[0 : D - 1, at, :]),
            load(gd_hbm.at[:, at, :], gd.at[:, at, :]),
            load(b_hbm.at[:, at, :], bb.at[:, at, :]),
        ])
        for copy in chunk_loads[-1]:
            copy.start()

    lane = lax.broadcasted_iota(jnp.int32, (T, W), 1)
    sub = lax.broadcasted_iota(jnp.int32, (T, W), 0)
    zero = jnp.zeros((T, W), F32)

    def gate(condition, *actions):
        @pl.when(condition)
        def _():
            for action in actions:
                action()

    out_slot = [2]

    def remote(src, dst, recv, peer, send=None):
        if send is None:
            send = out_sem.at[out_slot[0]]
            out_slot[0] += 1
        return pltpu.make_async_remote_copy(
            src_ref=src, dst_ref=dst, send_sem=send, recv_sem=recv,
            device_id=peer, device_id_type=MESH,
        )

    def wait_rows(count, sem):
        pltpu.make_async_copy(sized.at[0:count], sized.at[0:count], sem).wait()

    def lanes(t):
        return slice(t * W, (t + 1) * W)

    def tile_at(r):
        return pl.ds(pl.multiple_of(r, T), T)

    cl_edge.wait()
    packs = []
    for s in range(D):
        packed = zero
        for i in range(ni):
            k = s * ni + i
            value = cl[loc[s], i * T : (i + 1) * T, lanes(nt - 1)]
            packed = jnp.where(lane == k, pltpu.roll(value, (k + 1) % W, axis=1), packed)
        packs.append(packed)
    col_out[...] = (packs[0] + packs[1]) + (packs[2] + packs[3])
    rw_edge.wait()
    for s in range(D):
        for t in range(nt):
            row_out[s, t : t + 1, :] = rwp[loc[s], rows + T - 1 : rows + T, lanes(t)]

    pl.semaphore_wait(barrier, len(near))
    row_copy = remote(row_out, row_in, s_recv.at[0], px_peer(1))
    col_copy = remote(col_out, col_in, s_recv.at[1], py_peer(1))
    gate(has_right, col_copy.start)
    gate(has_lower, row_copy.start)
    for peer in near:
        pl.semaphore_signal(far_sem.at[0], inc=1, device_id=peer, device_id_type=MESH)
    pieces = chunks
    piece = rows // pieces
    c3_copies = [
        remote(c3.at[pl.ds(c * piece, piece)], c3.at[pl.ds(c * piece, piece)], s_recv.at[2 + c], partner)
        for c in range(pieces)
    ]

    def join(i, carry):
        at = tile_at(i * T)
        c3[at, :] = vi[D - 1, at, :] * mk[D - 1, at, :].astype(F32)
        return carry

    @pl.when(bottom)
    def _():
        for copy in top_loads:
            copy.wait()
        for c in range(pieces):
            lax.fori_loop(c * piece // T, (c + 1) * piece // T, join, 0)
            c3_copies[c].start()

    gated = [(has_lower, row_copy), (has_right, col_copy)]
    sends = []

    hops = []
    while (2 << len(hops)) < pxs // 2:
        hops.append(2 << len(hops))

    def greet(n):
        if n < len(hops):
            for d in (hops[n], pxs - hops[n]):
                pl.semaphore_signal(far_sem.at[1 + n], inc=1, device_id=px_peer(d), device_id_type=MESH)

    def greeted(n):
        if n < len(hops):
            pl.semaphore_wait(far_sem.at[1 + n], 2)

    def inner(i):
        r = i * T
        return [(r, t) for t in range(1, nt - 1)]

    def sides(j):
        starts = [j * 4 * T + m * T for m in range(4)]
        return [(r, t) for r in starts for t in (0, nt - 1)]

    def ends(j):
        r = j * (rows - T)
        return [(r, t) for t in range(1, nt - 1)]

    def edge_work(body, carry):
        carry = lax.fori_loop(0, ni // 4, lambda j, c: body(sides(j), c), carry)
        return lax.fori_loop(0, 2, lambda j, c: body(ends(j), c), carry)

    def inner_work(body, carry, start=1, stop=None):
        stop = ni - 1 if stop is None else stop
        return lax.fori_loop(start, stop, lambda i, c: body(inner(i), c), carry)

    def spread(packed, k, to):
        return pltpu.roll(packed, lax.rem(to + W - k, W), axis=1)

    def coupling(s, at, t):
        return vi[via[s], at, lanes(t)] * mk[via[s], at, lanes(t)].astype(F32)

    def factor(items, carry):
        g = [None] * len(items)
        n = [None] * len(items)
        below = [None] * len(items)
        for s in range(D):
            l = loc[s]
            for m, (r, t) in enumerate(items):
                at = tile_at(r)
                rw = rwp[l, tile_at(r + T), lanes(t)]
                before = rwp[l, at, lanes(t)]
                up = pltpu.roll(jnp.where(sub == T - 1, before, rw), 1, axis=0)
                c = cl[l, at, lanes(t)]
                if t == 0:
                    k = s * ni + r // T
                    left = jnp.where(lane == 0, spread(col_in[...], k, 0), pltpu.roll(c, 1, axis=1))
                else:
                    left = pltpu.roll(jnp.where(lane == W - 1, cl[l, at, lanes(t - 1)], c), 1, axis=1)
                if s < D - 1:
                    above = coupling(s, at, t)
                else:
                    above = c3[at, lanes(t)]
                diagonal = gd[l, at, lanes(t)] + rw + up + c + left + above
                right_side = bb[l, at, lanes(t)]
                if s:
                    diagonal = diagonal + below[m]
                    inverse = 1.0 / (diagonal - below[m] * g[m])
                    n[m] = right_side + g[m] * n[m]
                else:
                    inverse = 1.0 / diagonal
                    n[m] = right_side
                below[m] = above
                g[m] = above * inverse
                inv[s, at, lanes(t)] = inverse
                gain[s, at, lanes(t)] = g[m]
                num[s, at, lanes(t)] = n[m]
                if s == D - 1:
                    fg_out[0, at, lanes(t)] = n[m] * inverse
                    fg_out[1, at, lanes(t)] = g[m]
        return carry

    regions = [
        (pl.ds(T, rows - 2 * T), pl.ds(W, cols - 2 * W)),
        (pl.ds(0, rows), pl.ds(0, W)),
        (pl.ds(0, rows), pl.ds(cols - W, W)),
        (pl.ds(0, T), pl.ds(W, cols - 2 * W)),
        (pl.ds(rows - T, T), pl.ds(W, cols - 2 * W)),
    ]

    def middle(out, into, which, base):
        copies = []
        for e, (i, j) in enumerate(which):
            if len(out.shape) == 3:
                src, dst = out.at[:, i, j], into.at[:, i, j]
            else:
                src, dst = out.at[i, j], into.at[i, j]
            copies.append(remote(src, dst, m_recv.at[base + e], partner))
        for copy in copies:
            copy.start()
        sends.extend(copies)
        return copies

    def deep(i):
        r = i * T
        return [(r, t) for t in range(1, nt)]

    fg_inner = []
    for c in range(chunks):
        for copy in chunk_loads[c]:
            copy.wait()
        gate(jnp.logical_not(bottom), c3_copies[c].wait_recv)
        lo, hi = max(T, c * step), (c + 1) * step
        lax.fori_loop(lo // T, hi // T, lambda i, x: factor(deep(i), x), 0)
        fg_inner += middle(fg_out, fg_in, [(pl.ds(lo, hi - lo), pl.ds(W, cols - W))], c)

    pl.semaphore_wait(far_sem.at[0], len(near))
    greet(0)
    gate(has_left, col_copy.wait_recv)
    gate(has_upper, row_copy.wait_recv)
    for s in range(D):
        for t in range(nt):
            rwp[loc[s], T - 1 : T, lanes(t)] = jnp.where(has_upper, row_in[s, t : t + 1, :], 0.0)
    col_in[...] = jnp.where(has_left, col_in[...], 0.0)
    group_of = min(8, ni)
    lax.fori_loop(
        0, ni // group_of,
        lambda j, x: factor([(j * group_of * T + m * T, 0) for m in range(group_of)], x), 0,
    )
    lax.fori_loop(0, 1, lambda i, x: factor(deep(i), x), 0)
    fg_edge = middle(fg_out, fg_in, [(pl.ds(0, rows), pl.ds(0, W)), (pl.ds(0, T), pl.ds(W, cols - W))], 4)

    def solve(first, z, q, f_ref, items, carry):
        rho, pack_l, pack_r = carry
        following = [None] * len(items)
        terms = []
        for s in range(D - 1, -1, -1):
            l = loc[s]
            for m, (r, t) in enumerate(items):
                at = tile_at(r)
                if s == D - 1:
                    if first:
                        other = fg_in[1, at, lanes(t)]
                        g = gain[s, at, lanes(t)]
                        quotient = 1.0 / (1.0 - g * other)
                        scale = quotient * inv[s, at, lanes(t)]
                        g = quotient * g
                        q3a[at, lanes(t)] = scale
                        q3b[at, lanes(t)] = g
                        theirs = fg_in[0, at, lanes(t)]
                    else:
                        scale = q3a[at, lanes(t)]
                        g = q3b[at, lanes(t)]
                        theirs = f_ref[at, lanes(t)]
                    value = scale * num[s, at, lanes(t)] + g * theirs
                else:
                    value = num[s, at, lanes(t)] * inv[s, at, lanes(t)] + gain[s, at, lanes(t)] * following[m]
                following[m] = value
                z[s, t, tile_at(r + T), :] = value
                q[s, t, tile_at(r + T), :] = rwp[l, tile_at(r + T), lanes(t)] * value
                if first:
                    terms.append(bb[l, at, lanes(t)] * value)
                if t == 0:
                    k = s * ni + r // T
                    pack_l = jnp.where(lane == k, pltpu.roll(value, k, axis=1), pack_l)
                if t == nt - 1:
                    k = s * ni + r // T
                    side = cl[l, at, lanes(t)] * value
                    pack_r = jnp.where(lane == k, pltpu.roll(side, k + 1, axis=1), pack_r)
        if first:
            rho = rho + tree(terms)
        return rho, pack_l, pack_r

    def tree(values):
        while len(values) > 1:
            values = [a + b for a, b in zip(values[::2], values[1::2])] + ([values[-1]] if len(values) % 2 else [])
        return values[0]

    def halo_send(z, q, pack_l, pack_r, stage):
        zcol_out[stage, 0] = pack_l
        zcol_out[stage, 1] = pack_r
        for s in range(D):
            for t in range(nt):
                zrow_out[stage, 0, s, t : t + 1, :] = z[s, t, T : T + 1, :]
                zrow_out[stage, 1, s, t : t + 1, :] = q[s, t, rows + T - 1 : rows + T, :]
        copies = [
            remote(out, into, z_recv.at[4 * stage + n], peer)
            for n, (out, into, peer) in enumerate((
                (zcol_out.at[stage, 0], zcol_in.at[stage, 0], py_peer(pys - 1)),
                (zcol_out.at[stage, 1], zcol_in.at[stage, 1], py_peer(1)),
                (zrow_out.at[stage, 0], zrow_in.at[stage, 0], px_peer(pxs - 1)),
                (zrow_out.at[stage, 1], zrow_in.at[stage, 1], px_peer(1)),
            ))
        ]
        for condition, copy in zip((has_upper, has_lower, has_left, has_right), copies[2:] + copies[:2]):
            gate(condition, copy.start)
            gated.append((condition, copy))
        return copies

    def halo_wait(copies, stage):
        for condition, copy in zip((has_right, has_left, has_lower, has_upper), copies):
            gate(condition, copy.wait_recv)
        zcol_in[stage, 0] = jnp.where(has_right, zcol_in[stage, 0], 0.0)
        zcol_in[stage, 1] = jnp.where(has_left, zcol_in[stage, 1], 0.0)
        zrow_in[stage, 0] = jnp.where(has_lower, zrow_in[stage, 0], 0.0)
        zrow_in[stage, 1] = jnp.where(has_upper, zrow_in[stage, 1], 0.0)

    def place_rows(z, q, stage):
        for s in range(D):
            for t in range(nt):
                z[s, t, rows + T : rows + T + 1, :] = zrow_in[stage, 0, s, t : t + 1, :]
                q[s, t, T - 1 : T, :] = zrow_in[stage, 1, s, t : t + 1, :]

    solve_z = functools.partial(solve, True, zb, qb, None)
    for copy in fg_inner:
        copy.wait_recv()
    rho_inner = inner_work(solve_z, (zero, zero, zero))[0]
    for copy in fg_edge:
        copy.wait_recv()
    rho_edge, pack_l, pack_r = edge_work(solve_z, (zero, zero, zero))
    z_copies = halo_send(zb, qb, pack_l, pack_r, 0)

    def coupled(z, q, stage, s, items):
        l = loc[s]
        zs, ps, out = {}, {}, []

        def own(m, r, t):
            if (m, t) not in zs:
                zs[m, t] = z[s, t, tile_at(r + T), :]
            return zs[m, t]

        def product(m, r, t):
            if (m, t) not in ps:
                ps[m, t] = cl[l, tile_at(r), lanes(t)] * own(m, r, t)
            return ps[m, t]

        rows_seen = []
        for r, t in items:
            m = next((n for n, other in enumerate(rows_seen) if other is r), None)
            if m is None:
                rows_seen.append(r)
                m = len(rows_seen) - 1
            at = tile_at(r)
            value = own(m, r, t)
            down = z[s, t, pl.ds(r + T + 1, T), :]
            up = q[s, t, pl.ds(r + T - 1, T), :]
            k = s * ni + r // T
            if t == nt - 1 and stage is None:
                right = pltpu.roll(jnp.where(lane == 0, 0.0, value), W - 1, axis=1)
            elif t == nt - 1:
                right = jnp.where(lane == W - 1, spread(zcol_in[stage, 0], k, W - 1), pltpu.roll(value, W - 1, axis=1))
            else:
                right = pltpu.roll(jnp.where(lane == 0, own(m, r, t + 1), value), W - 1, axis=1)
            if t == 0 and stage is None:
                left = pltpu.roll(jnp.where(lane == W - 1, 0.0, product(m, r, t)), 1, axis=1)
            elif t == 0:
                left = jnp.where(lane == 0, spread(zcol_in[stage, 1], k, 0), pltpu.roll(product(m, r, t), 1, axis=1))
            else:
                left = pltpu.roll(jnp.where(lane == W - 1, product(m, r, t - 1), product(m, r, t)), 1, axis=1)
            rw = rwp[l, tile_at(r + T), lanes(t)]
            c = cl[l, at, lanes(t)]
            out.append((value, rw * down + up + (c * right + left)))
        return out

    def apply_z(items, curve):
        n = [None] * len(items)
        terms = []
        for s in range(D):
            for m, ((r, t), (value, h)) in enumerate(zip(items, coupled(zb, qb, 0, s, items))):
                at = tile_at(r)
                w = bb[loc[s], at, lanes(t)] - h
                w_ref[s, at, lanes(t)] = w
                terms.append(value * w)
                n[m] = w if s == 0 else w + gain[s - 1, at, lanes(t)] * n[m]
                num[s, at, lanes(t)] = n[m]
                if s == D - 1:
                    f_out[at, lanes(t)] = n[m] * inv[s, at, lanes(t)]
        return curve + tree(terms)

    def down(value):
        return jnp.sum(value, axis=0, keepdims=True)

    def full(value):
        return jnp.sum(down(value), axis=1, keepdims=True)

    row_lane = lax.broadcasted_iota(jnp.int32, (1, W), 1)

    def line(values):
        out = jnp.zeros((1, W), F32)
        for n, value in enumerate(values):
            out = jnp.where(row_lane == n, value, out)
        return out

    def gather_group(values):
        part[0] = line(values)
        group[pl.ds(me1, 1)] = line(values)[None]
        for d in range(1, size1):
            remote(part.at[0], group.at[me1], g_recv, group_peer(d), out_sem.at[0]).start()

    def group_sum():
        wait_rows(size1 - 1, g_recv)
        return tree([group[m] for m in range(size1)])

    curve_inner = inner_work(apply_z, zero)
    f_inner = middle(f_out, f_in, regions[:1], 6)
    greeted(0)
    greet(1)
    gather_group([full(rho_inner), full(curve_inner)])
    halo_wait(z_copies, 0)
    place_rows(zb, qb, 0)

    curve_edge = edge_work(apply_z, zero)
    f_edge = middle(f_out, f_in, regions[1:], 7)
    for n in range(1, len(hops)):
        greeted(n)
        greet(n + 1)
    for d in range(1, size1):
        pl.semaphore_signal(met_sem, inc=1, device_id=group_peer(d), device_id_type=MESH)

    solve_y = functools.partial(solve, False, yb, qyb, f_in)
    carry = (zero, zero, zero)
    for copy in f_inner:
        copy.wait_recv()
    carry = inner_work(solve_y, carry)
    for copy in f_edge:
        copy.wait_recv()
    carry = edge_work(solve_y, carry)
    y_copies = halo_send(yb, qyb, carry[1], carry[2], 1)

    sums = group_sum()

    def pick(value, n):
        return jnp.sum(jnp.where(row_lane == n, value, 0.0), axis=1, keepdims=True)

    rho_group, curve_group = pick(sums, 0), pick(sums, 1)
    ok = (rho_group > 0.0) & (curve_group > 0.0)
    centre = jnp.where(ok, rho_group / jnp.where(ok, curve_group, 1.0), 1.0)
    centre_tile = jnp.broadcast_to(centre, (T, W))

    def apply_y(items, acc):
        terms = [[] for _ in acc]
        for s in range(D):
            for (r, t), (y, h) in zip(items, coupled(yb, qyb, None, s, items)):
                at = tile_at(r)
                w = w_ref[s, at, lanes(t)]
                v = w - h
                v_ref[s, at, lanes(t)] = v
                z = zb[s, t, tile_at(r + T), :]
                res = bb[loc[s], at, lanes(t)] - centre_tile * w
                pre = z - centre_tile * y
                image = w - centre_tile * v
                for n, term in enumerate((res * pre, w * y, pre * image, y * v, z * v)):
                    terms[n].append(term)
        return tuple(a + tree(b) for a, b in zip(acc, terms))

    for s in range(D):
        for t in range(nt):
            yb[s, t, rows + T : rows + 2 * T, :] = zero
            qyb[s, t, 0:T, :] = zero

    def whole(i):
        r = i * T
        return [(r, t) for t in range(nt)]

    acc = lax.fori_loop(0, ni, lambda i, c: apply_y(whole(i), c), (zero,) * 5)
    halo_wait(y_copies, 1)

    def edge_sums(stage):
        cols_part = tree([zcol_out[stage, n] * zcol_in[1, 1 - n] for n in range(2)])
        rows_part = tree([zrow_out[stage, n, s] * zrow_in[1, 1 - n, s] for n in range(2) for s in range(D)])
        return down(cols_part) + down(rows_part)

    edge_y, edge_z = edge_sums(1), edge_sums(0)
    acc = tuple(down(a) for a in acc)
    acc = (acc[0], acc[1], acc[2] + centre * (edge_z - centre * edge_y), acc[3] - edge_y, acc[4] - edge_z)

    s0, s2, t0, t2, zv, rho_own, curve_own = (
        full(value) for value in acc + (rho_inner + rho_edge, curve_inner + curve_edge)
    )
    total_out[...] = line([
        s0, 2.0 * (curve_own - centre * s2), s2,
        t0, s2 + zv - 2.0 * centre * t2, t2,
        rho_own, curve_own, centre,
    ])
    pl.semaphore_wait(met_sem, size1 - 1)
    mine = table_ref.at[pl.ds((layer * pxs + px) * pys + py, 1), :]
    pz = 4 if pxs % 4 == 0 else pxs
    px_hi = pxs // pz
    there = [
        (a, x, z, y) for a in range(layers) for x in range(px_hi) for z in range(pz) for y in range(pys)
    ]
    ring = lambda d, n: min(d, n - d)
    there.sort(key=lambda o: -(ring(o[1], px_hi) + ring(o[2], pz) + ring(o[3], pys)))
    for a, x, z, y in there:
        if a or x or z or y:
            peer = {
                "layer": lax.rem(layer + a, layers),
                "px": lax.rem(px // pz + x, px_hi) * pz + lax.rem(lax.rem(px, pz) + z, pz),
                "py": lax.rem(py + y, pys),
            }
            remote(total_out, mine, p_recv, peer, out_sem.at[1]).start()
    pltpu.make_async_copy(total_out, mine, p_recv).start()
    for s in range(D):
        for t in range(nt):
            v_ref[s, 0:1, lanes(t)] = v_ref[s, 0:1, lanes(t)] - zrow_in[1, 1, s, t : t + 1, :]
            v_ref[s, rows - 1 : rows, lanes(t)] = (
                v_ref[s, rows - 1 : rows, lanes(t)] - row_out[s, t : t + 1, :] * zrow_in[1, 0, s, t : t + 1, :]
            )
    right_part = col_out[...] * zcol_in[1, 0]
    left_part = zcol_in[1, 1]

    def mend(i, carry):
        at = tile_at(i * T)
        for s in range(D):
            k = s * ni + i
            first, final = lanes(0), lanes(nt - 1)
            v_ref[s, at, first] = v_ref[s, at, first] - jnp.where(lane == 0, spread(left_part, k, 0), 0.0)
            v_ref[s, at, final] = v_ref[s, at, final] - jnp.where(lane == W - 1, spread(right_part, k, W - 1), 0.0)
        return carry

    lax.fori_loop(0, ni, mend, 0)
    pltpu.make_async_copy(table_ref, table_ref, p_recv).wait()
    table = table_ref[...]
    table_lane = lax.broadcasted_iota(jnp.int32, table.shape, 1)
    centres = jnp.sum(jnp.where(table_lane == 8, table, 0.0), axis=1, keepdims=True)
    plain = jnp.sum(table, axis=0, keepdims=True)
    rho, curve_first = pick(plain, 6), pick(plain, 7)
    alpha = rho / curve_first
    delta = alpha - centres
    linear = (table_lane == 1) | (table_lane == 4)
    square = (table_lane == 2) | (table_lane == 5)
    powers = jnp.where(linear, -delta, jnp.where(square, delta * delta, 1.0))
    moved = jnp.sum(table * powers, axis=0, keepdims=True)
    rho_next = jnp.sum(jnp.where(row_lane < 3, moved, 0.0), axis=1, keepdims=True)
    curve = jnp.sum(jnp.where((row_lane >= 3) & (row_lane < 6), moved, 0.0), axis=1, keepdims=True)
    beta = rho_next / rho
    alpha_next = rho_next / (curve - beta * rho_next / alpha)
    factors[0] = jnp.broadcast_to(alpha + alpha_next * (1.0 + beta), (T, W))
    factors[1] = jnp.broadcast_to(alpha * alpha_next, (T, W))
    for copy in sends:
        copy.wait_send()
    for condition, copy in gated:
        gate(condition, copy.wait_send)
    wait_rows(size1 - 1, out_sem.at[0])
    wait_rows(len(there) - 1, out_sem.at[1])

    @pl.when(bottom)
    def _():
        for copy in c3_copies:
            copy.wait_send()


def finish(shape, bb, zb, yb, w_ref, v_ref, factors, x_hbm, r_hbm, x_buf, r_buf, sem):
    rows, cols = shape
    layer = lax.axis_index("layer")
    loc = [s + layer * (D - 1 - 2 * s) for s in range(D)]
    big, small = factors[0], factors[1]
    stops = [0, T, rows // 4, rows // 2, 3 * rows // 4, rows]
    copies = []

    def body(i, carry):
        r = i * T
        at = pl.ds(pl.multiple_of(r, T), T)
        above = pl.ds(pl.multiple_of(r + T, T), T)
        for s in range(D):
            l = loc[s]
            for t in range(cols // W):
                col = slice(t * W, (t + 1) * W)
                x_buf[l, at, col] = big * zb[s, t, above, :] - small * yb[s, t, above, :]
                r_buf[l, at, col] = bb[l, at, col] - big * w_ref[s, at, col] + small * v_ref[s, at, col]
        return carry

    for c, (lo, hi) in enumerate(zip(stops, stops[1:])):
        if hi == lo:
            continue
        lax.fori_loop(lo // T, hi // T, body, 0)
        at = pl.ds(lo, hi - lo)
        for n, (src, dst) in enumerate(((x_buf, x_hbm), (r_buf, r_hbm))):
            copies.append(pltpu.make_async_copy(src.at[:, at, :], dst.at[:, at, :], sem.at[2 * c + n]))
            copies[-1].start()
    for copy in copies:
        copy.wait()


def solution(mesh):
    layers, pxs, pys = (mesh.shape[a] for a in ("layer", "px", "py"))
    spec = P("layer", "px", "py")

    def step(*args):
        depth, rows, cols = args[0].shape
        nt = cols // W
        block = (depth, rows, cols)
        padded = (depth, nt, rows + 2 * T, W)
        size1 = layers * pys
        dma = pltpu.SemaphoreType.DMA
        vmem = lambda *dims: pltpu.VMEM(dims, F32)
        scratch = [
            vmem(depth, rows + T, cols), vmem(*block), vmem(*block), pltpu.VMEM(block, jnp.int32), vmem(*block),
            vmem(*block), vmem(*block), vmem(*block), vmem(rows, cols), vmem(rows, cols), vmem(rows, cols),
            vmem(*padded), vmem(*padded),
            vmem(2, rows, cols), vmem(2, rows, cols), vmem(rows, cols), vmem(rows, cols),
            vmem(depth, nt, W), vmem(depth, nt, W), vmem(T, W), vmem(T, W),
            vmem(2, 2, depth, nt, W), vmem(2, 2, depth, nt, W), vmem(2, 2, T, W), vmem(2, 2, T, W),
            vmem(1, 1, W), vmem(size1, 1, W), vmem(1, W), vmem(size1 * pxs, W), vmem(size1 * pxs, 1, W),
            dma((6,)), dma((8,)), dma((11,)), dma, dma, pltpu.SemaphoreType.REGULAR((4,)), pltpu.SemaphoreType.REGULAR,
        ]
        out = lambda *dims: jax.ShapeDtypeStruct(dims, F32)
        in_vmem = pl.BlockSpec(memory_space=pltpu.VMEM)
        in_hbm = pl.BlockSpec(memory_space=pltpu.HBM)
        kept = pl.pallas_call(
            functools.partial(kernel, (rows, cols), (layers, pxs, pys)),
            out_shape=(vmem(*block), vmem(*padded), vmem(*padded), vmem(*block), vmem(*block), vmem(2, T, W)),
            in_specs=[in_hbm] * 6,
            out_specs=(in_vmem,) * 6,
            scratch_shapes=scratch,
            compiler_params=pltpu.CompilerParams(
                collective_id=0, has_side_effects=True, vmem_limit_bytes=36 * 2**20
            ),
        )(*(pltpu.with_memory_space_constraint(arg, pltpu.HBM) for arg in args))
        return pl.pallas_call(
            functools.partial(finish, (rows, cols)),
            out_shape=(out(*block), out(*block)),
            in_specs=[in_vmem] * 6,
            out_specs=(in_hbm, in_hbm),
            scratch_shapes=[vmem(*block), vmem(*block), dma((10,))],
            compiler_params=pltpu.CompilerParams(vmem_limit_bytes=6 * 2**20),
        )(*kept)

    return jax.shard_map(step, mesh=mesh, in_specs=(spec,) * 6, out_specs=(spec, spec), check_vma=False)
```

```python
import functools

import jax
import jax.numpy as jnp
from jax import lax
from jax.experimental import pallas as pl
from jax.experimental.pallas import tpu as pltpu
from jax.sharding import PartitionSpec as P

MESH = pl.DeviceIdType.MESH
F32 = jnp.float32
D = 4
T = 8
W = 128


def kernel(shape, counts, *refs):
    dma = pltpu.SemaphoreType.DMA
    pl.run_scoped(functools.partial(solve_all, shape, counts, *refs), dma((28,)), dma((32,)))


def solve_all(
    shape, counts,
    b_hbm, rw_hbm, cl_hbm, vi_hbm, mk_hbm, gd_hbm,
    bb, zb, yb, w_ref, v_ref, factors,
    rwp, cl, vi, mk, gd, inv, gain, num, c3, q3a, q3b,
    qb, qyb, fg_out, fg_in, f_out, f_in,
    row_out, row_in, col_out, col_in,
    zrow_out, zrow_in, zcol_out, zcol_in,
    part, group, total_out, table_ref, sized,
    s_recv, z_recv, m_recv, g_recv, p_recv, far_sem, met_sem,
    load_sem, out_sem,
):
    rows, cols = shape
    layers, pxs, pys = counts
    nt = cols // W
    ni = rows // T
    layer = lax.axis_index("layer")
    px = lax.axis_index("px")
    py = lax.axis_index("py")
    bottom = layer == 0
    loc = [s + layer * (D - 1 - 2 * s) for s in range(D)]
    via = [s + layer * (D - 2 - 2 * s) for s in range(D - 1)]
    size1 = layers * pys
    me1 = layer * pys + py

    def group_peer(d):
        other = lax.rem(me1 + d, size1)
        return {"layer": other // pys, "py": lax.rem(other, pys)}

    def px_peer(d):
        return {"px": lax.rem(px + d, pxs)}

    def py_peer(d):
        return {"py": lax.rem(py + d, pys)}

    partner = {"layer": 1 - layer}
    near = [partner, px_peer(1), px_peer(pxs - 1), py_peer(1), py_peer(pys - 1)]

    barrier = pltpu.get_barrier_semaphore()
    for peer in near:
        pl.semaphore_signal(barrier, inc=1, device_id=peer, device_id_type=MESH)
    has_upper, has_lower = px > 0, px < pxs - 1
    has_left, has_right = py > 0, py < pys - 1

    slot = [0]

    def load(src, dst):
        copy = pltpu.make_async_copy(src, dst, load_sem.at[slot[0]])
        slot[0] += 1
        return copy

    last = (nt - 1) * W
    cl_edge = load(cl_hbm.at[:, :, last : last + W], cl.at[:, :, last : last + W])
    rw_edge = load(rw_hbm.at[:, rows - T : rows, :], rwp.at[:, rows : rows + T, :])
    top_loads = [load(vi_hbm.at[D - 1], vi.at[D - 1]), load(mk_hbm.at[D - 1], mk.at[D - 1])]
    cl_edge.start()
    rw_edge.start()

    @pl.when(bottom)
    def _():
        for copy in top_loads:
            copy.start()

    chunks = 4
    step = rows // chunks
    chunk_loads = []
    for c in range(chunks):
        at = pl.ds(c * step, step)
        short = step - T if c == chunks - 1 else step
        chunk_loads.append([
            load(rw_hbm.at[:, pl.ds(c * step, short), :], rwp.at[:, pl.ds(T + c * step, short), :]),
            load(cl_hbm.at[:, at, 0:last], cl.at[:, at, 0:last]),
            load(vi_hbm.at[0 : D - 1, at, :], vi.at[0 : D - 1, at, :]),
            load(mk_hbm.at[0 : D - 1, at, :], mk.at[0 : D - 1, at, :]),
            load(gd_hbm.at[:, at, :], gd.at[:, at, :]),
            load(b_hbm.at[:, at, :], bb.at[:, at, :]),
        ])
        for copy in chunk_loads[-1]:
            copy.start()

    lane = lax.broadcasted_iota(jnp.int32, (T, W), 1)
    sub = lax.broadcasted_iota(jnp.int32, (T, W), 0)
    zero = jnp.zeros((T, W), F32)

    def gate(condition, *actions):
        @pl.when(condition)
        def _():
            for action in actions:
                action()

    out_slot = [2]

    def remote(src, dst, recv, peer, send=None):
        if send is None:
            send = out_sem.at[out_slot[0]]
            out_slot[0] += 1
        return pltpu.make_async_remote_copy(
            src_ref=src, dst_ref=dst, send_sem=send, recv_sem=recv,
            device_id=peer, device_id_type=MESH,
        )

    def wait_rows(count, sem):
        pltpu.make_async_copy(sized.at[0:count], sized.at[0:count], sem).wait()

    def lanes(t):
        return slice(t * W, (t + 1) * W)

    def tile_at(r):
        return pl.ds(pl.multiple_of(r, T), T)

    cl_edge.wait()
    packs = []
    for s in range(D):
        packed = zero
        for i in range(ni):
            k = s * ni + i
            value = cl[loc[s], i * T : (i + 1) * T, lanes(nt - 1)]
            packed = jnp.where(lane == k, pltpu.roll(value, (k + 1) % W, axis=1), packed)
        packs.append(packed)
    col_out[...] = (packs[0] + packs[1]) + (packs[2] + packs[3])
    rw_edge.wait()
    for s in range(D):
        for t in range(nt):
            row_out[s, t : t + 1, :] = rwp[loc[s], rows + T - 1 : rows + T, lanes(t)]

    pl.semaphore_wait(barrier, len(near))
    row_copy = remote(row_out, row_in, s_recv.at[0], px_peer(1))
    col_copy = remote(col_out, col_in, s_recv.at[1], py_peer(1))
    gate(has_right, col_copy.start)
    gate(has_lower, row_copy.start)
    for peer in near:
        pl.semaphore_signal(far_sem.at[0], inc=1, device_id=peer, device_id_type=MESH)
    pieces = chunks
    piece = rows // pieces
    c3_copies = [
        remote(c3.at[pl.ds(c * piece, piece)], c3.at[pl.ds(c * piece, piece)], s_recv.at[2 + c], partner)
        for c in range(pieces)
    ]

    def join(i, carry):
        at = tile_at(i * T)
        c3[at, :] = vi[D - 1, at, :] * mk[D - 1, at, :].astype(F32)
        return carry

    @pl.when(bottom)
    def _():
        for copy in top_loads:
            copy.wait()
        for c in range(pieces):
            lax.fori_loop(c * piece // T, (c + 1) * piece // T, join, 0)
            c3_copies[c].start()

    gated = [(has_lower, row_copy), (has_right, col_copy)]
    sends = []

    hops = []
    while (2 << len(hops)) < pxs // 2:
        hops.append(2 << len(hops))

    def greet(n):
        if n < len(hops):
            for d in (hops[n], pxs - hops[n]):
                pl.semaphore_signal(far_sem.at[1 + n], inc=1, device_id=px_peer(d), device_id_type=MESH)

    def greeted(n):
        if n < len(hops):
            pl.semaphore_wait(far_sem.at[1 + n], 2)

    def inner(i):
        r = i * T
        return [(r, t) for t in range(1, nt - 1)]

    span = 7 if (ni - 2) % 7 == 0 else 2

    def sides(j):
        starts = [(1 + j * span + m) * T for m in range(span)]
        return [(r, t) for r in starts for t in (0, nt - 1)]

    def ends(j):
        r = j * (rows - T)
        return [(r, t) for t in range(nt)]

    def ends_work(body, carry):
        return lax.fori_loop(0, 2, lambda j, c: body(ends(j), c), carry)

    def sides_work(body, carry):
        return lax.fori_loop(0, (ni - 2) // span, lambda j, c: body(sides(j), c), carry)

    def inner_work(body, carry, start=1, stop=None):
        stop = ni - 1 if stop is None else stop
        return lax.fori_loop(start, stop, lambda i, c: body(inner(i), c), carry)

    def spread(packed, k, to):
        return pltpu.roll(packed, lax.rem(to + W - k, W), axis=1)

    def coupling(s, at, t):
        return vi[via[s], at, lanes(t)] * mk[via[s], at, lanes(t)].astype(F32)

    def factor(items, carry):
        g = [None] * len(items)
        n = [None] * len(items)
        below = [None] * len(items)
        for s in range(D):
            l = loc[s]
            for m, (r, t) in enumerate(items):
                at = tile_at(r)
                rw = rwp[l, tile_at(r + T), lanes(t)]
                before = rwp[l, at, lanes(t)]
                up = pltpu.roll(jnp.where(sub == T - 1, before, rw), 1, axis=0)
                c = cl[l, at, lanes(t)]
                if t == 0:
                    k = s * ni + r // T
                    left = jnp.where(lane == 0, spread(col_in[...], k, 0), pltpu.roll(c, 1, axis=1))
                else:
                    left = pltpu.roll(jnp.where(lane == W - 1, cl[l, at, lanes(t - 1)], c), 1, axis=1)
                if s < D - 1:
                    above = coupling(s, at, t)
                else:
                    above = c3[at, lanes(t)]
                diagonal = gd[l, at, lanes(t)] + rw + up + c + left + above
                right_side = bb[l, at, lanes(t)]
                if s:
                    diagonal = diagonal + below[m]
                    inverse = 1.0 / (diagonal - below[m] * g[m])
                    n[m] = right_side + g[m] * n[m]
                else:
                    inverse = 1.0 / diagonal
                    n[m] = right_side
                below[m] = above
                g[m] = above * inverse
                inv[s, at, lanes(t)] = inverse
                gain[s, at, lanes(t)] = g[m]
                num[s, at, lanes(t)] = n[m]
                if s == D - 1:
                    fg_out[0, at, lanes(t)] = n[m] * inverse
                    fg_out[1, at, lanes(t)] = g[m]
        return carry

    regions = [
        (pl.ds(T, rows - 2 * T), pl.ds(W, cols - 2 * W)),
        (pl.ds(0, rows), pl.ds(0, W)),
        (pl.ds(0, rows), pl.ds(cols - W, W)),
        (pl.ds(0, T), pl.ds(W, cols - 2 * W)),
        (pl.ds(rows - T, T), pl.ds(W, cols - 2 * W)),
    ]

    def middle(out, into, which, base):
        copies = []
        for e, (i, j) in enumerate(which):
            if len(out.shape) == 3:
                src, dst = out.at[:, i, j], into.at[:, i, j]
            else:
                src, dst = out.at[i, j], into.at[i, j]
            copies.append(remote(src, dst, m_recv.at[base + e], partner))
        for copy in copies:
            copy.start()
        sends.extend(copies)
        return copies

    def deep(i):
        r = i * T
        return [(r, t) for t in range(1, nt)]

    fg_inner = []
    for c in range(chunks):
        for copy in chunk_loads[c]:
            copy.wait()
        gate(jnp.logical_not(bottom), c3_copies[c].wait_recv)
        lo, hi = max(T, c * step), (c + 1) * step
        lax.fori_loop(lo // T, hi // T, lambda i, x: factor(deep(i), x), 0)
        fg_inner += middle(fg_out, fg_in, [(pl.ds(lo, hi - lo), pl.ds(W, cols - W))], c)

    pl.semaphore_wait(far_sem.at[0], len(near))
    greet(0)
    gate(has_left, col_copy.wait_recv)
    gate(has_upper, row_copy.wait_recv)
    for s in range(D):
        for t in range(nt):
            rwp[loc[s], T - 1 : T, lanes(t)] = jnp.where(has_upper, row_in[s, t : t + 1, :], 0.0)
    col_in[...] = jnp.where(has_left, col_in[...], 0.0)
    group_of = min(8, ni)
    lax.fori_loop(
        0, ni // group_of,
        lambda j, x: factor([(j * group_of * T + m * T, 0) for m in range(group_of)], x), 0,
    )
    lax.fori_loop(0, 1, lambda i, x: factor(deep(i), x), 0)
    fg_edge = middle(fg_out, fg_in, [(pl.ds(0, rows), pl.ds(0, W)), (pl.ds(0, T), pl.ds(W, cols - W))], 4)

    def solve(first, z, q, f_ref, items, carry):
        rho, pack_l, pack_r = carry
        following = [None] * len(items)
        terms = []
        for s in range(D - 1, -1, -1):
            l = loc[s]
            for m, (r, t) in enumerate(items):
                at = tile_at(r)
                if s == D - 1:
                    if first:
                        other = fg_in[1, at, lanes(t)]
                        g = gain[s, at, lanes(t)]
                        quotient = 1.0 / (1.0 - g * other)
                        scale = quotient * inv[s, at, lanes(t)]
                        g = quotient * g
                        q3a[at, lanes(t)] = scale
                        q3b[at, lanes(t)] = g
                        theirs = fg_in[0, at, lanes(t)]
                    else:
                        scale = q3a[at, lanes(t)]
                        g = q3b[at, lanes(t)]
                        theirs = f_ref[at, lanes(t)]
                    value = scale * num[s, at, lanes(t)] + g * theirs
                else:
                    value = num[s, at, lanes(t)] * inv[s, at, lanes(t)] + gain[s, at, lanes(t)] * following[m]
                following[m] = value
                z[s, t, tile_at(r + T), :] = value
                q[s, t, tile_at(r + T), :] = rwp[l, tile_at(r + T), lanes(t)] * value
                if first:
                    terms.append(bb[l, at, lanes(t)] * value)
                if t == 0:
                    k = s * ni + r // T
                    pack_l = jnp.where(lane == k, pltpu.roll(value, k, axis=1), pack_l)
                if t == nt - 1:
                    k = s * ni + r // T
                    side = cl[l, at, lanes(t)] * value
                    pack_r = jnp.where(lane == k, pltpu.roll(side, k + 1, axis=1), pack_r)
        if first:
            rho = rho + tree(terms)
        return rho, pack_l, pack_r

    def tree(values):
        while len(values) > 1:
            values = [a + b for a, b in zip(values[::2], values[1::2])] + ([values[-1]] if len(values) % 2 else [])
        return values[0]

    def start_halos(stage, first, pairs):
        copies = []
        for n, (condition, out, into, peer) in enumerate(pairs):
            copy = remote(out, into, z_recv.at[4 * stage + first + n], peer)
            gate(condition, copy.start)
            gated.append((condition, copy))
            copies.append(copy)
        return copies

    def send_rows(z, q, stage):
        for s in range(D):
            for t in range(nt):
                zrow_out[stage, 0, s, t : t + 1, :] = z[s, t, T : T + 1, :]
                zrow_out[stage, 1, s, t : t + 1, :] = q[s, t, rows + T - 1 : rows + T, :]
        return start_halos(stage, 0, (
            (has_upper, zrow_out.at[stage, 0], zrow_in.at[stage, 0], px_peer(pxs - 1)),
            (has_lower, zrow_out.at[stage, 1], zrow_in.at[stage, 1], px_peer(1)),
        ))

    def send_cols(pack_l, pack_r, stage):
        zcol_out[stage, 0] = pack_l
        zcol_out[stage, 1] = pack_r
        return start_halos(stage, 2, (
            (has_left, zcol_out.at[stage, 0], zcol_in.at[stage, 0], py_peer(pys - 1)),
            (has_right, zcol_out.at[stage, 1], zcol_in.at[stage, 1], py_peer(1)),
        ))

    def halo_wait(copies, stage):
        for condition, copy in zip((has_lower, has_upper, has_right, has_left), copies):
            gate(condition, copy.wait_recv)
        zcol_in[stage, 0] = jnp.where(has_right, zcol_in[stage, 0], 0.0)
        zcol_in[stage, 1] = jnp.where(has_left, zcol_in[stage, 1], 0.0)
        zrow_in[stage, 0] = jnp.where(has_lower, zrow_in[stage, 0], 0.0)
        zrow_in[stage, 1] = jnp.where(has_upper, zrow_in[stage, 1], 0.0)

    def mend_rows(ref, stage):
        for s in range(D):
            for t in range(nt):
                ref[s, 0:1, lanes(t)] = ref[s, 0:1, lanes(t)] - zrow_in[stage, 1, s, t : t + 1, :]
                ref[s, rows - 1 : rows, lanes(t)] = (
                    ref[s, rows - 1 : rows, lanes(t)] - row_out[s, t : t + 1, :] * zrow_in[stage, 0, s, t : t + 1, :]
                )

    def col_term(left_part, right_part, k, t):
        if t == 0:
            return jnp.where(lane == 0, spread(left_part, k, 0), 0.0)
        return jnp.where(lane == W - 1, spread(right_part, k, W - 1), 0.0)

    for z, q in ((zb, qb), (yb, qyb)):
        for s in range(D):
            for t in range(nt):
                z[s, t, rows + T : rows + 2 * T, :] = zero
                q[s, t, 0:T, :] = zero

    solve_z = functools.partial(solve, True, zb, qb, None)
    for copy in fg_inner:
        copy.wait_recv()
    rho_inner = inner_work(solve_z, (zero, zero, zero))[0]
    for copy in fg_edge:
        copy.wait_recv()
    carry = ends_work(solve_z, (zero, zero, zero))
    z_copies = send_rows(zb, qb, 0)
    rho_edge, pack_l, pack_r = sides_work(solve_z, carry)
    z_copies += send_cols(pack_l, pack_r, 0)

    def coupled(z, q, s, items):
        l = loc[s]
        zs, ps, out = {}, {}, []

        def own(m, r, t):
            if (m, t) not in zs:
                zs[m, t] = z[s, t, tile_at(r + T), :]
            return zs[m, t]

        def product(m, r, t):
            if (m, t) not in ps:
                ps[m, t] = cl[l, tile_at(r), lanes(t)] * own(m, r, t)
            return ps[m, t]

        rows_seen = []
        for r, t in items:
            m = next((n for n, other in enumerate(rows_seen) if other is r), None)
            if m is None:
                rows_seen.append(r)
                m = len(rows_seen) - 1
            at = tile_at(r)
            value = own(m, r, t)
            down = z[s, t, pl.ds(r + T + 1, T), :]
            up = q[s, t, pl.ds(r + T - 1, T), :]
            after = own(m, r, t + 1) if t < nt - 1 else 0.0
            before = product(m, r, t - 1) if t else 0.0
            right = pltpu.roll(jnp.where(lane == 0, after, value), W - 1, axis=1)
            left = pltpu.roll(jnp.where(lane == W - 1, before, product(m, r, t)), 1, axis=1)
            rw = rwp[l, tile_at(r + T), lanes(t)]
            c = cl[l, at, lanes(t)]
            out.append((value, rw * down + up + (c * right + left)))
        return out

    def apply_z(items, curve):
        n = [None] * len(items)
        terms = []
        for s in range(D):
            for m, ((r, t), (value, h)) in enumerate(zip(items, coupled(zb, qb, s, items))):
                at = tile_at(r)
                w = bb[loc[s], at, lanes(t)] - h
                w_ref[s, at, lanes(t)] = w
                terms.append(value * w)
                n[m] = w if s == 0 else w + gain[s - 1, at, lanes(t)] * n[m]
                num[s, at, lanes(t)] = n[m]
                if s == D - 1:
                    f_out[at, lanes(t)] = n[m] * inv[s, at, lanes(t)]
        return curve + tree(terms)

    def start_edge(items, carry):
        for s in range(D):
            for (r, t), (_, h) in zip(items, coupled(zb, qb, s, items)):
                at = tile_at(r)
                w_ref[s, at, lanes(t)] = bb[loc[s], at, lanes(t)] - h
        return carry

    def end_edge(left_part, right_part, items, curve):
        n = [None] * len(items)
        terms = []
        for s in range(D):
            for m, (r, t) in enumerate(items):
                at = tile_at(r)
                w = w_ref[s, at, lanes(t)]
                if t in (0, nt - 1):
                    w = w - col_term(left_part, right_part, s * ni + r // T, t)
                    w_ref[s, at, lanes(t)] = w
                terms.append(zb[s, t, tile_at(r + T), :] * w)
                n[m] = w if s == 0 else w + gain[s - 1, at, lanes(t)] * n[m]
                num[s, at, lanes(t)] = n[m]
                if s == D - 1:
                    f_out[at, lanes(t)] = n[m] * inv[s, at, lanes(t)]
        return curve + tree(terms)

    def down(value):
        return jnp.sum(value, axis=0, keepdims=True)

    def full(value):
        return jnp.sum(down(value), axis=1, keepdims=True)

    row_lane = lax.broadcasted_iota(jnp.int32, (1, W), 1)

    def line(values):
        out = jnp.zeros((1, W), F32)
        for n, value in enumerate(values):
            out = jnp.where(row_lane == n, value, out)
        return out

    def gather_group(values):
        part[0] = line(values)
        group[pl.ds(me1, 1)] = line(values)[None]
        for d in range(1, size1):
            remote(part.at[0], group.at[me1], g_recv, group_peer(d), out_sem.at[0]).start()

    def group_sum():
        wait_rows(size1 - 1, g_recv)
        return tree([group[m] for m in range(size1)])

    curve_inner = inner_work(apply_z, zero)
    f_inner = middle(f_out, f_in, regions[:1], 6)
    greeted(0)
    greet(1)
    gather_group([full(rho_inner), full(curve_inner)])
    sides_work(start_edge, ends_work(start_edge, 0))
    halo_wait(z_copies, 0)
    mend_rows(w_ref, 0)
    end_z = functools.partial(end_edge, zcol_in[0, 1], col_out[...] * zcol_in[0, 0])

    curve_edge = sides_work(end_z, ends_work(end_z, zero))
    f_edge = middle(f_out, f_in, regions[1:], 7)
    for n in range(1, len(hops)):
        greeted(n)
        greet(n + 1)
    for d in range(1, size1):
        pl.semaphore_signal(met_sem, inc=1, device_id=group_peer(d), device_id_type=MESH)

    solve_y = functools.partial(solve, False, yb, qyb, f_in)
    carry = (zero, zero, zero)
    for copy in f_inner:
        copy.wait_recv()
    carry = inner_work(solve_y, carry)
    for copy in f_edge:
        copy.wait_recv()
    carry = ends_work(solve_y, carry)
    y_copies = send_rows(yb, qyb, 1)
    carry = sides_work(solve_y, carry)
    y_copies += send_cols(carry[1], carry[2], 1)

    sums = group_sum()

    def pick(value, n):
        return jnp.sum(jnp.where(row_lane == n, value, 0.0), axis=1, keepdims=True)

    rho_group, curve_group = pick(sums, 0), pick(sums, 1)
    ok = (rho_group > 0.0) & (curve_group > 0.0)
    centre = jnp.where(ok, rho_group / jnp.where(ok, curve_group, 1.0), 1.0)
    centre_tile = jnp.broadcast_to(centre, (T, W))

    def apply_y(items, acc):
        terms = [[] for _ in acc]
        for s in range(D):
            for (r, t), (y, h) in zip(items, coupled(yb, qyb, s, items)):
                at = tile_at(r)
                w = w_ref[s, at, lanes(t)]
                v = w - h
                v_ref[s, at, lanes(t)] = v
                z = zb[s, t, tile_at(r + T), :]
                res = bb[loc[s], at, lanes(t)] - centre_tile * w
                pre = z - centre_tile * y
                image = w - centre_tile * v
                for n, term in enumerate((res * pre, w * y, pre * image, y * v, z * v)):
                    terms[n].append(term)
        return tuple(a + tree(b) for a, b in zip(acc, terms))

    def whole(i):
        r = i * T
        return [(r, t) for t in range(nt)]

    acc = lax.fori_loop(0, ni, lambda i, c: apply_y(whole(i), c), (zero,) * 5)
    halo_wait(y_copies, 1)

    def edge_sums(stage):
        cols_part = tree([zcol_out[stage, n] * zcol_in[1, 1 - n] for n in range(2)])
        rows_part = tree([zrow_out[stage, n, s] * zrow_in[1, 1 - n, s] for n in range(2) for s in range(D)])
        return down(cols_part) + down(rows_part)

    edge_y, edge_z = edge_sums(1), edge_sums(0)
    acc = tuple(down(a) for a in acc)
    acc = (acc[0], acc[1], acc[2] + centre * (edge_z - centre * edge_y), acc[3] - edge_y, acc[4] - edge_z)

    s0, s2, t0, t2, zv, rho_own, curve_own = (
        full(value) for value in acc + (rho_inner + rho_edge, curve_inner + curve_edge)
    )
    total_out[...] = line([
        s0, 2.0 * (curve_own - centre * s2), s2,
        t0, s2 + zv - 2.0 * centre * t2, t2,
        rho_own, curve_own, centre,
    ])
    pl.semaphore_wait(met_sem, size1 - 1)
    mine = table_ref.at[pl.ds((layer * pxs + px) * pys + py, 1), :]
    pz = 4 if pxs % 4 == 0 else pxs
    px_hi = pxs // pz
    there = [
        (a, x, z, y) for a in range(layers) for x in range(px_hi) for z in range(pz) for y in range(pys)
    ]
    ring = lambda d, n: min(d, n - d)
    there.sort(key=lambda o: -(ring(o[1], px_hi) + ring(o[2], pz) + ring(o[3], pys)))
    for a, x, z, y in there:
        if a or x or z or y:
            peer = {
                "layer": lax.rem(layer + a, layers),
                "px": lax.rem(px // pz + x, px_hi) * pz + lax.rem(lax.rem(px, pz) + z, pz),
                "py": lax.rem(py + y, pys),
            }
            remote(total_out, mine, p_recv, peer, out_sem.at[1]).start()
    pltpu.make_async_copy(total_out, mine, p_recv).start()
    mend_rows(v_ref, 1)
    left_part, right_part = zcol_in[1, 1], col_out[...] * zcol_in[1, 0]

    def mend(i, carry):
        at = tile_at(i * T)
        for s in range(D):
            for t in (0, nt - 1):
                v_ref[s, at, lanes(t)] = v_ref[s, at, lanes(t)] - col_term(left_part, right_part, s * ni + i, t)
        return carry

    lax.fori_loop(0, ni, mend, 0)
    pltpu.make_async_copy(table_ref, table_ref, p_recv).wait()
    table = table_ref[...]
    table_lane = lax.broadcasted_iota(jnp.int32, table.shape, 1)
    centres = jnp.sum(jnp.where(table_lane == 8, table, 0.0), axis=1, keepdims=True)
    plain = jnp.sum(table, axis=0, keepdims=True)
    rho, curve_first = pick(plain, 6), pick(plain, 7)
    alpha = rho / curve_first
    delta = alpha - centres
    linear = (table_lane == 1) | (table_lane == 4)
    square = (table_lane == 2) | (table_lane == 5)
    powers = jnp.where(linear, -delta, jnp.where(square, delta * delta, 1.0))
    moved = jnp.sum(table * powers, axis=0, keepdims=True)
    rho_next = jnp.sum(jnp.where(row_lane < 3, moved, 0.0), axis=1, keepdims=True)
    curve = jnp.sum(jnp.where((row_lane >= 3) & (row_lane < 6), moved, 0.0), axis=1, keepdims=True)
    beta = rho_next / rho
    alpha_next = rho_next / (curve - beta * rho_next / alpha)
    factors[0] = jnp.broadcast_to(alpha + alpha_next * (1.0 + beta), (T, W))
    factors[1] = jnp.broadcast_to(alpha * alpha_next, (T, W))
    for copy in sends:
        copy.wait_send()
    for condition, copy in gated:
        gate(condition, copy.wait_send)
    wait_rows(size1 - 1, out_sem.at[0])
    wait_rows(len(there) - 1, out_sem.at[1])

    @pl.when(bottom)
    def _():
        for copy in c3_copies:
            copy.wait_send()


def finish(shape, bb, zb, yb, w_ref, v_ref, factors, x_hbm, r_hbm, x_buf, r_buf, sem):
    rows, cols = shape
    layer = lax.axis_index("layer")
    loc = [s + layer * (D - 1 - 2 * s) for s in range(D)]
    big, small = factors[0], factors[1]
    stops = [0, T, rows // 4, rows // 2, 3 * rows // 4, rows]
    copies = []

    def body(i, carry):
        r = i * T
        at = pl.ds(pl.multiple_of(r, T), T)
        above = pl.ds(pl.multiple_of(r + T, T), T)
        for s in range(D):
            l = loc[s]
            for t in range(cols // W):
                col = slice(t * W, (t + 1) * W)
                x_buf[l, at, col] = big * zb[s, t, above, :] - small * yb[s, t, above, :]
                r_buf[l, at, col] = bb[l, at, col] - big * w_ref[s, at, col] + small * v_ref[s, at, col]
        return carry

    for c, (lo, hi) in enumerate(zip(stops, stops[1:])):
        if hi == lo:
            continue
        lax.fori_loop(lo // T, hi // T, body, 0)
        at = pl.ds(lo, hi - lo)
        for n, (src, dst) in enumerate(((x_buf, x_hbm), (r_buf, r_hbm))):
            copies.append(pltpu.make_async_copy(src.at[:, at, :], dst.at[:, at, :], sem.at[2 * c + n]))
            copies[-1].start()
    for copy in copies:
        copy.wait()


def solution(mesh):
    layers, pxs, pys = (mesh.shape[a] for a in ("layer", "px", "py"))
    spec = P("layer", "px", "py")

    def step(*args):
        depth, rows, cols = args[0].shape
        nt = cols // W
        block = (depth, rows, cols)
        padded = (depth, nt, rows + 2 * T, W)
        size1 = layers * pys
        dma = pltpu.SemaphoreType.DMA
        vmem = lambda *dims: pltpu.VMEM(dims, F32)
        scratch = [
            vmem(depth, rows + T, cols), vmem(*block), vmem(*block), pltpu.VMEM(block, jnp.int32), vmem(*block),
            vmem(*block), vmem(*block), vmem(*block), vmem(rows, cols), vmem(rows, cols), vmem(rows, cols),
            vmem(*padded), vmem(*padded),
            vmem(2, rows, cols), vmem(2, rows, cols), vmem(rows, cols), vmem(rows, cols),
            vmem(depth, nt, W), vmem(depth, nt, W), vmem(T, W), vmem(T, W),
            vmem(2, 2, depth, nt, W), vmem(2, 2, depth, nt, W), vmem(2, 2, T, W), vmem(2, 2, T, W),
            vmem(1, 1, W), vmem(size1, 1, W), vmem(1, W), vmem(size1 * pxs, W), vmem(size1 * pxs, 1, W),
            dma((6,)), dma((8,)), dma((11,)), dma, dma, pltpu.SemaphoreType.REGULAR((4,)), pltpu.SemaphoreType.REGULAR,
        ]
        out = lambda *dims: jax.ShapeDtypeStruct(dims, F32)
        in_vmem = pl.BlockSpec(memory_space=pltpu.VMEM)
        in_hbm = pl.BlockSpec(memory_space=pltpu.HBM)
        kept = pl.pallas_call(
            functools.partial(kernel, (rows, cols), (layers, pxs, pys)),
            out_shape=(vmem(*block), vmem(*padded), vmem(*padded), vmem(*block), vmem(*block), vmem(2, T, W)),
            in_specs=[in_hbm] * 6,
            out_specs=(in_vmem,) * 6,
            scratch_shapes=scratch,
            compiler_params=pltpu.CompilerParams(
                collective_id=0, has_side_effects=True, vmem_limit_bytes=36 * 2**20
            ),
        )(*(pltpu.with_memory_space_constraint(arg, pltpu.HBM) for arg in args))
        return pl.pallas_call(
            functools.partial(finish, (rows, cols)),
            out_shape=(out(*block), out(*block)),
            in_specs=[in_vmem] * 6,
            out_specs=(in_hbm, in_hbm),
            scratch_shapes=[vmem(*block), vmem(*block), dma((10,))],
            compiler_params=pltpu.CompilerParams(vmem_limit_bytes=6 * 2**20),
        )(*kept)

    return jax.shard_map(step, mesh=mesh, in_specs=(spec,) * 6, out_specs=(spec, spec), check_vma=False)
```

```python
import functools

import jax
import jax.numpy as jnp
from jax import lax
from jax.experimental import pallas as pl
from jax.experimental.pallas import tpu as pltpu
from jax.sharding import PartitionSpec as P

MESH = pl.DeviceIdType.MESH
F32 = jnp.float32
D = 4
T = 8
W = 128


def kernel(shape, counts, *refs):
    dma = pltpu.SemaphoreType.DMA
    pl.run_scoped(functools.partial(solve_all, shape, counts, *refs), dma((34,)), dma((34,)))


def solve_all(
    shape, counts,
    b_hbm, rw_hbm, cl_hbm, vi_hbm, mk_hbm, gd_hbm,
    bb, zb, yb, w_ref, v_ref, factors,
    rwp, cl, vi, mk, gd, inv, gain, num, c3, q3a, q3b,
    qb, qyb, fg_out, fg_in, f_out, f_in,
    row_out, row_in, col_out, col_in,
    zrow_out, zrow_in, zcol_out, zcol_in,
    part, group, total_out, table_ref, sized,
    s_recv, z_recv, m_recv, g_recv, p_recv, far_sem, met_sem,
    load_sem, out_sem,
):
    rows, cols = shape
    layers, pxs, pys = counts
    nt = cols // W
    ni = rows // T
    layer = lax.axis_index("layer")
    px = lax.axis_index("px")
    py = lax.axis_index("py")
    bottom = layer == 0
    loc = [s + layer * (D - 1 - 2 * s) for s in range(D)]
    via = [s + layer * (D - 2 - 2 * s) for s in range(D - 1)]
    size1 = layers * pys
    me1 = layer * pys + py

    def group_peer(d):
        other = lax.rem(me1 + d, size1)
        return {"layer": other // pys, "py": lax.rem(other, pys)}

    def px_peer(d):
        return {"px": lax.rem(px + d, pxs)}

    def py_peer(d):
        return {"py": lax.rem(py + d, pys)}

    partner = {"layer": 1 - layer}
    near = [partner, px_peer(1), px_peer(pxs - 1), py_peer(1), py_peer(pys - 1)]

    barrier = pltpu.get_barrier_semaphore()
    for peer in near:
        pl.semaphore_signal(barrier, inc=1, device_id=peer, device_id_type=MESH)
    has_upper, has_lower = px > 0, px < pxs - 1
    has_left, has_right = py > 0, py < pys - 1

    slot = [0]

    def load(src, dst):
        copy = pltpu.make_async_copy(src, dst, load_sem.at[slot[0]])
        slot[0] += 1
        return copy

    last = (nt - 1) * W
    cl_edge = load(cl_hbm.at[:, :, last : last + W], cl.at[:, :, last : last + W])
    rw_edge = load(rw_hbm.at[:, rows - T : rows, :], rwp.at[:, rows : rows + T, :])
    top_loads = [load(vi_hbm.at[D - 1], vi.at[D - 1]), load(mk_hbm.at[D - 1], mk.at[D - 1])]
    cl_edge.start()
    rw_edge.start()

    @pl.when(bottom)
    def _():
        for copy in top_loads:
            copy.start()

    quarter = rows // 4
    stops = [0, quarter, 2 * quarter, 3 * quarter]
    if quarter >= 4 * T:
        stops.append(rows - 2 * T)
    stops.append(rows)
    chunks = list(zip(stops, stops[1:]))
    chunk_loads = []
    for lo, hi in chunks:
        at = pl.ds(lo, hi - lo)
        short = pl.ds(lo, min(hi, rows - T) - lo)
        chunk_loads.append([] if lo >= rows - T else [
            load(rw_hbm.at[:, short, :], rwp.at[:, pl.ds(T + lo, min(hi, rows - T) - lo), :]),
        ])
        chunk_loads[-1] += [
            load(cl_hbm.at[:, at, 0:last], cl.at[:, at, 0:last]),
            load(vi_hbm.at[0 : D - 1, at, :], vi.at[0 : D - 1, at, :]),
            load(mk_hbm.at[0 : D - 1, at, :], mk.at[0 : D - 1, at, :]),
            load(gd_hbm.at[:, at, :], gd.at[:, at, :]),
            load(b_hbm.at[:, at, :], bb.at[:, at, :]),
        ]
        for copy in chunk_loads[-1]:
            copy.start()

    lane = lax.broadcasted_iota(jnp.int32, (T, W), 1)
    sub = lax.broadcasted_iota(jnp.int32, (T, W), 0)
    zero = jnp.zeros((T, W), F32)

    def gate(condition, *actions):
        @pl.when(condition)
        def _():
            for action in actions:
                action()

    out_slot = [2]

    def remote(src, dst, recv, peer, send=None):
        if send is None:
            send = out_sem.at[out_slot[0]]
            out_slot[0] += 1
        return pltpu.make_async_remote_copy(
            src_ref=src, dst_ref=dst, send_sem=send, recv_sem=recv,
            device_id=peer, device_id_type=MESH,
        )

    def wait_rows(count, sem):
        pltpu.make_async_copy(sized.at[0:count], sized.at[0:count], sem).wait()

    def lanes(t):
        return slice(t * W, (t + 1) * W)

    def tile_at(r):
        return pl.ds(pl.multiple_of(r, T), T)

    cl_edge.wait()
    packs = []
    for s in range(D):
        packed = zero
        for i in range(ni):
            k = s * ni + i
            value = cl[loc[s], i * T : (i + 1) * T, lanes(nt - 1)]
            packed = jnp.where(lane == k, pltpu.roll(value, (k + 1) % W, axis=1), packed)
        packs.append(packed)
    col_out[...] = (packs[0] + packs[1]) + (packs[2] + packs[3])
    rw_edge.wait()
    for s in range(D):
        for t in range(nt):
            row_out[s, t : t + 1, :] = rwp[loc[s], rows + T - 1 : rows + T, lanes(t)]

    pl.semaphore_wait(barrier, len(near))
    row_copy = remote(row_out, row_in, s_recv.at[0], px_peer(1))
    col_copy = remote(col_out, col_in, s_recv.at[1], py_peer(1))
    gate(has_right, col_copy.start)
    gate(has_lower, row_copy.start)
    for peer in near:
        pl.semaphore_signal(far_sem.at[0], inc=1, device_id=peer, device_id_type=MESH)
    c3_copies = [
        remote(c3.at[pl.ds(lo, hi - lo)], c3.at[pl.ds(lo, hi - lo)], s_recv.at[2 + c], partner)
        for c, (lo, hi) in enumerate(chunks)
    ]

    def join(i, carry):
        at = tile_at(i * T)
        c3[at, :] = vi[D - 1, at, :] * mk[D - 1, at, :].astype(F32)
        return carry

    @pl.when(bottom)
    def _():
        for copy in top_loads:
            copy.wait()
        for (lo, hi), copy in zip(chunks, c3_copies):
            lax.fori_loop(lo // T, hi // T, join, 0)
            copy.start()

    gated = [(has_lower, row_copy), (has_right, col_copy)]
    sends = []

    hops = []
    while (2 << len(hops)) < pxs // 2:
        hops.append(2 << len(hops))

    def greet(n):
        if n < len(hops):
            for d in (hops[n], pxs - hops[n]):
                pl.semaphore_signal(far_sem.at[1 + n], inc=1, device_id=px_peer(d), device_id_type=MESH)

    def greeted(n):
        if n < len(hops):
            pl.semaphore_wait(far_sem.at[1 + n], 2)

    def inner(i):
        r = i * T
        return [(r, t) for t in range(1, nt - 1)]

    span = 7 if (ni - 2) % 7 == 0 else 2

    def sides(j):
        starts = [(1 + j * span + m) * T for m in range(span)]
        return [(r, t) for r in starts for t in (0, nt - 1)]

    def ends(j):
        r = j * (rows - T)
        return [(r, t) for t in range(nt)]

    def ends_work(body, carry):
        return lax.fori_loop(0, 2, lambda j, c: body(ends(j), c), carry)

    def sides_work(body, carry):
        return lax.fori_loop(0, (ni - 2) // span, lambda j, c: body(sides(j), c), carry)

    def inner_work(body, carry, start=1, stop=None):
        stop = ni - 1 if stop is None else stop
        return lax.fori_loop(start, stop, lambda i, c: body(inner(i), c), carry)

    def spread(packed, k, to):
        return pltpu.roll(packed, lax.rem(to + W - k, W), axis=1)

    def coupling(s, at, t):
        return vi[via[s], at, lanes(t)] * mk[via[s], at, lanes(t)].astype(F32)

    def factor(items, carry):
        g = [None] * len(items)
        n = [None] * len(items)
        below = [None] * len(items)
        for s in range(D):
            l = loc[s]
            for m, (r, t) in enumerate(items):
                at = tile_at(r)
                rw = rwp[l, tile_at(r + T), lanes(t)]
                before = rwp[l, at, lanes(t)]
                up = pltpu.roll(jnp.where(sub == T - 1, before, rw), 1, axis=0)
                c = cl[l, at, lanes(t)]
                if t == 0:
                    k = s * ni + r // T
                    left = jnp.where(lane == 0, spread(col_in[...], k, 0), pltpu.roll(c, 1, axis=1))
                else:
                    left = pltpu.roll(jnp.where(lane == W - 1, cl[l, at, lanes(t - 1)], c), 1, axis=1)
                if s < D - 1:
                    above = coupling(s, at, t)
                else:
                    above = c3[at, lanes(t)]
                diagonal = gd[l, at, lanes(t)] + rw + up + c + left + above
                right_side = bb[l, at, lanes(t)]
                if s:
                    diagonal = diagonal + below[m]
                    inverse = 1.0 / (diagonal - below[m] * g[m])
                    n[m] = right_side + g[m] * n[m]
                else:
                    inverse = 1.0 / diagonal
                    n[m] = right_side
                below[m] = above
                g[m] = above * inverse
                inv[s, at, lanes(t)] = inverse
                gain[s, at, lanes(t)] = g[m]
                num[s, at, lanes(t)] = n[m]
                if s == D - 1:
                    fg_out[0, at, lanes(t)] = n[m] * inverse
                    fg_out[1, at, lanes(t)] = g[m]
        return carry

    cut = max(2, 9 * ni // 16)
    regions = [
        (pl.ds(T, (cut - 1) * T), pl.ds(W, cols - 2 * W)),
        (pl.ds(cut * T, (ni - 1 - cut) * T), pl.ds(W, cols - 2 * W)),
        (pl.ds(0, rows), pl.ds(0, W)),
        (pl.ds(0, rows), pl.ds(cols - W, W)),
        (pl.ds(0, T), pl.ds(W, cols - 2 * W)),
        (pl.ds(rows - T, T), pl.ds(W, cols - 2 * W)),
    ]

    def middle(out, into, which, base):
        copies = []
        for e, (i, j) in enumerate(which):
            if len(out.shape) == 3:
                src, dst = out.at[:, i, j], into.at[:, i, j]
            else:
                src, dst = out.at[i, j], into.at[i, j]
            copies.append(remote(src, dst, m_recv.at[base + e], partner))
        for copy in copies:
            copy.start()
        sends.extend(copies)
        return copies

    def deep(i):
        r = i * T
        return [(r, t) for t in range(1, nt)]

    fg_inner = []
    for c, (lo, hi) in enumerate(chunks):
        for copy in chunk_loads[c]:
            copy.wait()
        gate(jnp.logical_not(bottom), c3_copies[c].wait_recv)
        lo = max(T, lo)
        lax.fori_loop(lo // T, hi // T, lambda i, x: factor(deep(i), x), 0)
        fg_inner += middle(fg_out, fg_in, [(pl.ds(lo, hi - lo), pl.ds(W, cols - W))], c)

    gate(has_left, col_copy.wait_recv)
    gate(has_upper, row_copy.wait_recv)
    for s in range(D):
        for t in range(nt):
            rwp[loc[s], T - 1 : T, lanes(t)] = jnp.where(has_upper, row_in[s, t : t + 1, :], 0.0)
    col_in[...] = jnp.where(has_left, col_in[...], 0.0)
    group_of = min(8, ni)
    lax.fori_loop(
        0, ni // group_of,
        lambda j, x: factor([(j * group_of * T + m * T, 0) for m in range(group_of)], x), 0,
    )
    lax.fori_loop(0, 1, lambda i, x: factor(deep(i), x), 0)
    pl.semaphore_wait(far_sem.at[0], len(near))
    greet(0)
    fg_edge = middle(fg_out, fg_in, [(pl.ds(0, rows), pl.ds(0, W)), (pl.ds(0, T), pl.ds(W, cols - W))], len(chunks))

    def solve(first, z, q, f_ref, items, carry):
        rho, pack_l, pack_r = carry
        following = [None] * len(items)
        terms = []
        for s in range(D - 1, -1, -1):
            l = loc[s]
            for m, (r, t) in enumerate(items):
                at = tile_at(r)
                if s == D - 1:
                    if first:
                        other = fg_in[1, at, lanes(t)]
                        g = gain[s, at, lanes(t)]
                        quotient = 1.0 / (1.0 - g * other)
                        scale = quotient * inv[s, at, lanes(t)]
                        g = quotient * g
                        q3a[at, lanes(t)] = scale
                        q3b[at, lanes(t)] = g
                        theirs = fg_in[0, at, lanes(t)]
                    else:
                        scale = q3a[at, lanes(t)]
                        g = q3b[at, lanes(t)]
                        theirs = f_ref[at, lanes(t)]
                    value = scale * num[s, at, lanes(t)] + g * theirs
                else:
                    value = num[s, at, lanes(t)] * inv[s, at, lanes(t)] + gain[s, at, lanes(t)] * following[m]
                following[m] = value
                z[s, t, tile_at(r + T), :] = value
                q[s, t, tile_at(r + T), :] = rwp[l, tile_at(r + T), lanes(t)] * value
                if first:
                    terms.append(bb[l, at, lanes(t)] * value)
                if t == 0:
                    k = s * ni + r // T
                    pack_l = jnp.where(lane == k, pltpu.roll(value, k, axis=1), pack_l)
                if t == nt - 1:
                    k = s * ni + r // T
                    side = cl[l, at, lanes(t)] * value
                    pack_r = jnp.where(lane == k, pltpu.roll(side, k + 1, axis=1), pack_r)
        if first:
            rho = rho + tree(terms)
        return rho, pack_l, pack_r

    def tree(values):
        while len(values) > 1:
            values = [a + b for a, b in zip(values[::2], values[1::2])] + ([values[-1]] if len(values) % 2 else [])
        return values[0]

    def start_halos(stage, first, pairs):
        copies = []
        for n, (condition, out, into, peer) in enumerate(pairs):
            copy = remote(out, into, z_recv.at[4 * stage + first + n], peer)
            gate(condition, copy.start)
            gated.append((condition, copy))
            copies.append(copy)
        return copies

    def send_rows(z, q, stage):
        for s in range(D):
            for t in range(nt):
                zrow_out[stage, 0, s, t : t + 1, :] = z[s, t, T : T + 1, :]
                zrow_out[stage, 1, s, t : t + 1, :] = q[s, t, rows + T - 1 : rows + T, :]
        return start_halos(stage, 0, (
            (has_upper, zrow_out.at[stage, 0], zrow_in.at[stage, 0], px_peer(pxs - 1)),
            (has_lower, zrow_out.at[stage, 1], zrow_in.at[stage, 1], px_peer(1)),
        ))

    def send_cols(pack_l, pack_r, stage):
        zcol_out[stage, 0] = pack_l
        zcol_out[stage, 1] = pack_r
        return start_halos(stage, 2, (
            (has_left, zcol_out.at[stage, 0], zcol_in.at[stage, 0], py_peer(pys - 1)),
            (has_right, zcol_out.at[stage, 1], zcol_in.at[stage, 1], py_peer(1)),
        ))

    def halo_wait(copies, stage):
        for condition, copy in zip((has_lower, has_upper, has_right, has_left), copies):
            gate(condition, copy.wait_recv)
        zcol_in[stage, 0] = jnp.where(has_right, zcol_in[stage, 0], 0.0)
        zcol_in[stage, 1] = jnp.where(has_left, zcol_in[stage, 1], 0.0)
        zrow_in[stage, 0] = jnp.where(has_lower, zrow_in[stage, 0], 0.0)
        zrow_in[stage, 1] = jnp.where(has_upper, zrow_in[stage, 1], 0.0)

    def mend_rows(ref, stage):
        for s in range(D):
            for t in range(nt):
                ref[s, 0:1, lanes(t)] = ref[s, 0:1, lanes(t)] - zrow_in[stage, 1, s, t : t + 1, :]
                ref[s, rows - 1 : rows, lanes(t)] = (
                    ref[s, rows - 1 : rows, lanes(t)] - row_out[s, t : t + 1, :] * zrow_in[stage, 0, s, t : t + 1, :]
                )

    def col_term(left_part, right_part, k, t):
        if t == 0:
            return jnp.where(lane == 0, spread(left_part, k, 0), 0.0)
        return jnp.where(lane == W - 1, spread(right_part, k, W - 1), 0.0)

    for z, q in ((zb, qb), (yb, qyb)):
        for s in range(D):
            for t in range(nt):
                z[s, t, rows + T : rows + 2 * T, :] = zero
                q[s, t, 0:T, :] = zero

    solve_z = functools.partial(solve, True, zb, qb, None)
    for copy in fg_inner:
        copy.wait_recv()
    rho_inner = inner_work(solve_z, (zero, zero, zero), 1, cut)[0]
    rho_rest = inner_work(solve_z, (zero, zero, zero), cut)[0]
    for copy in fg_edge:
        copy.wait_recv()
    carry = ends_work(solve_z, (zero, zero, zero))
    z_copies = send_rows(zb, qb, 0)
    rho_edge, pack_l, pack_r = sides_work(solve_z, carry)
    z_copies += send_cols(pack_l, pack_r, 0)

    def coupled(z, q, s, items):
        l = loc[s]
        zs, ps, out = {}, {}, []

        def own(m, r, t):
            if (m, t) not in zs:
                zs[m, t] = z[s, t, tile_at(r + T), :]
            return zs[m, t]

        def product(m, r, t):
            if (m, t) not in ps:
                ps[m, t] = cl[l, tile_at(r), lanes(t)] * own(m, r, t)
            return ps[m, t]

        rows_seen = []
        for r, t in items:
            m = next((n for n, other in enumerate(rows_seen) if other is r), None)
            if m is None:
                rows_seen.append(r)
                m = len(rows_seen) - 1
            at = tile_at(r)
            value = own(m, r, t)
            down = z[s, t, pl.ds(r + T + 1, T), :]
            up = q[s, t, pl.ds(r + T - 1, T), :]
            after = own(m, r, t + 1) if t < nt - 1 else 0.0
            before = product(m, r, t - 1) if t else 0.0
            right = pltpu.roll(jnp.where(lane == 0, after, value), W - 1, axis=1)
            left = pltpu.roll(jnp.where(lane == W - 1, before, product(m, r, t)), 1, axis=1)
            rw = rwp[l, tile_at(r + T), lanes(t)]
            c = cl[l, at, lanes(t)]
            out.append((value, rw * down + up + (c * right + left)))
        return out

    def apply_z(items, curve):
        n = [None] * len(items)
        terms = []
        for s in range(D):
            for m, ((r, t), (value, h)) in enumerate(zip(items, coupled(zb, qb, s, items))):
                at = tile_at(r)
                w = bb[loc[s], at, lanes(t)] - h
                w_ref[s, at, lanes(t)] = w
                terms.append(value * w)
                n[m] = w if s == 0 else w + gain[s - 1, at, lanes(t)] * n[m]
                num[s, at, lanes(t)] = n[m]
                if s == D - 1:
                    f_out[at, lanes(t)] = n[m] * inv[s, at, lanes(t)]
        return curve + tree(terms)

    def start_edge(items, carry):
        for s in range(D):
            for (r, t), (_, h) in zip(items, coupled(zb, qb, s, items)):
                at = tile_at(r)
                w_ref[s, at, lanes(t)] = bb[loc[s], at, lanes(t)] - h
        return carry

    def end_edge(left_part, right_part, items, curve):
        n = [None] * len(items)
        terms = []
        for s in range(D):
            for m, (r, t) in enumerate(items):
                at = tile_at(r)
                w = w_ref[s, at, lanes(t)]
                if t in (0, nt - 1):
                    w = w - col_term(left_part, right_part, s * ni + r // T, t)
                    w_ref[s, at, lanes(t)] = w
                terms.append(zb[s, t, tile_at(r + T), :] * w)
                n[m] = w if s == 0 else w + gain[s - 1, at, lanes(t)] * n[m]
                num[s, at, lanes(t)] = n[m]
                if s == D - 1:
                    f_out[at, lanes(t)] = n[m] * inv[s, at, lanes(t)]
        return curve + tree(terms)

    def down(value):
        return jnp.sum(value, axis=0, keepdims=True)

    def full(value):
        return jnp.sum(down(value), axis=1, keepdims=True)

    row_lane = lax.broadcasted_iota(jnp.int32, (1, W), 1)

    def line(values):
        out = jnp.zeros((1, W), F32)
        for n, value in enumerate(values):
            out = jnp.where(row_lane == n, value, out)
        return out

    def gather_group(values):
        part[0] = line(values)
        group[pl.ds(me1, 1)] = line(values)[None]
        for d in range(1, size1):
            remote(part.at[0], group.at[me1], g_recv, group_peer(d), out_sem.at[0]).start()

    def group_sum():
        wait_rows(size1 - 1, g_recv)
        return tree([group[m] for m in range(size1)])

    curve_inner = inner_work(apply_z, zero, 1, cut)
    f_inner = middle(f_out, f_in, regions[:1], len(chunks) + 2)
    greeted(0)
    greet(1)
    gather_group([full(rho_inner), full(curve_inner)])
    sides_work(start_edge, ends_work(start_edge, 0))
    halo_wait(z_copies, 0)
    mend_rows(w_ref, 0)
    end_z = functools.partial(end_edge, zcol_in[0, 1], col_out[...] * zcol_in[0, 0])

    curve_edge = sides_work(end_z, ends_work(end_z, zero))
    f_edge = middle(f_out, f_in, regions[2:], len(chunks) + 4)
    curve_rest = inner_work(apply_z, zero, cut)
    f_rest = middle(f_out, f_in, regions[1:2], len(chunks) + 3)
    for n in range(1, len(hops)):
        greeted(n)
        greet(n + 1)
    for d in range(1, size1):
        pl.semaphore_signal(met_sem, inc=1, device_id=group_peer(d), device_id_type=MESH)

    solve_y = functools.partial(solve, False, yb, qyb, f_in)
    carry = (zero, zero, zero)
    for copy in f_inner:
        copy.wait_recv()
    inner_work(solve_y, carry, 1, cut)
    for copy in f_edge:
        copy.wait_recv()
    carry = ends_work(solve_y, carry)
    y_copies = send_rows(yb, qyb, 1)
    carry = sides_work(solve_y, carry)
    y_copies += send_cols(carry[1], carry[2], 1)
    for copy in f_rest:
        copy.wait_recv()
    inner_work(solve_y, carry, cut)

    sums = group_sum()

    def pick(value, n):
        return jnp.sum(jnp.where(row_lane == n, value, 0.0), axis=1, keepdims=True)

    rho_group, curve_group = pick(sums, 0), pick(sums, 1)
    ok = (rho_group > 0.0) & (curve_group > 0.0)
    centre = jnp.where(ok, rho_group / jnp.where(ok, curve_group, 1.0), 1.0)
    centre_tile = jnp.broadcast_to(centre, (T, W))

    def apply_y(items, acc):
        terms = [[] for _ in acc]
        for s in range(D):
            for (r, t), (y, h) in zip(items, coupled(yb, qyb, s, items)):
                at = tile_at(r)
                w = w_ref[s, at, lanes(t)]
                v = w - h
                v_ref[s, at, lanes(t)] = v
                z = zb[s, t, tile_at(r + T), :]
                res = bb[loc[s], at, lanes(t)] - centre_tile * w
                pre = z - centre_tile * y
                image = w - centre_tile * v
                for n, term in enumerate((res * pre, w * y, pre * image, y * v, z * v)):
                    terms[n].append(term)
        return tuple(a + tree(b) for a, b in zip(acc, terms))

    def whole(i):
        r = i * T
        return [(r, t) for t in range(nt)]

    acc = lax.fori_loop(0, ni, lambda i, c: apply_y(whole(i), c), (zero,) * 5)
    halo_wait(y_copies, 1)

    def edge_sums(stage):
        cols_part = tree([zcol_out[stage, n] * zcol_in[1, 1 - n] for n in range(2)])
        rows_part = tree([zrow_out[stage, n, s] * zrow_in[1, 1 - n, s] for n in range(2) for s in range(D)])
        return down(cols_part) + down(rows_part)

    edge_y, edge_z = edge_sums(1), edge_sums(0)
    acc = tuple(down(a) for a in acc)
    acc = (acc[0], acc[1], acc[2] + centre * (edge_z - centre * edge_y), acc[3] - edge_y, acc[4] - edge_z)

    s0, s2, t0, t2, zv, rho_own, curve_own = (
        full(value) for value in acc + (rho_inner + rho_rest + rho_edge, curve_inner + curve_rest + curve_edge)
    )
    total_out[...] = line([
        s0, 2.0 * (curve_own - centre * s2), s2,
        t0, s2 + zv - 2.0 * centre * t2, t2,
        rho_own, curve_own, centre,
    ])
    pl.semaphore_wait(met_sem, size1 - 1)
    mine = table_ref.at[pl.ds((layer * pxs + px) * pys + py, 1), :]
    pz = 4 if pxs % 4 == 0 else pxs
    px_hi = pxs // pz
    there = [
        (a, x, z, y) for a in range(layers) for x in range(px_hi) for z in range(pz) for y in range(pys)
    ]
    ring = lambda d, n: min(d, n - d)
    there.sort(key=lambda o: -(ring(o[1], px_hi) + ring(o[2], pz) + ring(o[3], pys)))
    for a, x, z, y in there:
        if a or x or z or y:
            peer = {
                "layer": lax.rem(layer + a, layers),
                "px": lax.rem(px // pz + x, px_hi) * pz + lax.rem(lax.rem(px, pz) + z, pz),
                "py": lax.rem(py + y, pys),
            }
            remote(total_out, mine, p_recv, peer, out_sem.at[1]).start()
    pltpu.make_async_copy(total_out, mine, p_recv).start()
    mend_rows(v_ref, 1)
    left_part, right_part = zcol_in[1, 1], col_out[...] * zcol_in[1, 0]

    def mend(i, carry):
        at = tile_at(i * T)
        for s in range(D):
            for t in (0, nt - 1):
                v_ref[s, at, lanes(t)] = v_ref[s, at, lanes(t)] - col_term(left_part, right_part, s * ni + i, t)
        return carry

    lax.fori_loop(0, ni, mend, 0)
    pltpu.make_async_copy(table_ref, table_ref, p_recv).wait()
    table = table_ref[...]
    table_lane = lax.broadcasted_iota(jnp.int32, table.shape, 1)
    centres = jnp.sum(jnp.where(table_lane == 8, table, 0.0), axis=1, keepdims=True)
    plain = jnp.sum(table, axis=0, keepdims=True)
    rho, curve_first = pick(plain, 6), pick(plain, 7)
    alpha = rho / curve_first
    delta = alpha - centres
    linear = (table_lane == 1) | (table_lane == 4)
    square = (table_lane == 2) | (table_lane == 5)
    powers = jnp.where(linear, -delta, jnp.where(square, delta * delta, 1.0))
    moved = jnp.sum(table * powers, axis=0, keepdims=True)
    rho_next = jnp.sum(jnp.where(row_lane < 3, moved, 0.0), axis=1, keepdims=True)
    curve = jnp.sum(jnp.where((row_lane >= 3) & (row_lane < 6), moved, 0.0), axis=1, keepdims=True)
    beta = rho_next / rho
    alpha_next = rho_next / (curve - beta * rho_next / alpha)
    factors[0] = jnp.broadcast_to(alpha + alpha_next * (1.0 + beta), (T, W))
    factors[1] = jnp.broadcast_to(alpha * alpha_next, (T, W))
    for copy in sends:
        copy.wait_send()
    for condition, copy in gated:
        gate(condition, copy.wait_send)
    wait_rows(size1 - 1, out_sem.at[0])
    wait_rows(len(there) - 1, out_sem.at[1])

    @pl.when(bottom)
    def _():
        for copy in c3_copies:
            copy.wait_send()


def finish(shape, bb, zb, yb, w_ref, v_ref, factors, x_hbm, r_hbm, x_buf, r_buf, sem):
    rows, cols = shape
    layer = lax.axis_index("layer")
    loc = [s + layer * (D - 1 - 2 * s) for s in range(D)]
    big, small = factors[0], factors[1]
    stops = [0, T, rows // 4, rows // 2, 3 * rows // 4, rows]
    copies = []

    def body(i, carry):
        r = i * T
        at = pl.ds(pl.multiple_of(r, T), T)
        above = pl.ds(pl.multiple_of(r + T, T), T)
        for s in range(D):
            l = loc[s]
            for t in range(cols // W):
                col = slice(t * W, (t + 1) * W)
                x_buf[l, at, col] = big * zb[s, t, above, :] - small * yb[s, t, above, :]
                r_buf[l, at, col] = bb[l, at, col] - big * w_ref[s, at, col] + small * v_ref[s, at, col]
        return carry

    for c, (lo, hi) in enumerate(zip(stops, stops[1:])):
        if hi == lo:
            continue
        lax.fori_loop(lo // T, hi // T, body, 0)
        at = pl.ds(lo, hi - lo)
        for n, (src, dst) in enumerate(((x_buf, x_hbm), (r_buf, r_hbm))):
            copies.append(pltpu.make_async_copy(src.at[:, at, :], dst.at[:, at, :], sem.at[2 * c + n]))
            copies[-1].start()
    for copy in copies:
        copy.wait()


def solution(mesh):
    layers, pxs, pys = (mesh.shape[a] for a in ("layer", "px", "py"))
    spec = P("layer", "px", "py")

    def step(*args):
        depth, rows, cols = args[0].shape
        nt = cols // W
        block = (depth, rows, cols)
        padded = (depth, nt, rows + 2 * T, W)
        size1 = layers * pys
        dma = pltpu.SemaphoreType.DMA
        vmem = lambda *dims: pltpu.VMEM(dims, F32)
        scratch = [
            vmem(depth, rows + T, cols), vmem(*block), vmem(*block), pltpu.VMEM(block, jnp.int32), vmem(*block),
            vmem(*block), vmem(*block), vmem(*block), vmem(rows, cols), vmem(rows, cols), vmem(rows, cols),
            vmem(*padded), vmem(*padded),
            vmem(2, rows, cols), vmem(2, rows, cols), vmem(rows, cols), vmem(rows, cols),
            vmem(depth, nt, W), vmem(depth, nt, W), vmem(T, W), vmem(T, W),
            vmem(2, 2, depth, nt, W), vmem(2, 2, depth, nt, W), vmem(2, 2, T, W), vmem(2, 2, T, W),
            vmem(1, 1, W), vmem(size1, 1, W), vmem(1, W), vmem(size1 * pxs, W), vmem(size1 * pxs, 1, W),
            dma((7,)), dma((8,)), dma((13,)), dma, dma, pltpu.SemaphoreType.REGULAR((4,)), pltpu.SemaphoreType.REGULAR,
        ]
        out = lambda *dims: jax.ShapeDtypeStruct(dims, F32)
        in_vmem = pl.BlockSpec(memory_space=pltpu.VMEM)
        in_hbm = pl.BlockSpec(memory_space=pltpu.HBM)
        kept = pl.pallas_call(
            functools.partial(kernel, (rows, cols), (layers, pxs, pys)),
            out_shape=(vmem(*block), vmem(*padded), vmem(*padded), vmem(*block), vmem(*block), vmem(2, T, W)),
            in_specs=[in_hbm] * 6,
            out_specs=(in_vmem,) * 6,
            scratch_shapes=scratch,
            compiler_params=pltpu.CompilerParams(
                collective_id=0, has_side_effects=True, vmem_limit_bytes=36 * 2**20
            ),
        )(*(pltpu.with_memory_space_constraint(arg, pltpu.HBM) for arg in args))
        return pl.pallas_call(
            functools.partial(finish, (rows, cols)),
            out_shape=(out(*block), out(*block)),
            in_specs=[in_vmem] * 6,
            out_specs=(in_hbm, in_hbm),
            scratch_shapes=[vmem(*block), vmem(*block), dma((10,))],
            compiler_params=pltpu.CompilerParams(vmem_limit_bytes=6 * 2**20),
        )(*kept)

    return jax.shard_map(step, mesh=mesh, in_specs=(spec,) * 6, out_specs=(spec, spec), check_vma=False)
```

```python
import functools

import jax
import jax.numpy as jnp
from jax import lax
from jax.experimental import pallas as pl
from jax.experimental.pallas import tpu as pltpu
from jax.sharding import PartitionSpec as P

MESH = pl.DeviceIdType.MESH
F32 = jnp.float32
D = 4
T = 8
W = 128


def kernel(shape, counts, *refs):
    dma = pltpu.SemaphoreType.DMA
    pl.run_scoped(functools.partial(solve_all, shape, counts, *refs), dma((34,)), dma((34,)))


def solve_all(
    shape, counts,
    b_hbm, rw_hbm, cl_hbm, vi_hbm, mk_hbm, gd_hbm,
    bb, zb, yb, w_ref, v_ref, factors,
    rwp, cl, vi, mk, gd, inv, gain, num, c3, q3a, q3b,
    qb, qyb, fg_out, fg_in, f_out, f_in,
    row_out, row_in, col_out, col_in,
    zrow_out, zrow_in, zcol_out, zcol_in,
    part, group, total_out, table_ref, sized,
    s_recv, z_recv, m_recv, g_recv, p_recv, far_sem, met_sem,
    load_sem, out_sem,
):
    rows, cols = shape
    layers, pxs, pys = counts
    nt = cols // W
    ni = rows // T
    layer = lax.axis_index("layer")
    px = lax.axis_index("px")
    py = lax.axis_index("py")
    bottom = layer == 0
    loc = [s + layer * (D - 1 - 2 * s) for s in range(D)]
    via = [s + layer * (D - 2 - 2 * s) for s in range(D - 1)]
    size1 = layers * pys
    me1 = layer * pys + py

    def group_peer(d):
        other = lax.rem(me1 + d, size1)
        return {"layer": other // pys, "py": lax.rem(other, pys)}

    def px_peer(d):
        return {"px": lax.rem(px + d, pxs)}

    def py_peer(d):
        return {"py": lax.rem(py + d, pys)}

    partner = {"layer": 1 - layer}
    near = [partner, px_peer(1), px_peer(pxs - 1), py_peer(1), py_peer(pys - 1)]

    barrier = pltpu.get_barrier_semaphore()
    for peer in near:
        pl.semaphore_signal(barrier, inc=1, device_id=peer, device_id_type=MESH)
    has_upper, has_lower = px > 0, px < pxs - 1
    has_left, has_right = py > 0, py < pys - 1

    slot = [0]

    def load(src, dst):
        copy = pltpu.make_async_copy(src, dst, load_sem.at[slot[0]])
        slot[0] += 1
        return copy

    last = (nt - 1) * W
    cl_edge = load(cl_hbm.at[:, :, last : last + W], cl.at[:, :, last : last + W])
    rw_edge = load(rw_hbm.at[:, rows - T : rows, :], rwp.at[:, rows : rows + T, :])
    top_loads = [load(vi_hbm.at[D - 1], vi.at[D - 1]), load(mk_hbm.at[D - 1], mk.at[D - 1])]
    rw_edge.start()
    cl_edge.start()

    @pl.when(bottom)
    def _():
        for copy in top_loads:
            copy.start()

    quarter = rows // 4
    stops = [0, quarter, 2 * quarter, 3 * quarter]
    if quarter >= 4 * T:
        stops.append(rows - 2 * T)
    stops.append(rows)
    chunks = list(zip(stops, stops[1:]))
    chunk_loads = []
    for lo, hi in chunks:
        at = pl.ds(lo, hi - lo)
        short = pl.ds(lo, min(hi, rows - T) - lo)
        chunk_loads.append([] if lo >= rows - T else [
            load(rw_hbm.at[:, short, :], rwp.at[:, pl.ds(T + lo, min(hi, rows - T) - lo), :]),
        ])
        chunk_loads[-1] += [
            load(cl_hbm.at[:, at, 0:last], cl.at[:, at, 0:last]),
            load(vi_hbm.at[0 : D - 1, at, :], vi.at[0 : D - 1, at, :]),
            load(mk_hbm.at[0 : D - 1, at, :], mk.at[0 : D - 1, at, :]),
            load(gd_hbm.at[:, at, :], gd.at[:, at, :]),
            load(b_hbm.at[:, at, :], bb.at[:, at, :]),
        ]
        for copy in chunk_loads[-1]:
            copy.start()

    lane = lax.broadcasted_iota(jnp.int32, (T, W), 1)
    sub = lax.broadcasted_iota(jnp.int32, (T, W), 0)
    zero = jnp.zeros((T, W), F32)

    def gate(condition, *actions):
        @pl.when(condition)
        def _():
            for action in actions:
                action()

    out_slot = [2]

    def remote(src, dst, recv, peer, send=None):
        if send is None:
            send = out_sem.at[out_slot[0]]
            out_slot[0] += 1
        return pltpu.make_async_remote_copy(
            src_ref=src, dst_ref=dst, send_sem=send, recv_sem=recv,
            device_id=peer, device_id_type=MESH,
        )

    def wait_rows(count, sem):
        pltpu.make_async_copy(sized.at[0:count], sized.at[0:count], sem).wait()

    def lanes(t):
        return slice(t * W, (t + 1) * W)

    def tile_at(r):
        return pl.ds(pl.multiple_of(r, T), T)

    cl_edge.wait()
    packs = []
    for s in range(D):
        packed = zero
        for i in range(ni):
            k = s * ni + i
            value = cl[loc[s], i * T : (i + 1) * T, lanes(nt - 1)]
            packed = jnp.where(lane == k, pltpu.roll(value, (k + 1) % W, axis=1), packed)
        packs.append(packed)
    col_out[...] = (packs[0] + packs[1]) + (packs[2] + packs[3])
    rw_edge.wait()
    for s in range(D):
        for t in range(nt):
            row_out[s, t : t + 1, :] = rwp[loc[s], rows + T - 1 : rows + T, lanes(t)]

    pl.semaphore_wait(barrier, len(near))
    row_copy = remote(row_out, row_in, s_recv.at[0], px_peer(1))
    col_copy = remote(col_out, col_in, s_recv.at[1], py_peer(1))
    gate(has_lower, row_copy.start)
    gate(has_right, col_copy.start)
    for peer in near:
        pl.semaphore_signal(far_sem.at[0], inc=1, device_id=peer, device_id_type=MESH)
    c3_copies = [
        remote(c3.at[pl.ds(lo, hi - lo)], c3.at[pl.ds(lo, hi - lo)], s_recv.at[2 + c], partner)
        for c, (lo, hi) in enumerate(chunks)
    ]

    def join(i, carry):
        at = tile_at(i * T)
        c3[at, :] = vi[D - 1, at, :] * mk[D - 1, at, :].astype(F32)
        return carry

    @pl.when(bottom)
    def _():
        for copy in top_loads:
            copy.wait()
        for (lo, hi), copy in zip(chunks, c3_copies):
            lax.fori_loop(lo // T, hi // T, join, 0)
            copy.start()

    gated = [(has_lower, row_copy), (has_right, col_copy)]
    sends = []

    hops = []
    while (2 << len(hops)) < pxs // 2:
        hops.append(2 << len(hops))

    def greet(n):
        if n < len(hops):
            for d in (hops[n], pxs - hops[n]):
                pl.semaphore_signal(far_sem.at[1 + n], inc=1, device_id=px_peer(d), device_id_type=MESH)

    def greeted(n):
        if n < len(hops):
            pl.semaphore_wait(far_sem.at[1 + n], 2)

    def inner(i):
        r = i * T
        return [(r, t) for t in range(1, nt - 1)]

    span = 7 if (ni - 2) % 7 == 0 else 2

    def sides(j):
        starts = [(1 + j * span + m) * T for m in range(span)]
        return [(r, t) for r in starts for t in (0, nt - 1)]

    def ends(j):
        r = j * (rows - T)
        return [(r, t) for t in range(nt)]

    def ends_work(body, carry):
        return lax.fori_loop(0, 2, lambda j, c: body(ends(j), c), carry)

    def sides_work(body, carry):
        return lax.fori_loop(0, (ni - 2) // span, lambda j, c: body(sides(j), c), carry)

    def inner_work(body, carry, start=1, stop=None):
        stop = ni - 1 if stop is None else stop
        return lax.fori_loop(start, stop, lambda i, c: body(inner(i), c), carry)

    def spread(packed, k, to):
        return pltpu.roll(packed, lax.rem(to + W - k, W), axis=1)

    def coupling(s, at, t):
        return vi[via[s], at, lanes(t)] * mk[via[s], at, lanes(t)].astype(F32)

    def factor(items, carry):
        g = [None] * len(items)
        n = [None] * len(items)
        below = [None] * len(items)
        for s in range(D):
            l = loc[s]
            for m, (r, t) in enumerate(items):
                at = tile_at(r)
                rw = rwp[l, tile_at(r + T), lanes(t)]
                before = rwp[l, at, lanes(t)]
                up = pltpu.roll(jnp.where(sub == T - 1, before, rw), 1, axis=0)
                c = cl[l, at, lanes(t)]
                if t == 0:
                    k = s * ni + r // T
                    left = jnp.where(lane == 0, spread(col_in[...], k, 0), pltpu.roll(c, 1, axis=1))
                else:
                    left = pltpu.roll(jnp.where(lane == W - 1, cl[l, at, lanes(t - 1)], c), 1, axis=1)
                if s < D - 1:
                    above = coupling(s, at, t)
                else:
                    above = c3[at, lanes(t)]
                diagonal = gd[l, at, lanes(t)] + rw + up + c + left + above
                right_side = bb[l, at, lanes(t)]
                if s:
                    diagonal = diagonal + below[m]
                    inverse = 1.0 / (diagonal - below[m] * g[m])
                    n[m] = right_side + g[m] * n[m]
                else:
                    inverse = 1.0 / diagonal
                    n[m] = right_side
                below[m] = above
                g[m] = above * inverse
                inv[s, at, lanes(t)] = inverse
                gain[s, at, lanes(t)] = g[m]
                num[s, at, lanes(t)] = n[m]
                if s == D - 1:
                    fg_out[0, at, lanes(t)] = n[m] * inverse
                    fg_out[1, at, lanes(t)] = g[m]
        return carry

    cut = max(2, 9 * ni // 16)
    regions = [
        (pl.ds(T, (cut - 1) * T), pl.ds(W, cols - 2 * W)),
        (pl.ds(cut * T, (ni - 1 - cut) * T), pl.ds(W, cols - 2 * W)),
        (pl.ds(0, rows), pl.ds(0, W)),
        (pl.ds(0, rows), pl.ds(cols - W, W)),
        (pl.ds(0, T), pl.ds(W, cols - 2 * W)),
        (pl.ds(rows - T, T), pl.ds(W, cols - 2 * W)),
    ]

    def middle(out, into, which, base):
        copies = []
        for e, (i, j) in enumerate(which):
            if len(out.shape) == 3:
                src, dst = out.at[:, i, j], into.at[:, i, j]
            else:
                src, dst = out.at[i, j], into.at[i, j]
            copies.append(remote(src, dst, m_recv.at[base + e], partner))
        for copy in copies:
            copy.start()
        sends.extend(copies)
        return copies

    def deep(i):
        r = i * T
        return [(r, t) for t in range(1, nt)]

    fg_inner = []
    for c, (lo, hi) in enumerate(chunks):
        for copy in chunk_loads[c]:
            copy.wait()
        gate(jnp.logical_not(bottom), c3_copies[c].wait_recv)
        lo = max(T, lo)
        lax.fori_loop(lo // T, hi // T, lambda i, x: factor(deep(i), x), 0)
        fg_inner += middle(fg_out, fg_in, [(pl.ds(lo, hi - lo), pl.ds(W, cols - W))], c)

    gate(has_left, col_copy.wait_recv)
    gate(has_upper, row_copy.wait_recv)
    for s in range(D):
        for t in range(nt):
            rwp[loc[s], T - 1 : T, lanes(t)] = jnp.where(has_upper, row_in[s, t : t + 1, :], 0.0)
    col_in[...] = jnp.where(has_left, col_in[...], 0.0)
    group_of = min(8, ni)
    lax.fori_loop(
        0, ni // group_of,
        lambda j, x: factor([(j * group_of * T + m * T, 0) for m in range(group_of)], x), 0,
    )
    lax.fori_loop(0, 1, lambda i, x: factor(deep(i), x), 0)
    pl.semaphore_wait(far_sem.at[0], len(near))
    greet(0)
    fg_edge = middle(fg_out, fg_in, [(pl.ds(0, rows), pl.ds(0, W)), (pl.ds(0, T), pl.ds(W, cols - W))], len(chunks))

    def solve(first, z, q, f_ref, items, carry):
        rho, pack_l, pack_r = carry
        following = [None] * len(items)
        terms = []
        for s in range(D - 1, -1, -1):
            l = loc[s]
            for m, (r, t) in enumerate(items):
                at = tile_at(r)
                if s == D - 1:
                    if first:
                        other = fg_in[1, at, lanes(t)]
                        g = gain[s, at, lanes(t)]
                        quotient = 1.0 / (1.0 - g * other)
                        scale = quotient * inv[s, at, lanes(t)]
                        g = quotient * g
                        q3a[at, lanes(t)] = scale
                        q3b[at, lanes(t)] = g
                        theirs = fg_in[0, at, lanes(t)]
                    else:
                        scale = q3a[at, lanes(t)]
                        g = q3b[at, lanes(t)]
                        theirs = f_ref[at, lanes(t)]
                    value = scale * num[s, at, lanes(t)] + g * theirs
                else:
                    value = num[s, at, lanes(t)] * inv[s, at, lanes(t)] + gain[s, at, lanes(t)] * following[m]
                following[m] = value
                z[s, t, tile_at(r + T), :] = value
                q[s, t, tile_at(r + T), :] = rwp[l, tile_at(r + T), lanes(t)] * value
                if first:
                    terms.append(bb[l, at, lanes(t)] * value)
                if t == 0:
                    k = s * ni + r // T
                    pack_l = jnp.where(lane == k, pltpu.roll(value, k, axis=1), pack_l)
                if t == nt - 1:
                    k = s * ni + r // T
                    side = cl[l, at, lanes(t)] * value
                    pack_r = jnp.where(lane == k, pltpu.roll(side, k + 1, axis=1), pack_r)
        if first:
            rho = rho + tree(terms)
        return rho, pack_l, pack_r

    def tree(values):
        while len(values) > 1:
            values = [a + b for a, b in zip(values[::2], values[1::2])] + ([values[-1]] if len(values) % 2 else [])
        return values[0]

    def start_halos(stage, first, pairs):
        copies = []
        for n, (condition, out, into, peer) in enumerate(pairs):
            copy = remote(out, into, z_recv.at[4 * stage + first + n], peer)
            gate(condition, copy.start)
            gated.append((condition, copy))
            copies.append(copy)
        return copies

    def send_rows(z, q, stage):
        for s in range(D):
            for t in range(nt):
                zrow_out[stage, 0, s, t : t + 1, :] = z[s, t, T : T + 1, :]
                zrow_out[stage, 1, s, t : t + 1, :] = q[s, t, rows + T - 1 : rows + T, :]
        return start_halos(stage, 0, (
            (has_upper, zrow_out.at[stage, 0], zrow_in.at[stage, 0], px_peer(pxs - 1)),
            (has_lower, zrow_out.at[stage, 1], zrow_in.at[stage, 1], px_peer(1)),
        ))

    def send_cols(pack_l, pack_r, stage):
        zcol_out[stage, 0] = pack_l
        zcol_out[stage, 1] = pack_r
        return start_halos(stage, 2, (
            (has_left, zcol_out.at[stage, 0], zcol_in.at[stage, 0], py_peer(pys - 1)),
            (has_right, zcol_out.at[stage, 1], zcol_in.at[stage, 1], py_peer(1)),
        ))

    def halo_wait(copies, stage):
        for condition, copy in zip((has_lower, has_upper, has_right, has_left), copies):
            gate(condition, copy.wait_recv)
        zcol_in[stage, 0] = jnp.where(has_right, zcol_in[stage, 0], 0.0)
        zcol_in[stage, 1] = jnp.where(has_left, zcol_in[stage, 1], 0.0)
        zrow_in[stage, 0] = jnp.where(has_lower, zrow_in[stage, 0], 0.0)
        zrow_in[stage, 1] = jnp.where(has_upper, zrow_in[stage, 1], 0.0)

    def mend_rows(ref, stage):
        for s in range(D):
            for t in range(nt):
                ref[s, 0:1, lanes(t)] = ref[s, 0:1, lanes(t)] - zrow_in[stage, 1, s, t : t + 1, :]
                ref[s, rows - 1 : rows, lanes(t)] = (
                    ref[s, rows - 1 : rows, lanes(t)] - row_out[s, t : t + 1, :] * zrow_in[stage, 0, s, t : t + 1, :]
                )

    def col_term(left_part, right_part, k, t):
        if t == 0:
            return jnp.where(lane == 0, spread(left_part, k, 0), 0.0)
        return jnp.where(lane == W - 1, spread(right_part, k, W - 1), 0.0)

    for z, q in ((zb, qb), (yb, qyb)):
        for s in range(D):
            for t in range(nt):
                z[s, t, rows + T : rows + 2 * T, :] = zero
                q[s, t, 0:T, :] = zero

    solve_z = functools.partial(solve, True, zb, qb, None)
    for copy in fg_inner:
        copy.wait_recv()
    rho_inner = inner_work(solve_z, (zero, zero, zero), 1, cut)[0]
    rho_rest = inner_work(solve_z, (zero, zero, zero), cut)[0]
    for copy in fg_edge:
        copy.wait_recv()
    carry = ends_work(solve_z, (zero, zero, zero))
    z_copies = send_rows(zb, qb, 0)
    rho_edge, pack_l, pack_r = sides_work(solve_z, carry)
    z_copies += send_cols(pack_l, pack_r, 0)

    def coupled(z, q, s, items):
        l = loc[s]
        zs, ps, out = {}, {}, []

        def own(m, r, t):
            if (m, t) not in zs:
                zs[m, t] = z[s, t, tile_at(r + T), :]
            return zs[m, t]

        def product(m, r, t):
            if (m, t) not in ps:
                ps[m, t] = cl[l, tile_at(r), lanes(t)] * own(m, r, t)
            return ps[m, t]

        rows_seen = []
        for r, t in items:
            m = next((n for n, other in enumerate(rows_seen) if other is r), None)
            if m is None:
                rows_seen.append(r)
                m = len(rows_seen) - 1
            at = tile_at(r)
            value = own(m, r, t)
            down = z[s, t, pl.ds(r + T + 1, T), :]
            up = q[s, t, pl.ds(r + T - 1, T), :]
            after = own(m, r, t + 1) if t < nt - 1 else 0.0
            before = product(m, r, t - 1) if t else 0.0
            right = pltpu.roll(jnp.where(lane == 0, after, value), W - 1, axis=1)
            left = pltpu.roll(jnp.where(lane == W - 1, before, product(m, r, t)), 1, axis=1)
            rw = rwp[l, tile_at(r + T), lanes(t)]
            c = cl[l, at, lanes(t)]
            out.append((value, rw * down + up + (c * right + left)))
        return out

    def apply_z(items, curve):
        n = [None] * len(items)
        terms = []
        for s in range(D):
            for m, ((r, t), (value, h)) in enumerate(zip(items, coupled(zb, qb, s, items))):
                at = tile_at(r)
                w = bb[loc[s], at, lanes(t)] - h
                w_ref[s, at, lanes(t)] = w
                terms.append(value * w)
                n[m] = w if s == 0 else w + gain[s - 1, at, lanes(t)] * n[m]
                num[s, at, lanes(t)] = n[m]
                if s == D - 1:
                    f_out[at, lanes(t)] = n[m] * inv[s, at, lanes(t)]
        return curve + tree(terms)

    def start_edge(items, carry):
        for s in range(D):
            for (r, t), (_, h) in zip(items, coupled(zb, qb, s, items)):
                at = tile_at(r)
                w_ref[s, at, lanes(t)] = bb[loc[s], at, lanes(t)] - h
        return carry

    def end_edge(left_part, right_part, items, curve):
        n = [None] * len(items)
        terms = []
        for s in range(D):
            for m, (r, t) in enumerate(items):
                at = tile_at(r)
                w = w_ref[s, at, lanes(t)]
                if t in (0, nt - 1):
                    w = w - col_term(left_part, right_part, s * ni + r // T, t)
                    w_ref[s, at, lanes(t)] = w
                terms.append(zb[s, t, tile_at(r + T), :] * w)
                n[m] = w if s == 0 else w + gain[s - 1, at, lanes(t)] * n[m]
                num[s, at, lanes(t)] = n[m]
                if s == D - 1:
                    f_out[at, lanes(t)] = n[m] * inv[s, at, lanes(t)]
        return curve + tree(terms)

    def down(value):
        return jnp.sum(value, axis=0, keepdims=True)

    def full(value):
        return jnp.sum(down(value), axis=1, keepdims=True)

    row_lane = lax.broadcasted_iota(jnp.int32, (1, W), 1)

    def line(values):
        out = jnp.zeros((1, W), F32)
        for n, value in enumerate(values):
            out = jnp.where(row_lane == n, value, out)
        return out

    def gather_group(values):
        part[0] = line(values)
        group[pl.ds(me1, 1)] = line(values)[None]
        for d in range(1, size1):
            remote(part.at[0], group.at[me1], g_recv, group_peer(d), out_sem.at[0]).start()

    def group_sum():
        wait_rows(size1 - 1, g_recv)
        return tree([group[m] for m in range(size1)])

    curve_inner = inner_work(apply_z, zero, 1, cut)
    f_inner = middle(f_out, f_in, regions[:1], len(chunks) + 2)
    gather_group([full(rho_inner), full(curve_inner)])
    sides_work(start_edge, ends_work(start_edge, 0))
    halo_wait(z_copies, 0)
    mend_rows(w_ref, 0)
    end_z = functools.partial(end_edge, zcol_in[0, 1], col_out[...] * zcol_in[0, 0])

    curve_edge = sides_work(end_z, ends_work(end_z, zero))
    f_edge = middle(f_out, f_in, regions[2:], len(chunks) + 4)
    curve_rest = inner_work(apply_z, zero, cut)
    f_rest = middle(f_out, f_in, regions[1:2], len(chunks) + 3)
    greeted(0)
    greet(1)
    solve_y = functools.partial(solve, False, yb, qyb, f_in)
    carry = (zero, zero, zero)
    for copy in f_inner:
        copy.wait_recv()
    inner_work(solve_y, carry, 1, cut)
    for copy in f_edge:
        copy.wait_recv()
    carry = ends_work(solve_y, carry)
    y_copies = send_rows(yb, qyb, 1)
    carry = sides_work(solve_y, carry)
    y_copies += send_cols(carry[1], carry[2], 1)
    for copy in f_rest:
        copy.wait_recv()
    inner_work(solve_y, carry, cut)

    for n in range(1, len(hops)):
        greeted(n)
        greet(n + 1)
    for d in range(1, size1):
        pl.semaphore_signal(met_sem, inc=1, device_id=group_peer(d), device_id_type=MESH)
    sums = group_sum()

    def pick(value, n):
        return jnp.sum(jnp.where(row_lane == n, value, 0.0), axis=1, keepdims=True)

    rho_group, curve_group = pick(sums, 0), pick(sums, 1)
    ok = (rho_group > 0.0) & (curve_group > 0.0)
    centre = jnp.where(ok, rho_group / jnp.where(ok, curve_group, 1.0), 1.0)
    centre_tile = jnp.broadcast_to(centre, (T, W))

    def apply_y(items, acc):
        terms = [[] for _ in acc]
        for s in range(D):
            for (r, t), (y, h) in zip(items, coupled(yb, qyb, s, items)):
                at = tile_at(r)
                w = w_ref[s, at, lanes(t)]
                v = w - h
                v_ref[s, at, lanes(t)] = v
                z = zb[s, t, tile_at(r + T), :]
                res = bb[loc[s], at, lanes(t)] - centre_tile * w
                pre = z - centre_tile * y
                image = w - centre_tile * v
                for n, term in enumerate((res * pre, w * y, pre * image, y * v, z * v)):
                    terms[n].append(term)
        return tuple(a + tree(b) for a, b in zip(acc, terms))

    def whole(i):
        r = i * T
        return [(r, t) for t in range(nt)]

    acc = lax.fori_loop(0, ni, lambda i, c: apply_y(whole(i), c), (zero,) * 5)
    halo_wait(y_copies, 1)

    def edge_sums(stage):
        cols_part = tree([zcol_out[stage, n] * zcol_in[1, 1 - n] for n in range(2)])
        rows_part = tree([zrow_out[stage, n, s] * zrow_in[1, 1 - n, s] for n in range(2) for s in range(D)])
        return down(cols_part) + down(rows_part)

    edge_y, edge_z = edge_sums(1), edge_sums(0)
    acc = tuple(down(a) for a in acc)
    acc = (acc[0], acc[1], acc[2] + centre * (edge_z - centre * edge_y), acc[3] - edge_y, acc[4] - edge_z)

    s0, s2, t0, t2, zv, rho_own, curve_own = (
        full(value) for value in acc + (rho_inner + rho_rest + rho_edge, curve_inner + curve_rest + curve_edge)
    )
    total_out[...] = line([
        s0, 2.0 * (curve_own - centre * s2), s2,
        t0, s2 + zv - 2.0 * centre * t2, t2,
        rho_own, curve_own, centre,
    ])
    pl.semaphore_wait(met_sem, size1 - 1)
    mine = table_ref.at[pl.ds((layer * pxs + px) * pys + py, 1), :]
    pz = 4 if pxs % 4 == 0 else pxs
    px_hi = pxs // pz
    there = [
        (a, x, z, y) for a in range(layers) for x in range(px_hi) for z in range(pz) for y in range(pys)
    ]
    ring = lambda d, n: min(d, n - d)
    there.sort(key=lambda o: -(ring(o[1], px_hi) + ring(o[2], pz) + ring(o[3], pys)))
    for a, x, z, y in there:
        if a or x or z or y:
            peer = {
                "layer": lax.rem(layer + a, layers),
                "px": lax.rem(px // pz + x, px_hi) * pz + lax.rem(lax.rem(px, pz) + z, pz),
                "py": lax.rem(py + y, pys),
            }
            remote(total_out, mine, p_recv, peer, out_sem.at[1]).start()
    pltpu.make_async_copy(total_out, mine, p_recv).start()
    mend_rows(v_ref, 1)
    left_part, right_part = zcol_in[1, 1], col_out[...] * zcol_in[1, 0]

    def mend(i, carry):
        at = tile_at(i * T)
        for s in range(D):
            for t in (0, nt - 1):
                v_ref[s, at, lanes(t)] = v_ref[s, at, lanes(t)] - col_term(left_part, right_part, s * ni + i, t)
        return carry

    lax.fori_loop(0, ni, mend, 0)
    pltpu.make_async_copy(table_ref, table_ref, p_recv).wait()
    table = table_ref[...]
    table_lane = lax.broadcasted_iota(jnp.int32, table.shape, 1)
    centres = jnp.sum(jnp.where(table_lane == 8, table, 0.0), axis=1, keepdims=True)
    plain = jnp.sum(table, axis=0, keepdims=True)
    rho, curve_first = pick(plain, 6), pick(plain, 7)
    alpha = rho / curve_first
    delta = alpha - centres
    linear = (table_lane == 1) | (table_lane == 4)
    square = (table_lane == 2) | (table_lane == 5)
    powers = jnp.where(linear, -delta, jnp.where(square, delta * delta, 1.0))
    moved = jnp.sum(table * powers, axis=0, keepdims=True)
    rho_next = jnp.sum(jnp.where(row_lane < 3, moved, 0.0), axis=1, keepdims=True)
    curve = jnp.sum(jnp.where((row_lane >= 3) & (row_lane < 6), moved, 0.0), axis=1, keepdims=True)
    beta = rho_next / rho
    alpha_next = rho_next / (curve - beta * rho_next / alpha)
    factors[0] = jnp.broadcast_to(alpha + alpha_next * (1.0 + beta), (T, W))
    factors[1] = jnp.broadcast_to(alpha * alpha_next, (T, W))
    for copy in sends:
        copy.wait_send()
    for condition, copy in gated:
        gate(condition, copy.wait_send)
    wait_rows(size1 - 1, out_sem.at[0])
    wait_rows(len(there) - 1, out_sem.at[1])

    @pl.when(bottom)
    def _():
        for copy in c3_copies:
            copy.wait_send()


def finish(shape, bb, zb, yb, w_ref, v_ref, factors, x_hbm, r_hbm, x_buf, r_buf, sem):
    rows, cols = shape
    layer = lax.axis_index("layer")
    loc = [s + layer * (D - 1 - 2 * s) for s in range(D)]
    big, small = factors[0], factors[1]
    stops = [0, T, rows // 4, rows // 2, 3 * rows // 4, rows]
    copies = []

    def body(i, carry):
        r = i * T
        at = pl.ds(pl.multiple_of(r, T), T)
        above = pl.ds(pl.multiple_of(r + T, T), T)
        for s in range(D):
            l = loc[s]
            for t in range(cols // W):
                col = slice(t * W, (t + 1) * W)
                x_buf[l, at, col] = big * zb[s, t, above, :] - small * yb[s, t, above, :]
                r_buf[l, at, col] = bb[l, at, col] - big * w_ref[s, at, col] + small * v_ref[s, at, col]
        return carry

    for c, (lo, hi) in enumerate(zip(stops, stops[1:])):
        if hi == lo:
            continue
        lax.fori_loop(lo // T, hi // T, body, 0)
        at = pl.ds(lo, hi - lo)
        for n, (src, dst) in enumerate(((x_buf, x_hbm), (r_buf, r_hbm))):
            copies.append(pltpu.make_async_copy(src.at[:, at, :], dst.at[:, at, :], sem.at[2 * c + n]))
            copies[-1].start()
    for copy in copies:
        copy.wait()


def solution(mesh):
    layers, pxs, pys = (mesh.shape[a] for a in ("layer", "px", "py"))
    spec = P("layer", "px", "py")

    def step(*args):
        depth, rows, cols = args[0].shape
        nt = cols // W
        block = (depth, rows, cols)
        padded = (depth, nt, rows + 2 * T, W)
        size1 = layers * pys
        dma = pltpu.SemaphoreType.DMA
        vmem = lambda *dims: pltpu.VMEM(dims, F32)
        scratch = [
            vmem(depth, rows + T, cols), vmem(*block), vmem(*block), pltpu.VMEM(block, jnp.int32), vmem(*block),
            vmem(*block), vmem(*block), vmem(*block), vmem(rows, cols), vmem(rows, cols), vmem(rows, cols),
            vmem(*padded), vmem(*padded),
            vmem(2, rows, cols), vmem(2, rows, cols), vmem(rows, cols), vmem(rows, cols),
            vmem(depth, nt, W), vmem(depth, nt, W), vmem(T, W), vmem(T, W),
            vmem(2, 2, depth, nt, W), vmem(2, 2, depth, nt, W), vmem(2, 2, T, W), vmem(2, 2, T, W),
            vmem(1, 1, W), vmem(size1, 1, W), vmem(1, W), vmem(size1 * pxs, W), vmem(size1 * pxs, 1, W),
            dma((7,)), dma((8,)), dma((13,)), dma, dma, pltpu.SemaphoreType.REGULAR((4,)), pltpu.SemaphoreType.REGULAR,
        ]
        out = lambda *dims: jax.ShapeDtypeStruct(dims, F32)
        in_vmem = pl.BlockSpec(memory_space=pltpu.VMEM)
        in_hbm = pl.BlockSpec(memory_space=pltpu.HBM)
        kept = pl.pallas_call(
            functools.partial(kernel, (rows, cols), (layers, pxs, pys)),
            out_shape=(vmem(*block), vmem(*padded), vmem(*padded), vmem(*block), vmem(*block), vmem(2, T, W)),
            in_specs=[in_hbm] * 6,
            out_specs=(in_vmem,) * 6,
            scratch_shapes=scratch,
            compiler_params=pltpu.CompilerParams(
                collective_id=0, has_side_effects=True, vmem_limit_bytes=36 * 2**20
            ),
        )(*(pltpu.with_memory_space_constraint(arg, pltpu.HBM) for arg in args))
        return pl.pallas_call(
            functools.partial(finish, (rows, cols)),
            out_shape=(out(*block), out(*block)),
            in_specs=[in_vmem] * 6,
            out_specs=(in_hbm, in_hbm),
            scratch_shapes=[vmem(*block), vmem(*block), dma((10,))],
            compiler_params=pltpu.CompilerParams(vmem_limit_bytes=6 * 2**20),
        )(*kept)

    return jax.shard_map(step, mesh=mesh, in_specs=(spec,) * 6, out_specs=(spec, spec), check_vma=False)
```

```python
import functools

import jax
import jax.numpy as jnp
from jax import lax
from jax.experimental import pallas as pl
from jax.experimental.pallas import tpu as pltpu
from jax.sharding import PartitionSpec as P

MESH = pl.DeviceIdType.MESH
F32 = jnp.float32
D = 4
T = 8
W = 128


def kernel(shape, counts, *refs):
    dma = pltpu.SemaphoreType.DMA
    pl.run_scoped(functools.partial(solve_all, shape, counts, *refs), dma((34,)), dma((34,)))


def solve_all(
    shape, counts,
    b_hbm, rw_hbm, cl_hbm, vi_hbm, mk_hbm, gd_hbm,
    bb, zb, yb, w_ref, v_ref, factors,
    rwp, cl, vi, mk, gd, inv, gain, num, c3, q3a, q3b,
    qb, qyb, fg_out, fg_in, f_out, f_in,
    row_out, row_in, col_out, col_in,
    zrow_out, zrow_in, zcol_out, zcol_in,
    part, group, total_out, table_ref, sized,
    s_recv, z_recv, m_recv, g_recv, p_recv, far_sem, met_sem,
    load_sem, out_sem,
):
    rows, cols = shape
    layers, pxs, pys = counts
    nt = cols // W
    ni = rows // T
    layer = lax.axis_index("layer")
    px = lax.axis_index("px")
    py = lax.axis_index("py")
    bottom = layer == 0
    loc = [s + layer * (D - 1 - 2 * s) for s in range(D)]
    via = [s + layer * (D - 2 - 2 * s) for s in range(D - 1)]
    size1 = layers * pys
    me1 = layer * pys + py

    def group_peer(d):
        other = lax.rem(me1 + d, size1)
        return {"layer": other // pys, "py": lax.rem(other, pys)}

    def px_peer(d):
        return {"px": lax.rem(px + d, pxs)}

    def py_peer(d):
        return {"py": lax.rem(py + d, pys)}

    partner = {"layer": 1 - layer}
    near = [partner, px_peer(1), px_peer(pxs - 1), py_peer(1), py_peer(pys - 1)]

    barrier = pltpu.get_barrier_semaphore()
    for peer in near:
        pl.semaphore_signal(barrier, inc=1, device_id=peer, device_id_type=MESH)
    has_upper, has_lower = px > 0, px < pxs - 1
    has_left, has_right = py > 0, py < pys - 1

    slot = [0]

    def load(src, dst):
        copy = pltpu.make_async_copy(src, dst, load_sem.at[slot[0]])
        slot[0] += 1
        return copy

    last = (nt - 1) * W
    cl_edge = load(cl_hbm.at[:, :, last : last + W], cl.at[:, :, last : last + W])
    rw_edge = load(rw_hbm.at[:, rows - T : rows, :], rwp.at[:, rows : rows + T, :])
    top_loads = [load(vi_hbm.at[D - 1], vi.at[D - 1]), load(mk_hbm.at[D - 1], mk.at[D - 1])]
    rw_edge.start()
    cl_edge.start()

    @pl.when(bottom)
    def _():
        for copy in top_loads:
            copy.start()

    quarter = rows // 4
    stops = [0, quarter, 2 * quarter, 3 * quarter]
    if quarter >= 4 * T:
        stops.append(rows - 2 * T)
    stops.append(rows)
    chunks = list(zip(stops, stops[1:]))
    chunk_loads = []
    for lo, hi in chunks:
        at = pl.ds(lo, hi - lo)
        short = pl.ds(lo, min(hi, rows - T) - lo)
        chunk_loads.append([] if lo >= rows - T else [
            load(rw_hbm.at[:, short, :], rwp.at[:, pl.ds(T + lo, min(hi, rows - T) - lo), :]),
        ])
        chunk_loads[-1] += [
            load(cl_hbm.at[:, at, 0:last], cl.at[:, at, 0:last]),
            load(vi_hbm.at[0 : D - 1, at, :], vi.at[0 : D - 1, at, :]),
            load(mk_hbm.at[0 : D - 1, at, :], mk.at[0 : D - 1, at, :]),
            load(gd_hbm.at[:, at, :], gd.at[:, at, :]),
            load(b_hbm.at[:, at, :], bb.at[:, at, :]),
        ]
        for copy in chunk_loads[-1]:
            copy.start()

    lane = lax.broadcasted_iota(jnp.int32, (T, W), 1)
    sub = lax.broadcasted_iota(jnp.int32, (T, W), 0)
    zero = jnp.zeros((T, W), F32)

    def gate(condition, *actions):
        @pl.when(condition)
        def _():
            for action in actions:
                action()

    out_slot = [2]

    def remote(src, dst, recv, peer, send=None):
        if send is None:
            send = out_sem.at[out_slot[0]]
            out_slot[0] += 1
        return pltpu.make_async_remote_copy(
            src_ref=src, dst_ref=dst, send_sem=send, recv_sem=recv,
            device_id=peer, device_id_type=MESH,
        )

    def wait_rows(count, sem):
        pltpu.make_async_copy(sized.at[0:count], sized.at[0:count], sem).wait()

    def lanes(t):
        return slice(t * W, (t + 1) * W)

    def tile_at(r):
        return pl.ds(pl.multiple_of(r, T), T)

    cl_edge.wait()
    packs = []
    for s in range(D):
        packed = zero
        for i in range(ni):
            k = s * ni + i
            value = cl[loc[s], i * T : (i + 1) * T, lanes(nt - 1)]
            packed = jnp.where(lane == k, pltpu.roll(value, (k + 1) % W, axis=1), packed)
        packs.append(packed)
    col_out[...] = (packs[0] + packs[1]) + (packs[2] + packs[3])
    rw_edge.wait()
    for s in range(D):
        for t in range(nt):
            row_out[s, t : t + 1, :] = rwp[loc[s], rows + T - 1 : rows + T, lanes(t)]

    pl.semaphore_wait(barrier, len(near))
    row_copy = remote(row_out, row_in, s_recv.at[0], px_peer(1))
    col_copy = remote(col_out, col_in, s_recv.at[1], py_peer(1))
    gate(has_lower, row_copy.start)
    gate(has_right, col_copy.start)
    for peer in near:
        pl.semaphore_signal(far_sem.at[0], inc=1, device_id=peer, device_id_type=MESH)
    c3_copies = [
        remote(c3.at[pl.ds(lo, hi - lo)], c3.at[pl.ds(lo, hi - lo)], s_recv.at[2 + c], partner)
        for c, (lo, hi) in enumerate(chunks)
    ]

    def join(i, carry):
        at = tile_at(i * T)
        c3[at, :] = vi[D - 1, at, :] * mk[D - 1, at, :].astype(F32)
        return carry

    @pl.when(bottom)
    def _():
        for copy in top_loads:
            copy.wait()
        for (lo, hi), copy in zip(chunks, c3_copies):
            lax.fori_loop(lo // T, hi // T, join, 0)
            copy.start()

    gated = [(has_lower, row_copy), (has_right, col_copy)]
    sends = []

    hops = []
    while (2 << len(hops)) < pxs // 2:
        hops.append(2 << len(hops))

    def greet(n):
        if n < len(hops):
            for d in (hops[n], pxs - hops[n]):
                pl.semaphore_signal(far_sem.at[1 + n], inc=1, device_id=px_peer(d), device_id_type=MESH)

    def greeted(n):
        if n < len(hops):
            pl.semaphore_wait(far_sem.at[1 + n], 2)

    def inner(i):
        r = i * T
        return [(r, t) for t in range(1, nt - 1)]

    span = 7 if (ni - 2) % 7 == 0 else 2

    def sides(j):
        starts = [(1 + j * span + m) * T for m in range(span)]
        return [(r, t) for r in starts for t in (0, nt - 1)]

    def ends(j):
        r = j * (rows - T)
        return [(r, t) for t in range(nt)]

    def ends_work(body, carry):
        return lax.fori_loop(0, 2, lambda j, c: body(ends(j), c), carry)

    def sides_work(body, carry):
        return lax.fori_loop(0, (ni - 2) // span, lambda j, c: body(sides(j), c), carry)

    def inner_work(body, carry, start=1, stop=None):
        stop = ni - 1 if stop is None else stop
        return lax.fori_loop(start, stop, lambda i, c: body(inner(i), c), carry)

    def spread(packed, k, to):
        return pltpu.roll(packed, lax.rem(to + W - k, W), axis=1)

    def coupling(s, at, t):
        return vi[via[s], at, lanes(t)] * mk[via[s], at, lanes(t)].astype(F32)

    def factor(items, carry):
        g = [None] * len(items)
        n = [None] * len(items)
        below = [None] * len(items)
        for s in range(D):
            l = loc[s]
            for m, (r, t) in enumerate(items):
                at = tile_at(r)
                rw = rwp[l, tile_at(r + T), lanes(t)]
                before = rwp[l, at, lanes(t)]
                up = pltpu.roll(jnp.where(sub == T - 1, before, rw), 1, axis=0)
                c = cl[l, at, lanes(t)]
                if t == 0:
                    k = s * ni + r // T
                    left = jnp.where(lane == 0, spread(col_in[...], k, 0), pltpu.roll(c, 1, axis=1))
                else:
                    left = pltpu.roll(jnp.where(lane == W - 1, cl[l, at, lanes(t - 1)], c), 1, axis=1)
                if s < D - 1:
                    above = coupling(s, at, t)
                else:
                    above = c3[at, lanes(t)]
                diagonal = gd[l, at, lanes(t)] + rw + up + c + left + above
                right_side = bb[l, at, lanes(t)]
                if s:
                    diagonal = diagonal + below[m]
                    inverse = 1.0 / (diagonal - below[m] * g[m])
                    n[m] = right_side + g[m] * n[m]
                else:
                    inverse = 1.0 / diagonal
                    n[m] = right_side
                below[m] = above
                g[m] = above * inverse
                inv[s, at, lanes(t)] = inverse
                gain[s, at, lanes(t)] = g[m]
                num[s, at, lanes(t)] = n[m]
                if s == D - 1:
                    fg_out[0, at, lanes(t)] = n[m] * inverse
                    fg_out[1, at, lanes(t)] = g[m]
        return carry

    cut = max(2, 9 * ni // 16)
    regions = [
        (pl.ds(T, (cut - 1) * T), pl.ds(W, cols - 2 * W)),
        (pl.ds(cut * T, (ni - 1 - cut) * T), pl.ds(W, cols - 2 * W)),
        (pl.ds(0, rows), pl.ds(0, W)),
        (pl.ds(0, rows), pl.ds(cols - W, W)),
        (pl.ds(0, T), pl.ds(W, cols - 2 * W)),
        (pl.ds(rows - T, T), pl.ds(W, cols - 2 * W)),
    ]

    def middle(out, into, which, base):
        copies = []
        for e, (i, j) in enumerate(which):
            if len(out.shape) == 3:
                src, dst = out.at[:, i, j], into.at[:, i, j]
            else:
                src, dst = out.at[i, j], into.at[i, j]
            copies.append(remote(src, dst, m_recv.at[base + e], partner))
        for copy in copies:
            copy.start()
        sends.extend(copies)
        return copies

    def deep(i):
        r = i * T
        return [(r, t) for t in range(1, nt)]

    fg_inner = []
    for c, (lo, hi) in enumerate(chunks):
        for copy in chunk_loads[c]:
            copy.wait()
        gate(jnp.logical_not(bottom), c3_copies[c].wait_recv)
        lo = max(T, lo)
        lax.fori_loop(lo // T, hi // T, lambda i, x: factor(deep(i), x), 0)
        fg_inner += middle(fg_out, fg_in, [(pl.ds(lo, hi - lo), pl.ds(W, cols - W))], c)

    gate(has_left, col_copy.wait_recv)
    gate(has_upper, row_copy.wait_recv)
    for s in range(D):
        for t in range(nt):
            rwp[loc[s], T - 1 : T, lanes(t)] = jnp.where(has_upper, row_in[s, t : t + 1, :], 0.0)
    col_in[...] = jnp.where(has_left, col_in[...], 0.0)
    group_of = min(8, ni)
    lax.fori_loop(
        0, ni // group_of,
        lambda j, x: factor([(j * group_of * T + m * T, 0) for m in range(group_of)], x), 0,
    )
    lax.fori_loop(0, 1, lambda i, x: factor(deep(i), x), 0)
    pl.semaphore_wait(far_sem.at[0], len(near))
    greet(0)
    fg_edge = middle(fg_out, fg_in, [(pl.ds(0, rows), pl.ds(0, W)), (pl.ds(0, T), pl.ds(W, cols - W))], len(chunks))

    def solve(first, z, q, f_ref, items, carry):
        rho, pack_l, pack_r = carry
        following = [None] * len(items)
        terms = []
        for s in range(D - 1, -1, -1):
            l = loc[s]
            for m, (r, t) in enumerate(items):
                at = tile_at(r)
                if s == D - 1:
                    if first:
                        other = fg_in[1, at, lanes(t)]
                        g = gain[s, at, lanes(t)]
                        quotient = 1.0 / (1.0 - g * other)
                        scale = quotient * inv[s, at, lanes(t)]
                        g = quotient * g
                        q3a[at, lanes(t)] = scale
                        q3b[at, lanes(t)] = g
                        theirs = fg_in[0, at, lanes(t)]
                    else:
                        scale = q3a[at, lanes(t)]
                        g = q3b[at, lanes(t)]
                        theirs = f_ref[at, lanes(t)]
                    value = scale * num[s, at, lanes(t)] + g * theirs
                else:
                    value = num[s, at, lanes(t)] * inv[s, at, lanes(t)] + gain[s, at, lanes(t)] * following[m]
                following[m] = value
                z[s, t, tile_at(r + T), :] = value
                q[s, t, tile_at(r + T), :] = rwp[l, tile_at(r + T), lanes(t)] * value
                if first:
                    terms.append(bb[l, at, lanes(t)] * value)
                if t == 0:
                    k = s * ni + r // T
                    pack_l = jnp.where(lane == k, pltpu.roll(value, k, axis=1), pack_l)
                if t == nt - 1:
                    k = s * ni + r // T
                    side = cl[l, at, lanes(t)] * value
                    pack_r = jnp.where(lane == k, pltpu.roll(side, k + 1, axis=1), pack_r)
        if first:
            rho = rho + tree(terms)
        return rho, pack_l, pack_r

    def tree(values):
        while len(values) > 1:
            values = [a + b for a, b in zip(values[::2], values[1::2])] + ([values[-1]] if len(values) % 2 else [])
        return values[0]

    def start_halos(stage, first, pairs):
        copies = []
        for n, (condition, out, into, peer) in enumerate(pairs):
            copy = remote(out, into, z_recv.at[4 * stage + first + n], peer)
            gate(condition, copy.start)
            gated.append((condition, copy))
            copies.append(copy)
        return copies

    def send_rows(z, q, stage):
        for s in range(D):
            for t in range(nt):
                zrow_out[stage, 0, s, t : t + 1, :] = z[s, t, T : T + 1, :]
                zrow_out[stage, 1, s, t : t + 1, :] = q[s, t, rows + T - 1 : rows + T, :]
        return start_halos(stage, 0, (
            (has_upper, zrow_out.at[stage, 0], zrow_in.at[stage, 0], px_peer(pxs - 1)),
            (has_lower, zrow_out.at[stage, 1], zrow_in.at[stage, 1], px_peer(1)),
        ))

    def send_cols(pack_l, pack_r, stage):
        zcol_out[stage, 0] = pack_l
        zcol_out[stage, 1] = pack_r
        return start_halos(stage, 2, (
            (has_left, zcol_out.at[stage, 0], zcol_in.at[stage, 0], py_peer(pys - 1)),
            (has_right, zcol_out.at[stage, 1], zcol_in.at[stage, 1], py_peer(1)),
        ))

    def halo_wait(copies, stage):
        for condition, copy in zip((has_lower, has_upper, has_right, has_left), copies):
            gate(condition, copy.wait_recv)
        zcol_in[stage, 0] = jnp.where(has_right, zcol_in[stage, 0], 0.0)
        zcol_in[stage, 1] = jnp.where(has_left, zcol_in[stage, 1], 0.0)
        zrow_in[stage, 0] = jnp.where(has_lower, zrow_in[stage, 0], 0.0)
        zrow_in[stage, 1] = jnp.where(has_upper, zrow_in[stage, 1], 0.0)

    def mend_rows(ref, stage):
        for s in range(D):
            for t in range(nt):
                ref[s, 0:1, lanes(t)] = ref[s, 0:1, lanes(t)] - zrow_in[stage, 1, s, t : t + 1, :]
                ref[s, rows - 1 : rows, lanes(t)] = (
                    ref[s, rows - 1 : rows, lanes(t)] - row_out[s, t : t + 1, :] * zrow_in[stage, 0, s, t : t + 1, :]
                )

    def col_term(left_part, right_part, k, t):
        if t == 0:
            return jnp.where(lane == 0, spread(left_part, k, 0), 0.0)
        return jnp.where(lane == W - 1, spread(right_part, k, W - 1), 0.0)

    for z, q in ((zb, qb), (yb, qyb)):
        for s in range(D):
            for t in range(nt):
                z[s, t, rows + T : rows + 2 * T, :] = zero
                q[s, t, 0:T, :] = zero

    solve_z = functools.partial(solve, True, zb, qb, None)
    for copy in fg_inner:
        copy.wait_recv()
    rho_inner = inner_work(solve_z, (zero, zero, zero), 1, cut)[0]
    rho_rest = inner_work(solve_z, (zero, zero, zero), cut)[0]
    for copy in fg_edge:
        copy.wait_recv()
    carry = ends_work(solve_z, (zero, zero, zero))
    z_copies = send_rows(zb, qb, 0)
    rho_edge, pack_l, pack_r = sides_work(solve_z, carry)
    z_copies += send_cols(pack_l, pack_r, 0)

    def coupled(z, q, s, items):
        l = loc[s]
        zs, ps, out = {}, {}, []

        def own(m, r, t):
            if (m, t) not in zs:
                zs[m, t] = z[s, t, tile_at(r + T), :]
            return zs[m, t]

        def product(m, r, t):
            if (m, t) not in ps:
                ps[m, t] = cl[l, tile_at(r), lanes(t)] * own(m, r, t)
            return ps[m, t]

        rows_seen = []
        for r, t in items:
            m = next((n for n, other in enumerate(rows_seen) if other is r), None)
            if m is None:
                rows_seen.append(r)
                m = len(rows_seen) - 1
            at = tile_at(r)
            value = own(m, r, t)
            down = z[s, t, pl.ds(r + T + 1, T), :]
            up = q[s, t, pl.ds(r + T - 1, T), :]
            after = own(m, r, t + 1) if t < nt - 1 else 0.0
            before = product(m, r, t - 1) if t else 0.0
            right = pltpu.roll(jnp.where(lane == 0, after, value), W - 1, axis=1)
            left = pltpu.roll(jnp.where(lane == W - 1, before, product(m, r, t)), 1, axis=1)
            rw = rwp[l, tile_at(r + T), lanes(t)]
            c = cl[l, at, lanes(t)]
            out.append((value, rw * down + up + (c * right + left)))
        return out

    def apply_z(items, curve):
        n = [None] * len(items)
        terms = []
        for s in range(D):
            for m, ((r, t), (value, h)) in enumerate(zip(items, coupled(zb, qb, s, items))):
                at = tile_at(r)
                w = bb[loc[s], at, lanes(t)] - h
                w_ref[s, at, lanes(t)] = w
                terms.append(value * w)
                n[m] = w if s == 0 else w + gain[s - 1, at, lanes(t)] * n[m]
                num[s, at, lanes(t)] = n[m]
                if s == D - 1:
                    f_out[at, lanes(t)] = n[m] * inv[s, at, lanes(t)]
        return curve + tree(terms)

    def start_edge(items, carry):
        for s in range(D):
            for (r, t), (_, h) in zip(items, coupled(zb, qb, s, items)):
                at = tile_at(r)
                w_ref[s, at, lanes(t)] = bb[loc[s], at, lanes(t)] - h
        return carry

    def end_edge(left_part, right_part, items, curve):
        n = [None] * len(items)
        terms = []
        for s in range(D):
            for m, (r, t) in enumerate(items):
                at = tile_at(r)
                w = w_ref[s, at, lanes(t)]
                if t in (0, nt - 1):
                    w = w - col_term(left_part, right_part, s * ni + r // T, t)
                    w_ref[s, at, lanes(t)] = w
                terms.append(zb[s, t, tile_at(r + T), :] * w)
                n[m] = w if s == 0 else w + gain[s - 1, at, lanes(t)] * n[m]
                num[s, at, lanes(t)] = n[m]
                if s == D - 1:
                    f_out[at, lanes(t)] = n[m] * inv[s, at, lanes(t)]
        return curve + tree(terms)

    def down(value):
        return jnp.sum(value, axis=0, keepdims=True)

    def full(value):
        return jnp.sum(down(value), axis=1, keepdims=True)

    row_lane = lax.broadcasted_iota(jnp.int32, (1, W), 1)

    def line(values):
        out = jnp.zeros((1, W), F32)
        for n, value in enumerate(values):
            out = jnp.where(row_lane == n, value, out)
        return out

    def gather_group(values):
        part[0] = line(values)
        group[pl.ds(me1, 1)] = line(values)[None]
        for d in range(1, size1):
            remote(part.at[0], group.at[me1], g_recv, group_peer(d), out_sem.at[0]).start()

    def group_sum():
        wait_rows(size1 - 1, g_recv)
        return tree([group[m] for m in range(size1)])

    curve_inner = inner_work(apply_z, zero, 1, cut)
    f_inner = middle(f_out, f_in, regions[:1], len(chunks) + 2)
    gather_group([full(rho_inner), full(curve_inner)])
    sides_work(start_edge, ends_work(start_edge, 0))
    halo_wait(z_copies, 0)
    greeted(0)
    greet(1)
    mend_rows(w_ref, 0)
    end_z = functools.partial(end_edge, zcol_in[0, 1], col_out[...] * zcol_in[0, 0])

    curve_edge = sides_work(end_z, ends_work(end_z, zero))
    f_edge = middle(f_out, f_in, regions[2:], len(chunks) + 4)
    curve_rest = inner_work(apply_z, zero, cut)
    f_rest = middle(f_out, f_in, regions[1:2], len(chunks) + 3)
    solve_y = functools.partial(solve, False, yb, qyb, f_in)
    carry = (zero, zero, zero)
    for copy in f_inner:
        copy.wait_recv()
    inner_work(solve_y, carry, 1, cut)
    for copy in f_edge:
        copy.wait_recv()
    carry = ends_work(solve_y, carry)
    y_copies = send_rows(yb, qyb, 1)
    carry = sides_work(solve_y, carry)
    y_copies += send_cols(carry[1], carry[2], 1)
    for copy in f_rest:
        copy.wait_recv()
    inner_work(solve_y, carry, cut)

    for n in range(1, len(hops)):
        greeted(n)
        greet(n + 1)
    for d in range(1, size1):
        pl.semaphore_signal(met_sem, inc=1, device_id=group_peer(d), device_id_type=MESH)
    sums = group_sum()

    def pick(value, n):
        return jnp.sum(jnp.where(row_lane == n, value, 0.0), axis=1, keepdims=True)

    rho_group, curve_group = pick(sums, 0), pick(sums, 1)
    ok = (rho_group > 0.0) & (curve_group > 0.0)
    centre = jnp.where(ok, rho_group / jnp.where(ok, curve_group, 1.0), 1.0)
    centre_tile = jnp.broadcast_to(centre, (T, W))

    def apply_y(items, acc):
        terms = [[] for _ in acc]
        for s in range(D):
            for (r, t), (y, h) in zip(items, coupled(yb, qyb, s, items)):
                at = tile_at(r)
                w = w_ref[s, at, lanes(t)]
                v = w - h
                v_ref[s, at, lanes(t)] = v
                z = zb[s, t, tile_at(r + T), :]
                res = bb[loc[s], at, lanes(t)] - centre_tile * w
                pre = z - centre_tile * y
                image = w - centre_tile * v
                for n, term in enumerate((res * pre, w * y, pre * image, y * v, z * v)):
                    terms[n].append(term)
        return tuple(a + tree(b) for a, b in zip(acc, terms))

    def whole(i):
        r = i * T
        return [(r, t) for t in range(nt)]

    acc = lax.fori_loop(0, ni, lambda i, c: apply_y(whole(i), c), (zero,) * 5)
    halo_wait(y_copies, 1)

    def edge_sums(stage):
        cols_part = tree([zcol_out[stage, n] * zcol_in[1, 1 - n] for n in range(2)])
        rows_part = tree([zrow_out[stage, n, s] * zrow_in[1, 1 - n, s] for n in range(2) for s in range(D)])
        return down(cols_part) + down(rows_part)

    edge_y, edge_z = edge_sums(1), edge_sums(0)
    acc = tuple(down(a) for a in acc)
    acc = (acc[0], acc[1], acc[2] + centre * (edge_z - centre * edge_y), acc[3] - edge_y, acc[4] - edge_z)

    s0, s2, t0, t2, zv, rho_own, curve_own = (
        full(value) for value in acc + (rho_inner + rho_rest + rho_edge, curve_inner + curve_rest + curve_edge)
    )
    total_out[...] = line([
        s0, 2.0 * (curve_own - centre * s2), s2,
        t0, s2 + zv - 2.0 * centre * t2, t2,
        rho_own, curve_own, centre,
    ])
    pl.semaphore_wait(met_sem, size1 - 1)
    mine = table_ref.at[pl.ds((layer * pxs + px) * pys + py, 1), :]
    pz = 4 if pxs % 4 == 0 else pxs
    px_hi = pxs // pz
    there = [
        (a, x, z, y) for a in range(layers) for x in range(px_hi) for z in range(pz) for y in range(pys)
    ]
    ring = lambda d, n: min(d, n - d)
    there.sort(key=lambda o: -(ring(o[1], px_hi) + ring(o[2], pz) + ring(o[3], pys)))
    for a, x, z, y in there:
        if a or x or z or y:
            peer = {
                "layer": lax.rem(layer + a, layers),
                "px": lax.rem(px // pz + x, px_hi) * pz + lax.rem(lax.rem(px, pz) + z, pz),
                "py": lax.rem(py + y, pys),
            }
            remote(total_out, mine, p_recv, peer, out_sem.at[1]).start()
    pltpu.make_async_copy(total_out, mine, p_recv).start()
    mend_rows(v_ref, 1)
    left_part, right_part = zcol_in[1, 1], col_out[...] * zcol_in[1, 0]

    def mend(i, carry):
        at = tile_at(i * T)
        for s in range(D):
            for t in (0, nt - 1):
                v_ref[s, at, lanes(t)] = v_ref[s, at, lanes(t)] - col_term(left_part, right_part, s * ni + i, t)
        return carry

    lax.fori_loop(0, ni, mend, 0)
    pltpu.make_async_copy(table_ref, table_ref, p_recv).wait()
    table = table_ref[...]
    table_lane = lax.broadcasted_iota(jnp.int32, table.shape, 1)
    centres = jnp.sum(jnp.where(table_lane == 8, table, 0.0), axis=1, keepdims=True)
    plain = jnp.sum(table, axis=0, keepdims=True)
    rho, curve_first = pick(plain, 6), pick(plain, 7)
    alpha = rho / curve_first
    delta = alpha - centres
    linear = (table_lane == 1) | (table_lane == 4)
    square = (table_lane == 2) | (table_lane == 5)
    powers = jnp.where(linear, -delta, jnp.where(square, delta * delta, 1.0))
    moved = jnp.sum(table * powers, axis=0, keepdims=True)
    rho_next = jnp.sum(jnp.where(row_lane < 3, moved, 0.0), axis=1, keepdims=True)
    curve = jnp.sum(jnp.where((row_lane >= 3) & (row_lane < 6), moved, 0.0), axis=1, keepdims=True)
    beta = rho_next / rho
    alpha_next = rho_next / (curve - beta * rho_next / alpha)
    factors[0] = jnp.broadcast_to(alpha + alpha_next * (1.0 + beta), (T, W))
    factors[1] = jnp.broadcast_to(alpha * alpha_next, (T, W))
    for copy in sends:
        copy.wait_send()
    for condition, copy in gated:
        gate(condition, copy.wait_send)
    wait_rows(size1 - 1, out_sem.at[0])
    wait_rows(len(there) - 1, out_sem.at[1])

    @pl.when(bottom)
    def _():
        for copy in c3_copies:
            copy.wait_send()


def finish(shape, bb, zb, yb, w_ref, v_ref, factors, x_hbm, r_hbm, x_buf, r_buf, sem):
    rows, cols = shape
    layer = lax.axis_index("layer")
    loc = [s + layer * (D - 1 - 2 * s) for s in range(D)]
    big, small = factors[0], factors[1]
    stops = [0, T, rows // 4, rows // 2, 3 * rows // 4, rows]
    copies = []

    def body(i, carry):
        r = i * T
        at = pl.ds(pl.multiple_of(r, T), T)
        above = pl.ds(pl.multiple_of(r + T, T), T)
        for s in range(D):
            l = loc[s]
            for t in range(cols // W):
                col = slice(t * W, (t + 1) * W)
                x_buf[l, at, col] = big * zb[s, t, above, :] - small * yb[s, t, above, :]
                r_buf[l, at, col] = bb[l, at, col] - big * w_ref[s, at, col] + small * v_ref[s, at, col]
        return carry

    for c, (lo, hi) in enumerate(zip(stops, stops[1:])):
        if hi == lo:
            continue
        lax.fori_loop(lo // T, hi // T, body, 0)
        at = pl.ds(lo, hi - lo)
        for n, (src, dst) in enumerate(((x_buf, x_hbm), (r_buf, r_hbm))):
            copies.append(pltpu.make_async_copy(src.at[:, at, :], dst.at[:, at, :], sem.at[2 * c + n]))
            copies[-1].start()
    for copy in copies:
        copy.wait()


def solution(mesh):
    layers, pxs, pys = (mesh.shape[a] for a in ("layer", "px", "py"))
    spec = P("layer", "px", "py")

    def step(*args):
        depth, rows, cols = args[0].shape
        nt = cols // W
        block = (depth, rows, cols)
        padded = (depth, nt, rows + 2 * T, W)
        size1 = layers * pys
        dma = pltpu.SemaphoreType.DMA
        vmem = lambda *dims: pltpu.VMEM(dims, F32)
        scratch = [
            vmem(depth, rows + T, cols), vmem(*block), vmem(*block), pltpu.VMEM(block, jnp.int32), vmem(*block),
            vmem(*block), vmem(*block), vmem(*block), vmem(rows, cols), vmem(rows, cols), vmem(rows, cols),
            vmem(*padded), vmem(*padded),
            vmem(2, rows, cols), vmem(2, rows, cols), vmem(rows, cols), vmem(rows, cols),
            vmem(depth, nt, W), vmem(depth, nt, W), vmem(T, W), vmem(T, W),
            vmem(2, 2, depth, nt, W), vmem(2, 2, depth, nt, W), vmem(2, 2, T, W), vmem(2, 2, T, W),
            vmem(1, 1, W), vmem(size1, 1, W), vmem(1, W), vmem(size1 * pxs, W), vmem(size1 * pxs, 1, W),
            dma((7,)), dma((8,)), dma((13,)), dma, dma, pltpu.SemaphoreType.REGULAR((4,)), pltpu.SemaphoreType.REGULAR,
        ]
        out = lambda *dims: jax.ShapeDtypeStruct(dims, F32)
        in_vmem = pl.BlockSpec(memory_space=pltpu.VMEM)
        in_hbm = pl.BlockSpec(memory_space=pltpu.HBM)
        kept = pl.pallas_call(
            functools.partial(kernel, (rows, cols), (layers, pxs, pys)),
            out_shape=(vmem(*block), vmem(*padded), vmem(*padded), vmem(*block), vmem(*block), vmem(2, T, W)),
            in_specs=[in_hbm] * 6,
            out_specs=(in_vmem,) * 6,
            scratch_shapes=scratch,
            compiler_params=pltpu.CompilerParams(
                collective_id=0, has_side_effects=True, vmem_limit_bytes=36 * 2**20
            ),
        )(*(pltpu.with_memory_space_constraint(arg, pltpu.HBM) for arg in args))
        return pl.pallas_call(
            functools.partial(finish, (rows, cols)),
            out_shape=(out(*block), out(*block)),
            in_specs=[in_vmem] * 6,
            out_specs=(in_hbm, in_hbm),
            scratch_shapes=[vmem(*block), vmem(*block), dma((10,))],
            compiler_params=pltpu.CompilerParams(vmem_limit_bytes=6 * 2**20),
        )(*kept)

    return jax.shard_map(step, mesh=mesh, in_specs=(spec,) * 6, out_specs=(spec, spec), check_vma=False)
```

```python
import functools

import jax
import jax.numpy as jnp
from jax import lax
from jax.experimental import pallas as pl
from jax.experimental.pallas import tpu as pltpu
from jax.sharding import PartitionSpec as P

MESH = pl.DeviceIdType.MESH
F32 = jnp.float32
D = 4
T = 8
W = 128


def kernel(shape, counts, *refs):
    dma = pltpu.SemaphoreType.DMA
    pl.run_scoped(functools.partial(solve_all, shape, counts, *refs), dma((34,)), dma((34,)))


def solve_all(
    shape, counts,
    b_hbm, rw_hbm, cl_hbm, vi_hbm, mk_hbm, gd_hbm,
    bb, zb, yb, w_ref, v_ref, factors,
    rwp, cl, vi, mk, gd, inv, gain, num, c3, q3a, q3b,
    qb, qyb, fg_out, fg_in, f_out, f_in,
    row_out, row_in, col_out, col_in,
    zrow_out, zrow_in, zcol_out, zcol_in,
    part, group, total_out, table_ref, sized,
    s_recv, z_recv, m_recv, g_recv, p_recv, far_sem, met_sem,
    load_sem, out_sem,
):
    rows, cols = shape
    layers, pxs, pys = counts
    nt = cols // W
    ni = rows // T
    layer = lax.axis_index("layer")
    px = lax.axis_index("px")
    py = lax.axis_index("py")
    bottom = layer == 0
    loc = [s + layer * (D - 1 - 2 * s) for s in range(D)]
    via = [s + layer * (D - 2 - 2 * s) for s in range(D - 1)]
    size1 = layers * pys
    me1 = layer * pys + py

    def group_peer(d):
        other = lax.rem(me1 + d, size1)
        return {"layer": other // pys, "py": lax.rem(other, pys)}

    def px_peer(d):
        return {"px": lax.rem(px + d, pxs)}

    def py_peer(d):
        return {"py": lax.rem(py + d, pys)}

    partner = {"layer": 1 - layer}
    near = [partner, px_peer(1), px_peer(pxs - 1), py_peer(1), py_peer(pys - 1)]

    barrier = pltpu.get_barrier_semaphore()
    for peer in near:
        pl.semaphore_signal(barrier, inc=1, device_id=peer, device_id_type=MESH)
    has_upper, has_lower = px > 0, px < pxs - 1
    has_left, has_right = py > 0, py < pys - 1

    slot = [0]

    def load(src, dst):
        copy = pltpu.make_async_copy(src, dst, load_sem.at[slot[0]])
        slot[0] += 1
        return copy

    last = (nt - 1) * W
    cl_edge = load(cl_hbm.at[:, :, last : last + W], cl.at[:, :, last : last + W])
    rw_edge = load(rw_hbm.at[:, rows - T : rows, :], rwp.at[:, rows : rows + T, :])
    top_loads = [load(vi_hbm.at[D - 1], vi.at[D - 1]), load(mk_hbm.at[D - 1], mk.at[D - 1])]
    rw_edge.start()
    cl_edge.start()

    @pl.when(bottom)
    def _():
        for copy in top_loads:
            copy.start()

    quarter = rows // 4
    stops = [0, quarter, 2 * quarter, 3 * quarter]
    if quarter >= 4 * T:
        stops.append(rows - 2 * T)
    stops.append(rows)
    chunks = list(zip(stops, stops[1:]))
    chunk_loads = []
    for lo, hi in chunks:
        at = pl.ds(lo, hi - lo)
        short = pl.ds(lo, min(hi, rows - T) - lo)
        chunk_loads.append([] if lo >= rows - T else [
            load(rw_hbm.at[:, short, :], rwp.at[:, pl.ds(T + lo, min(hi, rows - T) - lo), :]),
        ])
        chunk_loads[-1] += [
            load(cl_hbm.at[:, at, 0:last], cl.at[:, at, 0:last]),
            load(vi_hbm.at[0 : D - 1, at, :], vi.at[0 : D - 1, at, :]),
            load(mk_hbm.at[0 : D - 1, at, :], mk.at[0 : D - 1, at, :]),
            load(gd_hbm.at[:, at, :], gd.at[:, at, :]),
            load(b_hbm.at[:, at, :], bb.at[:, at, :]),
        ]
        for copy in chunk_loads[-1]:
            copy.start()

    lane = lax.broadcasted_iota(jnp.int32, (T, W), 1)
    sub = lax.broadcasted_iota(jnp.int32, (T, W), 0)
    zero = jnp.zeros((T, W), F32)

    def gate(condition, *actions):
        @pl.when(condition)
        def _():
            for action in actions:
                action()

    out_slot = [2]

    def remote(src, dst, recv, peer, send=None):
        if send is None:
            send = out_sem.at[out_slot[0]]
            out_slot[0] += 1
        return pltpu.make_async_remote_copy(
            src_ref=src, dst_ref=dst, send_sem=send, recv_sem=recv,
            device_id=peer, device_id_type=MESH,
        )

    def wait_rows(count, sem):
        pltpu.make_async_copy(sized.at[0:count], sized.at[0:count], sem).wait()

    def lanes(t):
        return slice(t * W, (t + 1) * W)

    def tile_at(r):
        return pl.ds(pl.multiple_of(r, T), T)

    cl_edge.wait()
    packs = []
    for s in range(D):
        packed = zero
        for i in range(ni):
            k = s * ni + i
            value = cl[loc[s], i * T : (i + 1) * T, lanes(nt - 1)]
            packed = jnp.where(lane == k, pltpu.roll(value, (k + 1) % W, axis=1), packed)
        packs.append(packed)
    col_out[...] = (packs[0] + packs[1]) + (packs[2] + packs[3])
    rw_edge.wait()
    for s in range(D):
        for t in range(nt):
            row_out[s, t : t + 1, :] = rwp[loc[s], rows + T - 1 : rows + T, lanes(t)]

    pl.semaphore_wait(barrier, len(near))
    row_copy = remote(row_out, row_in, s_recv.at[0], px_peer(1))
    col_copy = remote(col_out, col_in, s_recv.at[1], py_peer(1))
    gate(has_lower, row_copy.start)
    gate(has_right, col_copy.start)
    for peer in near:
        pl.semaphore_signal(far_sem.at[0], inc=1, device_id=peer, device_id_type=MESH)
    c3_copies = [
        remote(c3.at[pl.ds(lo, hi - lo)], c3.at[pl.ds(lo, hi - lo)], s_recv.at[2 + c], partner)
        for c, (lo, hi) in enumerate(chunks)
    ]

    def join(i, carry):
        at = tile_at(i * T)
        c3[at, :] = vi[D - 1, at, :] * mk[D - 1, at, :].astype(F32)
        return carry

    @pl.when(bottom)
    def _():
        for copy in top_loads:
            copy.wait()
        for (lo, hi), copy in zip(chunks, c3_copies):
            lax.fori_loop(lo // T, hi // T, join, 0)
            copy.start()

    gated = [(has_lower, row_copy), (has_right, col_copy)]
    sends = []

    hops = []
    while (2 << len(hops)) < pxs // 2:
        hops.append(2 << len(hops))

    def greet(n):
        if n < len(hops):
            for d in (hops[n], pxs - hops[n]):
                pl.semaphore_signal(far_sem.at[1 + n], inc=1, device_id=px_peer(d), device_id_type=MESH)

    def greeted(n):
        if n < len(hops):
            pl.semaphore_wait(far_sem.at[1 + n], 2)

    def inner(i):
        r = i * T
        return [(r, t) for t in range(1, nt - 1)]

    span = 7 if (ni - 2) % 7 == 0 else 2

    def sides(j):
        starts = [(1 + j * span + m) * T for m in range(span)]
        return [(r, t) for r in starts for t in (0, nt - 1)]

    def ends(j):
        r = j * (rows - T)
        return [(r, t) for t in range(nt)]

    def ends_work(body, carry):
        return lax.fori_loop(0, 2, lambda j, c: body(ends(j), c), carry)

    def sides_work(body, carry):
        return lax.fori_loop(0, (ni - 2) // span, lambda j, c: body(sides(j), c), carry)

    def inner_work(body, carry, start=1, stop=None):
        stop = ni - 1 if stop is None else stop
        return lax.fori_loop(start, stop, lambda i, c: body(inner(i), c), carry)

    def spread(packed, k, to):
        return pltpu.roll(packed, lax.rem(to + W - k, W), axis=1)

    def coupling(s, at, t):
        return vi[via[s], at, lanes(t)] * mk[via[s], at, lanes(t)].astype(F32)

    def factor(items, carry):
        g = [None] * len(items)
        n = [None] * len(items)
        below = [None] * len(items)
        for s in range(D):
            l = loc[s]
            for m, (r, t) in enumerate(items):
                at = tile_at(r)
                rw = rwp[l, tile_at(r + T), lanes(t)]
                before = rwp[l, at, lanes(t)]
                up = pltpu.roll(jnp.where(sub == T - 1, before, rw), 1, axis=0)
                c = cl[l, at, lanes(t)]
                if t == 0:
                    k = s * ni + r // T
                    left = jnp.where(lane == 0, spread(col_in[...], k, 0), pltpu.roll(c, 1, axis=1))
                else:
                    left = pltpu.roll(jnp.where(lane == W - 1, cl[l, at, lanes(t - 1)], c), 1, axis=1)
                if s < D - 1:
                    above = coupling(s, at, t)
                else:
                    above = c3[at, lanes(t)]
                diagonal = gd[l, at, lanes(t)] + rw + up + c + left + above
                right_side = bb[l, at, lanes(t)]
                if s:
                    diagonal = diagonal + below[m]
                    inverse = 1.0 / (diagonal - below[m] * g[m])
                    n[m] = right_side + g[m] * n[m]
                else:
                    inverse = 1.0 / diagonal
                    n[m] = right_side
                below[m] = above
                g[m] = above * inverse
                inv[s, at, lanes(t)] = inverse
                gain[s, at, lanes(t)] = g[m]
                num[s, at, lanes(t)] = n[m]
                if s == D - 1:
                    fg_out[0, at, lanes(t)] = n[m] * inverse
                    fg_out[1, at, lanes(t)] = g[m]
        return carry

    cut = max(2, 12 * ni // 16)
    regions = [
        (pl.ds(T, (cut - 1) * T), pl.ds(W, cols - 2 * W)),
        (pl.ds(cut * T, (ni - 1 - cut) * T), pl.ds(W, cols - 2 * W)),
        (pl.ds(0, rows), pl.ds(0, W)),
        (pl.ds(0, rows), pl.ds(cols - W, W)),
        (pl.ds(0, T), pl.ds(W, cols - 2 * W)),
        (pl.ds(rows - T, T), pl.ds(W, cols - 2 * W)),
    ]

    def middle(out, into, which, base):
        copies = []
        for e, (i, j) in enumerate(which):
            if len(out.shape) == 3:
                src, dst = out.at[:, i, j], into.at[:, i, j]
            else:
                src, dst = out.at[i, j], into.at[i, j]
            copies.append(remote(src, dst, m_recv.at[base + e], partner))
        for copy in copies:
            copy.start()
        sends.extend(copies)
        return copies

    def deep(i):
        r = i * T
        return [(r, t) for t in range(1, nt)]

    fg_inner = []
    for c, (lo, hi) in enumerate(chunks):
        for copy in chunk_loads[c]:
            copy.wait()
        gate(jnp.logical_not(bottom), c3_copies[c].wait_recv)
        lo = max(T, lo)
        lax.fori_loop(lo // T, hi // T, lambda i, x: factor(deep(i), x), 0)
        fg_inner += middle(fg_out, fg_in, [(pl.ds(lo, hi - lo), pl.ds(W, cols - W))], c)

    gate(has_left, col_copy.wait_recv)
    gate(has_upper, row_copy.wait_recv)
    for s in range(D):
        for t in range(nt):
            rwp[loc[s], T - 1 : T, lanes(t)] = jnp.where(has_upper, row_in[s, t : t + 1, :], 0.0)
    col_in[...] = jnp.where(has_left, col_in[...], 0.0)
    group_of = min(8, ni)
    lax.fori_loop(
        0, ni // group_of,
        lambda j, x: factor([(j * group_of * T + m * T, 0) for m in range(group_of)], x), 0,
    )
    lax.fori_loop(0, 1, lambda i, x: factor(deep(i), x), 0)
    pl.semaphore_wait(far_sem.at[0], len(near))
    greet(0)
    fg_edge = middle(fg_out, fg_in, [(pl.ds(0, rows), pl.ds(0, W)), (pl.ds(0, T), pl.ds(W, cols - W))], len(chunks))

    def solve(first, z, q, f_ref, items, carry):
        rho, pack_l, pack_r = carry
        following = [None] * len(items)
        terms = []
        for s in range(D - 1, -1, -1):
            l = loc[s]
            for m, (r, t) in enumerate(items):
                at = tile_at(r)
                if s == D - 1:
                    if first:
                        other = fg_in[1, at, lanes(t)]
                        g = gain[s, at, lanes(t)]
                        quotient = 1.0 / (1.0 - g * other)
                        scale = quotient * inv[s, at, lanes(t)]
                        g = quotient * g
                        q3a[at, lanes(t)] = scale
                        q3b[at, lanes(t)] = g
                        theirs = fg_in[0, at, lanes(t)]
                    else:
                        scale = q3a[at, lanes(t)]
                        g = q3b[at, lanes(t)]
                        theirs = f_ref[at, lanes(t)]
                    value = scale * num[s, at, lanes(t)] + g * theirs
                else:
                    value = num[s, at, lanes(t)] * inv[s, at, lanes(t)] + gain[s, at, lanes(t)] * following[m]
                following[m] = value
                z[s, t, tile_at(r + T), :] = value
                q[s, t, tile_at(r + T), :] = rwp[l, tile_at(r + T), lanes(t)] * value
                if first:
                    terms.append(bb[l, at, lanes(t)] * value)
                if t == 0:
                    k = s * ni + r // T
                    pack_l = jnp.where(lane == k, pltpu.roll(value, k, axis=1), pack_l)
                if t == nt - 1:
                    k = s * ni + r // T
                    side = cl[l, at, lanes(t)] * value
                    pack_r = jnp.where(lane == k, pltpu.roll(side, k + 1, axis=1), pack_r)
        if first:
            rho = rho + tree(terms)
        return rho, pack_l, pack_r

    def tree(values):
        while len(values) > 1:
            values = [a + b for a, b in zip(values[::2], values[1::2])] + ([values[-1]] if len(values) % 2 else [])
        return values[0]

    def start_halos(stage, first, pairs):
        copies = []
        for n, (condition, out, into, peer) in enumerate(pairs):
            copy = remote(out, into, z_recv.at[4 * stage + first + n], peer)
            gate(condition, copy.start)
            gated.append((condition, copy))
            copies.append(copy)
        return copies

    def send_rows(z, q, stage):
        for s in range(D):
            for t in range(nt):
                zrow_out[stage, 0, s, t : t + 1, :] = z[s, t, T : T + 1, :]
                zrow_out[stage, 1, s, t : t + 1, :] = q[s, t, rows + T - 1 : rows + T, :]
        return start_halos(stage, 0, (
            (has_upper, zrow_out.at[stage, 0], zrow_in.at[stage, 0], px_peer(pxs - 1)),
            (has_lower, zrow_out.at[stage, 1], zrow_in.at[stage, 1], px_peer(1)),
        ))

    def send_cols(pack_l, pack_r, stage):
        zcol_out[stage, 0] = pack_l
        zcol_out[stage, 1] = pack_r
        return start_halos(stage, 2, (
            (has_left, zcol_out.at[stage, 0], zcol_in.at[stage, 0], py_peer(pys - 1)),
            (has_right, zcol_out.at[stage, 1], zcol_in.at[stage, 1], py_peer(1)),
        ))

    def halo_wait(copies, stage):
        for condition, copy in zip((has_lower, has_upper, has_right, has_left), copies):
            gate(condition, copy.wait_recv)
        zcol_in[stage, 0] = jnp.where(has_right, zcol_in[stage, 0], 0.0)
        zcol_in[stage, 1] = jnp.where(has_left, zcol_in[stage, 1], 0.0)
        zrow_in[stage, 0] = jnp.where(has_lower, zrow_in[stage, 0], 0.0)
        zrow_in[stage, 1] = jnp.where(has_upper, zrow_in[stage, 1], 0.0)

    def mend_rows(ref, stage):
        for s in range(D):
            for t in range(nt):
                ref[s, 0:1, lanes(t)] = ref[s, 0:1, lanes(t)] - zrow_in[stage, 1, s, t : t + 1, :]
                ref[s, rows - 1 : rows, lanes(t)] = (
                    ref[s, rows - 1 : rows, lanes(t)] - row_out[s, t : t + 1, :] * zrow_in[stage, 0, s, t : t + 1, :]
                )

    def col_term(left_part, right_part, k, t):
        if t == 0:
            return jnp.where(lane == 0, spread(left_part, k, 0), 0.0)
        return jnp.where(lane == W - 1, spread(right_part, k, W - 1), 0.0)

    for z, q in ((zb, qb), (yb, qyb)):
        for s in range(D):
            for t in range(nt):
                z[s, t, rows + T : rows + 2 * T, :] = zero
                q[s, t, 0:T, :] = zero

    solve_z = functools.partial(solve, True, zb, qb, None)
    for copy in fg_inner:
        copy.wait_recv()
    rho_inner = inner_work(solve_z, (zero, zero, zero), 1, cut)[0]
    rho_rest = inner_work(solve_z, (zero, zero, zero), cut)[0]
    for copy in fg_edge:
        copy.wait_recv()
    carry = ends_work(solve_z, (zero, zero, zero))
    z_copies = send_rows(zb, qb, 0)
    rho_edge, pack_l, pack_r = sides_work(solve_z, carry)
    z_copies += send_cols(pack_l, pack_r, 0)

    def coupled(z, q, s, items):
        l = loc[s]
        zs, ps, out = {}, {}, []

        def own(m, r, t):
            if (m, t) not in zs:
                zs[m, t] = z[s, t, tile_at(r + T), :]
            return zs[m, t]

        def product(m, r, t):
            if (m, t) not in ps:
                ps[m, t] = cl[l, tile_at(r), lanes(t)] * own(m, r, t)
            return ps[m, t]

        rows_seen = []
        for r, t in items:
            m = next((n for n, other in enumerate(rows_seen) if other is r), None)
            if m is None:
                rows_seen.append(r)
                m = len(rows_seen) - 1
            at = tile_at(r)
            value = own(m, r, t)
            down = z[s, t, pl.ds(r + T + 1, T), :]
            up = q[s, t, pl.ds(r + T - 1, T), :]
            after = own(m, r, t + 1) if t < nt - 1 else 0.0
            before = product(m, r, t - 1) if t else 0.0
            right = pltpu.roll(jnp.where(lane == 0, after, value), W - 1, axis=1)
            left = pltpu.roll(jnp.where(lane == W - 1, before, product(m, r, t)), 1, axis=1)
            rw = rwp[l, tile_at(r + T), lanes(t)]
            c = cl[l, at, lanes(t)]
            out.append((value, rw * down + up + (c * right + left)))
        return out

    def apply_z(items, curve):
        n = [None] * len(items)
        terms = []
        for s in range(D):
            for m, ((r, t), (value, h)) in enumerate(zip(items, coupled(zb, qb, s, items))):
                at = tile_at(r)
                w = bb[loc[s], at, lanes(t)] - h
                w_ref[s, at, lanes(t)] = w
                terms.append(value * w)
                n[m] = w if s == 0 else w + gain[s - 1, at, lanes(t)] * n[m]
                num[s, at, lanes(t)] = n[m]
                if s == D - 1:
                    f_out[at, lanes(t)] = n[m] * inv[s, at, lanes(t)]
        return curve + tree(terms)

    def start_edge(items, carry):
        for s in range(D):
            for (r, t), (_, h) in zip(items, coupled(zb, qb, s, items)):
                at = tile_at(r)
                w_ref[s, at, lanes(t)] = bb[loc[s], at, lanes(t)] - h
        return carry

    def end_edge(left_part, right_part, items, curve):
        n = [None] * len(items)
        terms = []
        for s in range(D):
            for m, (r, t) in enumerate(items):
                at = tile_at(r)
                w = w_ref[s, at, lanes(t)]
                if t in (0, nt - 1):
                    w = w - col_term(left_part, right_part, s * ni + r // T, t)
                    w_ref[s, at, lanes(t)] = w
                terms.append(zb[s, t, tile_at(r + T), :] * w)
                n[m] = w if s == 0 else w + gain[s - 1, at, lanes(t)] * n[m]
                num[s, at, lanes(t)] = n[m]
                if s == D - 1:
                    f_out[at, lanes(t)] = n[m] * inv[s, at, lanes(t)]
        return curve + tree(terms)

    def down(value):
        return jnp.sum(value, axis=0, keepdims=True)

    def full(value):
        return jnp.sum(down(value), axis=1, keepdims=True)

    row_lane = lax.broadcasted_iota(jnp.int32, (1, W), 1)

    def line(values):
        out = jnp.zeros((1, W), F32)
        for n, value in enumerate(values):
            out = jnp.where(row_lane == n, value, out)
        return out

    def gather_group(values):
        part[0] = line(values)
        group[pl.ds(me1, 1)] = line(values)[None]
        for d in range(1, size1):
            remote(part.at[0], group.at[me1], g_recv, group_peer(d), out_sem.at[0]).start()

    def group_sum():
        wait_rows(size1 - 1, g_recv)
        return tree([group[m] for m in range(size1)])

    curve_inner = inner_work(apply_z, zero, 1, cut)
    f_inner = middle(f_out, f_in, regions[:1], len(chunks) + 2)
    gather_group([full(rho_inner), full(curve_inner)])
    sides_work(start_edge, ends_work(start_edge, 0))
    halo_wait(z_copies, 0)
    greeted(0)
    greet(1)
    mend_rows(w_ref, 0)
    end_z = functools.partial(end_edge, zcol_in[0, 1], col_out[...] * zcol_in[0, 0])

    curve_edge = sides_work(end_z, ends_work(end_z, zero))
    f_edge = middle(f_out, f_in, regions[2:], len(chunks) + 4)
    curve_rest = inner_work(apply_z, zero, cut)
    f_rest = middle(f_out, f_in, regions[1:2], len(chunks) + 3)
    solve_y = functools.partial(solve, False, yb, qyb, f_in)
    carry = (zero, zero, zero)
    for copy in f_inner:
        copy.wait_recv()
    inner_work(solve_y, carry, 1, cut)
    for copy in f_edge:
        copy.wait_recv()
    carry = ends_work(solve_y, carry)
    y_copies = send_rows(yb, qyb, 1)
    carry = sides_work(solve_y, carry)
    y_copies += send_cols(carry[1], carry[2], 1)
    for copy in f_rest:
        copy.wait_recv()
    inner_work(solve_y, carry, cut)

    for n in range(1, len(hops)):
        greeted(n)
        greet(n + 1)
    for d in range(1, size1):
        pl.semaphore_signal(met_sem, inc=1, device_id=group_peer(d), device_id_type=MESH)
    sums = group_sum()

    def pick(value, n):
        return jnp.sum(jnp.where(row_lane == n, value, 0.0), axis=1, keepdims=True)

    rho_group, curve_group = pick(sums, 0), pick(sums, 1)
    ok = (rho_group > 0.0) & (curve_group > 0.0)
    centre = jnp.where(ok, rho_group / jnp.where(ok, curve_group, 1.0), 1.0)
    centre_tile = jnp.broadcast_to(centre, (T, W))

    def apply_y(items, acc):
        terms = [[] for _ in acc]
        for s in range(D):
            for (r, t), (y, h) in zip(items, coupled(yb, qyb, s, items)):
                at = tile_at(r)
                w = w_ref[s, at, lanes(t)]
                v = w - h
                v_ref[s, at, lanes(t)] = v
                z = zb[s, t, tile_at(r + T), :]
                res = bb[loc[s], at, lanes(t)] - centre_tile * w
                pre = z - centre_tile * y
                image = w - centre_tile * v
                for n, term in enumerate((res * pre, w * y, pre * image, y * v, z * v)):
                    terms[n].append(term)
        return tuple(a + tree(b) for a, b in zip(acc, terms))

    def whole(i):
        r = i * T
        return [(r, t) for t in range(nt)]

    acc = lax.fori_loop(0, ni, lambda i, c: apply_y(whole(i), c), (zero,) * 5)
    halo_wait(y_copies, 1)

    def edge_sums(stage):
        cols_part = tree([zcol_out[stage, n] * zcol_in[1, 1 - n] for n in range(2)])
        rows_part = tree([zrow_out[stage, n, s] * zrow_in[1, 1 - n, s] for n in range(2) for s in range(D)])
        return down(cols_part) + down(rows_part)

    edge_y, edge_z = edge_sums(1), edge_sums(0)
    acc = tuple(down(a) for a in acc)
    acc = (acc[0], acc[1], acc[2] + centre * (edge_z - centre * edge_y), acc[3] - edge_y, acc[4] - edge_z)

    s0, s2, t0, t2, zv, rho_own, curve_own = (
        full(value) for value in acc + (rho_inner + rho_rest + rho_edge, curve_inner + curve_rest + curve_edge)
    )
    total_out[...] = line([
        s0, 2.0 * (curve_own - centre * s2), s2,
        t0, s2 + zv - 2.0 * centre * t2, t2,
        rho_own, curve_own, centre,
    ])
    pl.semaphore_wait(met_sem, size1 - 1)
    mine = table_ref.at[pl.ds((layer * pxs + px) * pys + py, 1), :]
    pz = 4 if pxs % 4 == 0 else pxs
    px_hi = pxs // pz
    there = [
        (a, x, z, y) for a in range(layers) for x in range(px_hi) for z in range(pz) for y in range(pys)
    ]
    ring = lambda d, n: min(d, n - d)
    there.sort(key=lambda o: -(ring(o[1], px_hi) + ring(o[2], pz) + ring(o[3], pys)))
    for a, x, z, y in there:
        if a or x or z or y:
            peer = {
                "layer": lax.rem(layer + a, layers),
                "px": lax.rem(px // pz + x, px_hi) * pz + lax.rem(lax.rem(px, pz) + z, pz),
                "py": lax.rem(py + y, pys),
            }
            remote(total_out, mine, p_recv, peer, out_sem.at[1]).start()
    pltpu.make_async_copy(total_out, mine, p_recv).start()
    mend_rows(v_ref, 1)
    left_part, right_part = zcol_in[1, 1], col_out[...] * zcol_in[1, 0]

    def mend(i, carry):
        at = tile_at(i * T)
        for s in range(D):
            for t in (0, nt - 1):
                v_ref[s, at, lanes(t)] = v_ref[s, at, lanes(t)] - col_term(left_part, right_part, s * ni + i, t)
        return carry

    lax.fori_loop(0, ni, mend, 0)
    pltpu.make_async_copy(table_ref, table_ref, p_recv).wait()
    table = table_ref[...]
    table_lane = lax.broadcasted_iota(jnp.int32, table.shape, 1)
    centres = jnp.sum(jnp.where(table_lane == 8, table, 0.0), axis=1, keepdims=True)
    plain = jnp.sum(table, axis=0, keepdims=True)
    rho, curve_first = pick(plain, 6), pick(plain, 7)
    alpha = rho / curve_first
    delta = alpha - centres
    linear = (table_lane == 1) | (table_lane == 4)
    square = (table_lane == 2) | (table_lane == 5)
    powers = jnp.where(linear, -delta, jnp.where(square, delta * delta, 1.0))
    moved = jnp.sum(table * powers, axis=0, keepdims=True)
    rho_next = jnp.sum(jnp.where(row_lane < 3, moved, 0.0), axis=1, keepdims=True)
    curve = jnp.sum(jnp.where((row_lane >= 3) & (row_lane < 6), moved, 0.0), axis=1, keepdims=True)
    beta = rho_next / rho
    alpha_next = rho_next / (curve - beta * rho_next / alpha)
    factors[0] = jnp.broadcast_to(alpha + alpha_next * (1.0 + beta), (T, W))
    factors[1] = jnp.broadcast_to(alpha * alpha_next, (T, W))
    for copy in sends:
        copy.wait_send()
    for condition, copy in gated:
        gate(condition, copy.wait_send)
    wait_rows(size1 - 1, out_sem.at[0])
    wait_rows(len(there) - 1, out_sem.at[1])

    @pl.when(bottom)
    def _():
        for copy in c3_copies:
            copy.wait_send()


def finish(shape, bb, zb, yb, w_ref, v_ref, factors, x_hbm, r_hbm, x_buf, r_buf, sem):
    rows, cols = shape
    layer = lax.axis_index("layer")
    loc = [s + layer * (D - 1 - 2 * s) for s in range(D)]
    big, small = factors[0], factors[1]
    stops = [0, T, rows // 4, rows // 2, 3 * rows // 4, rows]
    copies = []

    def body(i, carry):
        r = i * T
        at = pl.ds(pl.multiple_of(r, T), T)
        above = pl.ds(pl.multiple_of(r + T, T), T)
        for s in range(D):
            l = loc[s]
            for t in range(cols // W):
                col = slice(t * W, (t + 1) * W)
                x_buf[l, at, col] = big * zb[s, t, above, :] - small * yb[s, t, above, :]
                r_buf[l, at, col] = bb[l, at, col] - big * w_ref[s, at, col] + small * v_ref[s, at, col]
        return carry

    for c, (lo, hi) in enumerate(zip(stops, stops[1:])):
        if hi == lo:
            continue
        lax.fori_loop(lo // T, hi // T, body, 0)
        at = pl.ds(lo, hi - lo)
        for n, (src, dst) in enumerate(((x_buf, x_hbm), (r_buf, r_hbm))):
            copies.append(pltpu.make_async_copy(src.at[:, at, :], dst.at[:, at, :], sem.at[2 * c + n]))
            copies[-1].start()
    for copy in copies:
        copy.wait()


def solution(mesh):
    layers, pxs, pys = (mesh.shape[a] for a in ("layer", "px", "py"))
    spec = P("layer", "px", "py")

    def step(*args):
        depth, rows, cols = args[0].shape
        nt = cols // W
        block = (depth, rows, cols)
        padded = (depth, nt, rows + 2 * T, W)
        size1 = layers * pys
        dma = pltpu.SemaphoreType.DMA
        vmem = lambda *dims: pltpu.VMEM(dims, F32)
        scratch = [
            vmem(depth, rows + T, cols), vmem(*block), vmem(*block), pltpu.VMEM(block, jnp.int32), vmem(*block),
            vmem(*block), vmem(*block), vmem(*block), vmem(rows, cols), vmem(rows, cols), vmem(rows, cols),
            vmem(*padded), vmem(*padded),
            vmem(2, rows, cols), vmem(2, rows, cols), vmem(rows, cols), vmem(rows, cols),
            vmem(depth, nt, W), vmem(depth, nt, W), vmem(T, W), vmem(T, W),
            vmem(2, 2, depth, nt, W), vmem(2, 2, depth, nt, W), vmem(2, 2, T, W), vmem(2, 2, T, W),
            vmem(1, 1, W), vmem(size1, 1, W), vmem(1, W), vmem(size1 * pxs, W), vmem(size1 * pxs, 1, W),
            dma((7,)), dma((8,)), dma((13,)), dma, dma, pltpu.SemaphoreType.REGULAR((4,)), pltpu.SemaphoreType.REGULAR,
        ]
        out = lambda *dims: jax.ShapeDtypeStruct(dims, F32)
        in_vmem = pl.BlockSpec(memory_space=pltpu.VMEM)
        in_hbm = pl.BlockSpec(memory_space=pltpu.HBM)
        kept = pl.pallas_call(
            functools.partial(kernel, (rows, cols), (layers, pxs, pys)),
            out_shape=(vmem(*block), vmem(*padded), vmem(*padded), vmem(*block), vmem(*block), vmem(2, T, W)),
            in_specs=[in_hbm] * 6,
            out_specs=(in_vmem,) * 6,
            scratch_shapes=scratch,
            compiler_params=pltpu.CompilerParams(
                collective_id=0, has_side_effects=True, vmem_limit_bytes=36 * 2**20
            ),
        )(*(pltpu.with_memory_space_constraint(arg, pltpu.HBM) for arg in args))
        return pl.pallas_call(
            functools.partial(finish, (rows, cols)),
            out_shape=(out(*block), out(*block)),
            in_specs=[in_vmem] * 6,
            out_specs=(in_hbm, in_hbm),
            scratch_shapes=[vmem(*block), vmem(*block), dma((10,))],
            compiler_params=pltpu.CompilerParams(vmem_limit_bytes=6 * 2**20),
        )(*kept)

    return jax.shard_map(step, mesh=mesh, in_specs=(spec,) * 6, out_specs=(spec, spec), check_vma=False)
```
